32 devices in a mesh: fsdp: 32 (over z, y, x, core).
Axes of the slice: x: 2, y: 2, z: 4, core: 2. Of those that a mesh axis runs over, the one named last changes fastest.
Arguments:
- x: bfloat16 [32, 192, 1024], P('fsdp')
- lengths: int32 [32], P('fsdp')
- d_y: bfloat16 [32, 192, 1024], P('fsdp')
- w_attn: bfloat16 [2, 4, 1024, 1024], P(None, None, 'fsdp')
- b_attn: bfloat16 [2, 4, 1024], P(None, None, 'fsdp')
- ln_par: bfloat16 [2, 4, 1024], P(None, None, 'fsdp')
- w_up: bfloat16 [2, 1024, 4096], P(None, 'fsdp')
- b_up: bfloat16 [2, 4096], P(None, 'fsdp')
- w_down: bfloat16 [2, 4096, 1024], P(None, 'fsdp')
- b_down: bfloat16 [2, 1024], P(None, 'fsdp')
Outputs:
- output 1: bfloat16 [32, 192, 1024], P('fsdp')
- output 2: float32 [2, 4, 1024, 1024], P(None, None, 'fsdp')
- output 3: float32 [2, 4, 1024], P(None, None, 'fsdp')
- output 4: float32 [2, 4, 1024], P(None, None, 'fsdp')
- output 5: float32 [2, 1024, 4096], P(None, 'fsdp')
- output 6: float32 [2, 4096], P(None, 'fsdp')
- output 7: float32 [2, 4096, 1024], P(None, 'fsdp')
- output 8: float32 [2, 1024], P(None, 'fsdp')
All inputs are finite; a program needn't handle non-finite values.
Results may differ from the reference program's by a relative error of at most 0.0160853.
Values are sent between devices in bfloat16 or wider.
A program may use at most 1 GiB of HBM per device.

```python
import jax
import jax.numpy as jnp
from jax import lax

MODEL_DIM = 1024
FFN_DIM = 4096
HEAD_DIM = 64
NUM_LAYERS = 2
SEQ_LEN = 192
SEQ_DEV = 1
GROUP_SIZE = 32
EPS = 1e-5
THETA = 10000.0
NUM_HEADS = MODEL_DIM // HEAD_DIM
BATCH = SEQ_DEV * GROUP_SIZE
MIN_LEN = SEQ_LEN // 8


def setup_inputs(seed: int = 0) -> dict:
    key_list = jax.random.split(jax.random.key(seed), 10)
    seq_index = jnp.arange(BATCH)
    drawn_len = jax.random.randint(key_list[1], (BATCH,), MIN_LEN, SEQ_LEN + 1)
    lengths = jnp.where(seq_index == 0, SEQ_LEN, jnp.where(seq_index == 1, MIN_LEN, drawn_len)).astype(jnp.int32)
    act_shape = (BATCH, SEQ_LEN, MODEL_DIM)
    dy_scale = float(BATCH * SEQ_LEN) ** -0.25
    ln_base = jnp.array([1.0, 0.0, 1.0, 0.0], dtype=jnp.float32)[None, :, None]
    return {
        'x': jax.random.normal(key_list[0], act_shape, jnp.float32).astype(jnp.bfloat16),
        'lengths': lengths,
        'd_y': (dy_scale * jax.random.normal(key_list[2], act_shape, jnp.float32)).astype(jnp.bfloat16),
        'w_attn': (MODEL_DIM ** -0.5 * jax.random.normal(key_list[3], (NUM_LAYERS, 4, MODEL_DIM, MODEL_DIM), jnp.float32)).astype(jnp.bfloat16),
        'b_attn': (0.3 * jax.random.normal(key_list[4], (NUM_LAYERS, 4, MODEL_DIM), jnp.float32)).astype(jnp.bfloat16),
        'ln_par': (ln_base + 0.2 * jax.random.normal(key_list[5], (NUM_LAYERS, 4, MODEL_DIM), jnp.float32)).astype(jnp.bfloat16),
        'w_up': (MODEL_DIM ** -0.5 * jax.random.normal(key_list[6], (NUM_LAYERS, MODEL_DIM, FFN_DIM), jnp.float32)).astype(jnp.bfloat16),
        'b_up': (0.5 * jax.random.normal(key_list[7], (NUM_LAYERS, FFN_DIM), jnp.float32)).astype(jnp.bfloat16),
        'w_down': (FFN_DIM ** -0.5 * jax.random.normal(key_list[8], (NUM_LAYERS, FFN_DIM, MODEL_DIM), jnp.float32)).astype(jnp.bfloat16),
        'b_down': (0.3 * jax.random.normal(key_list[9], (NUM_LAYERS, MODEL_DIM), jnp.float32)).astype(jnp.bfloat16),
    }


def to_bf16(tensor):
    return tensor.astype(jnp.bfloat16).astype(jnp.float32)


def norm_fwd(x_in, gain, shift):
    row_mean = jnp.mean(x_in, axis=-1, keepdims=True)
    centered = x_in - row_mean
    variance = jnp.mean(centered * centered, axis=-1, keepdims=True)
    return centered * lax.rsqrt(variance + EPS) * gain + shift


def rotary_tables():
    half_dim = HEAD_DIM // 2
    inv_freq = 1.0 / (THETA ** (jnp.arange(half_dim, dtype=jnp.float32) * (2.0 / HEAD_DIM)))
    angles = jnp.arange(SEQ_LEN, dtype=jnp.float32)[:, None] * inv_freq[None, :]
    return jnp.cos(angles)[:, None, :], jnp.sin(angles)[:, None, :]


def rotate(tensor, cos_tab, sin_tab):
    half_dim = HEAD_DIM // 2
    first_half = tensor[..., :half_dim]
    second_half = tensor[..., half_dim:]
    return jnp.concatenate([first_half * cos_tab - second_half * sin_tab, second_half * cos_tab + first_half * sin_tab], axis=-1)


def layer_fwd(x, weights, lengths, tables):
    w_attn, b_attn, ln_par, w_up, b_up, w_down, b_down = weights
    cos_tab, sin_tab = tables
    num_seq = x.shape[0]
    h_one = to_bf16(norm_fwd(x, ln_par[0], ln_par[1]))
    projected = jnp.einsum('bld,kde->kble', h_one, w_attn[:3]) + b_attn[:3, None, None, :]
    projected = projected.reshape(3, num_seq, SEQ_LEN, NUM_HEADS, HEAD_DIM)
    query_rot = to_bf16(rotate(projected[0] * (HEAD_DIM ** -0.5), cos_tab, sin_tab))
    key_rot = to_bf16(rotate(projected[1], cos_tab, sin_tab))
    values = to_bf16(projected[2])
    scores = jnp.einsum('bqhd,bkhd->bhqk', query_rot, key_rot)
    key_valid = jnp.arange(SEQ_LEN)[None, None, None, :] < lengths[:, None, None, None]
    attn_probs = to_bf16(jax.nn.softmax(jnp.where(key_valid, scores, -1e30), axis=-1))
    context = to_bf16(jnp.einsum('bhqk,bkhd->bqhd', attn_probs, values)).reshape(num_seq, SEQ_LEN, MODEL_DIM)
    x_mid = to_bf16(x + jnp.einsum('bld,de->ble', context, w_attn[3]) + b_attn[3])
    h_two = to_bf16(norm_fwd(x_mid, ln_par[2], ln_par[3]))
    act_out = to_bf16(jax.nn.gelu(jnp.einsum('bld,df->blf', h_two, w_up) + b_up, approximate=False))
    return to_bf16(x_mid + jnp.einsum('blf,fd->bld', act_out, w_down) + b_down)


def reference(x, lengths, d_y, w_attn, b_attn, ln_par, w_up, b_up, w_down, b_down):
    params = tuple(tensor.astype(jnp.float32) for tensor in (w_attn, b_attn, ln_par, w_up, b_up, w_down, b_down))
    tables = rotary_tables()

    def stack_fwd(x_block, param_set, len_block):
        hidden = x_block
        for layer_idx in range(NUM_LAYERS):
            hidden = layer_fwd(hidden, tuple(tensor[layer_idx] for tensor in param_set), len_block, tables)
        return hidden

    def block_step(grad_acc, block_in):
        x_block, len_block, dy_block = block_in

        def block_fwd(x_local, param_local):
            return stack_fwd(x_local, param_local, len_block)

        _, pull_back = jax.vjp(block_fwd, x_block.astype(jnp.float32), params)
        d_x_block, d_params = pull_back(dy_block.astype(jnp.float32))
        return jax.tree.map(jnp.add, grad_acc, d_params), d_x_block.astype(jnp.bfloat16)

    grad_zero = jax.tree.map(jnp.zeros_like, params)
    blocks_in = (x.reshape(GROUP_SIZE, SEQ_DEV, SEQ_LEN, MODEL_DIM), lengths.reshape(GROUP_SIZE, SEQ_DEV), d_y.reshape(GROUP_SIZE, SEQ_DEV, SEQ_LEN, MODEL_DIM))
    grad_sum, d_x = lax.scan(block_step, grad_zero, blocks_in)
    return (d_x.reshape(BATCH, SEQ_LEN, MODEL_DIM), grad_sum[0], grad_sum[1], grad_sum[2], grad_sum[3], grad_sum[4], grad_sum[5], grad_sum[6])
```

```python
import functools
import math
import jax
import jax.numpy as jnp
from jax import lax
from jax.experimental import pallas as pl
from jax.experimental.pallas import tpu as pltpu
from jax.sharding import PartitionSpec as P

MESH = pl.DeviceIdType.MESH
LAYERS = 2
ORDERS = (("b", 0, 1), ("b", 1, 0), ("a", 0, 1), ("a", 1, 0), ("b", 0, 1), ("b", 1, 0))
UNITS = [(layer, piece) for layer in range(LAYERS) for piece in range(6)] + [(0, 6)]
STAGE_LAG = (0, 0, 1, 3)
AHEAD = 2


def gather_kernel(wa, wu, wd, sm, fa, fu, fd, fs, va, vu, vd, vs, load_sem, own_sem, xy_sem, z_sem,
                  push_send, push_recv, recv_sem):
    me = lax.axis_index("fsdp")
    core, xc, yc, zc = me % 2, (me // 2) % 2, (me // 4) % 2, me // 8
    partner = me + 1 - 2 * core
    near = (me + 2 - 4 * xc, me + 4 - 8 * yc)
    up, down = me + 8, me - 8
    has_up, has_down = zc < 3, zc > 0

    def full(u, src):
        layer, piece = UNITS[u]
        if piece < 2:
            return fa.at[layer, pl.ds(2 * piece, 2), pl.ds(pl.multiple_of(32 * src, 32), 32), :]
        if piece < 4:
            return fu.at[layer, pl.ds(pl.multiple_of(32 * src + 16 * (piece - 2), 16), 16), :]
        if piece < 6:
            return fd.at[pl.ds(pl.multiple_of(4096 * layer + 128 * src + 64 * (piece - 4), 64), 64), :]
        return fs.at[pl.ds(pl.multiple_of(8 * src, 8), 8), :]

    def own(u):
        layer, piece = UNITS[u]
        if piece < 2:
            return va.at[layer, pl.ds(2 * piece, 2)]
        if piece < 4:
            return vu.at[layer, pl.ds(16 * (piece - 2), 16), :]
        if piece < 6:
            return vd.at[layer, pl.ds(64 * (piece - 4), 64), :]
        return vs

    def kind(u):
        return (UNITS[u][1] + 0) // 2

    def order(u):
        return ORDERS[UNITS[u][1] % 6]

    def tiny(u):
        return 1 if UNITS[u][1] == 6 else 0

    barrier = pltpu.get_barrier_semaphore()
    for peer in (partner,) + near:
        pl.semaphore_signal(barrier, inc=1, device_id=(peer,), device_id_type=MESH)

    @pl.when(has_up)
    def _():
        pl.semaphore_signal(barrier, inc=1, device_id=(up,), device_id_type=MESH)

    @pl.when(has_down)
    def _():
        pl.semaphore_signal(barrier, inc=1, device_id=(down,), device_id_type=MESH)

    loads = [pltpu.make_async_copy(src, dst, load_sem.at[i])
             for i, (src, dst) in enumerate(((wa, va), (wu, vu), (wd, vd), (sm, vs)))]
    for load in loads:
        load.start()
    for load in loads:
        load.wait()
    pl.semaphore_wait(barrier, 3 + has_up.astype(jnp.int32) + has_down.astype(jnp.int32))

    def remote(u, src_ref, src, send, recv, dev):
        return pltpu.make_async_remote_copy(src_ref=src_ref, dst_ref=full(u, src), send_sem=send, recv_sem=recv,
                                            device_id=(dev,), device_id_type=MESH)

    def send_z(u, src_ref, src, slot, above, below):
        if above is not None:
            @pl.when(above)
            def _():
                remote(u, src_ref, src, z_sem.at[tiny(u)], recv_sem.at[u, slot], up).start()
        if below is not None:
            @pl.when(below)
            def _():
                remote(u, src_ref, src, z_sem.at[tiny(u)], recv_sem.at[u, slot], down).start()

    def send_xy(u, src_ref, src, dim, slot):
        remote(u, src_ref, src, xy_sem.at[tiny(u)], recv_sem.at[u, slot], near[dim]).start()

    def push(u, src_ref, src):
        remote(u, src_ref, src, push_send.at[kind(u)], push_recv.at[kind(u)], partner).start()

    def column(flip_p, p):
        base = me - 8 * zc
        if flip_p:
            base = base + (near[p] - me)
        return base

    def arrived(u, src, slot):
        remote(u, full(u, src), src, xy_sem.at[tiny(u)], recv_sem.at[u, slot], me).wait_recv()
        return full(u, src)

    def stage0(u):
        col, p, q = order(u)
        mine = own(u)
        send_z(u, mine, me, zc, has_up, has_down)
        send_xy(u, mine, me, p, 4 + zc)
        send_xy(u, mine, me, q, 8)
        push(u, mine, me)
        pltpu.make_async_copy(mine, full(u, me), own_sem.at[kind(u)]).start()

    def z_arrivals(u, flips, send_p):
        col, p, q = order(u)
        for dz in (1, 2, 3):
            for step in (-1, 1):
                for flip_p in flips:
                    zs = zc + step * dz
                    src = column(flip_p, p) + 8 * zs
                    slot = 4 * flip_p + zs
                    present = (zc >= dz) if step < 0 else (zc <= 3 - dz)

                    @pl.when(present)
                    def _(src=src, slot=slot, step=step):
                        ref = arrived(u, src, slot)
                        send_z(u, ref, src, slot, has_up if step < 0 else None, has_down if step > 0 else None)
                        if send_p:
                            send_xy(u, ref, src, p, 4 + slot)
                        send_xy(u, ref, src, q, 8)
                        push(u, ref, src)

    def stage1(u):
        col, p, q = order(u)
        if col == "a":
            z_arrivals(u, (0,), True)
        else:
            src = near[p]
            ref = arrived(u, src, 4 + zc)
            send_z(u, ref, src, 4 + zc, has_up, has_down)
            send_xy(u, ref, src, q, 8)
            push(u, ref, src)

    def stage2(u):
        col, p, q = order(u)
        if col == "a":
            for hop in range(4):
                zs = lax.rem(zc + hop, 4)
                src = column(1, p) + 8 * zs
                ref = arrived(u, src, 4 + zs)
                send_xy(u, ref, src, q, 8)
                push(u, ref, src)
        else:
            z_arrivals(u, (0, 1), False)

    def stage3(u):
        col, p, q = order(u)
        rows = fs.at[pl.ds(0, 64), :] if tiny(u) else fd.at[pl.ds(0, 512), :]
        pltpu.make_async_copy(rows, rows, recv_sem.at[u, 8]).wait()
        for flip_p in (0, 1):
            base = column(flip_p, p) + (near[q] - me)

            def body(zs, carry, base=base):
                src = base + 8 * zs
                push(u, full(u, src), src)
                return carry

            lax.fori_loop(0, 4, body, 0)

    stages = (stage0, stage1, stage2, stage3)
    count = len(UNITS)
    for rnd in range(count + STAGE_LAG[3]):
        for k in range(4):
            if k == 0:
                todo = range(AHEAD + 1) if rnd == 0 else [rnd + AHEAD]
            else:
                todo = [rnd - STAGE_LAG[k]]
            for u in todo:
                if 0 <= u < count:
                    stages[k](u)

    def drain(ref, sem):
        pltpu.make_async_copy(ref, ref, sem).wait()

    per_layer = 64 * LAYERS
    drain(fd.at[pl.ds(0, 60 * per_layer), :], xy_sem.at[0])
    drain(fs.at[pl.ds(0, 9 * 8), :], xy_sem.at[1])
    ends = jnp.logical_or(zc == 0, zc == 3)

    @pl.when(ends)
    def _():
        drain(fd.at[pl.ds(0, 10 * per_layer), :], z_sem.at[0])
        drain(fs.at[pl.ds(0, 2 * 8), :], z_sem.at[1])

    @pl.when(jnp.logical_not(ends))
    def _():
        drain(fd.at[pl.ds(0, 50 * per_layer), :], z_sem.at[0])
        drain(fs.at[pl.ds(0, 10 * 8), :], z_sem.at[1])

    halves = (fa.at[0], fu.at[0], fd.at[pl.ds(0, 4096), :], fs.at[pl.ds(0, 128), :])
    for i, half in enumerate(halves):
        drain(half, push_send.at[i])
        drain(half, push_recv.at[i])
    for i, ref in enumerate((va, vu, vd, vs)):
        drain(ref, own_sem.at[i])


def gather_weights(w_attn, w_up, w_down, small):
    shapes = (w_attn.shape, w_up.shape, w_down.shape, small.shape)
    dt = jnp.bfloat16
    return pl.pallas_call(
        gather_kernel,
        out_shape=(jax.ShapeDtypeStruct((LAYERS, 4, 1024, 1024), dt), jax.ShapeDtypeStruct((LAYERS, 1024, 4096), dt),
                   jax.ShapeDtypeStruct((LAYERS * 4096, 1024), dt), jax.ShapeDtypeStruct((32 * 8, 128), dt)),
        in_specs=[pl.BlockSpec(memory_space=pltpu.HBM)] * 4,
        out_specs=[pl.BlockSpec(memory_space=pltpu.HBM)] * 4,
        scratch_shapes=[pltpu.VMEM(s, dt) for s in shapes] + [
            pltpu.SemaphoreType.DMA((4,)), pltpu.SemaphoreType.DMA((4,)), pltpu.SemaphoreType.DMA((2,)),
            pltpu.SemaphoreType.DMA((2,)), pltpu.SemaphoreType.DMA((4,)), pltpu.SemaphoreType.DMA((4,)),
            pltpu.SemaphoreType.DMA((len(UNITS), 9))],
        compiler_params=pltpu.CompilerParams(collective_id=0, has_side_effects=True),
        name="gather_weights",
    )(w_attn, w_up, w_down, small)


HEAD_DIM = 64
EPS = 1e-5
THETA = 10000.0
NEG_BIG = -1e30


def rotary_tables(seq_len):
    half_dim = HEAD_DIM // 2
    inv_freq = 1.0 / (THETA ** (jnp.arange(half_dim, dtype=jnp.float32) * (2.0 / HEAD_DIM)))
    angles = jnp.arange(seq_len, dtype=jnp.float32)[:, None] * inv_freq[None, :]
    return jnp.cos(angles)[:, None, :], jnp.sin(angles)[:, None, :]


def rotate(tensor, cos_tab, sin_tab):
    half_dim = HEAD_DIM // 2
    first_half = tensor[..., :half_dim]
    second_half = tensor[..., half_dim:]
    return jnp.concatenate([first_half * cos_tab - second_half * sin_tab, second_half * cos_tab + first_half * sin_tab], axis=-1)


def rotate_back(tensor, cos_tab, sin_tab):
    return rotate(tensor, cos_tab, -sin_tab)


def norm_fwd(x_in, gain, shift):
    row_mean = jnp.mean(x_in, axis=-1, keepdims=True)
    centered = x_in - row_mean
    variance = jnp.mean(centered * centered, axis=-1, keepdims=True)
    return centered * lax.rsqrt(variance + EPS) * gain + shift


def gelu_slope(pre_act):
    normal_cdf = 0.5 * (1.0 + lax.erf(pre_act * (1.0 / math.sqrt(2.0))))
    density = jnp.exp(-0.5 * pre_act * pre_act) * (1.0 / math.sqrt(2.0 * math.pi))
    return normal_cdf + pre_act * density


def dot(a, b):
    return jnp.dot(a, b, preferred_element_type=jnp.float32)


def dot_t(a, b):
    return lax.dot_general(a, b, (((1,), (1,)), ((), ())), preferred_element_type=jnp.float32)


def dot_g(a, b):
    return lax.dot_general(a, b, (((0,), (0,)), ((), ())), preferred_element_type=jnp.float32)


def heads(tensor):
    return tensor.reshape(tensor.shape[0], -1, HEAD_DIM)


def layer_forward(x, weights, length, tables, last):
    w_attn, w_up, w_down, b_attn, ln_par, b_up, b_down = weights
    cos_tab, sin_tab = tables
    seq_len = x.shape[0]
    x_f32 = x.astype(jnp.float32)
    h_one = norm_fwd(x_f32, ln_par[0], ln_par[1]).astype(jnp.bfloat16)
    query, key, values = (heads(dot(h_one, w_attn[i]) + b_attn[i]) for i in range(3))
    query_rot = rotate(query * (HEAD_DIM ** -0.5), cos_tab, sin_tab).astype(jnp.bfloat16)
    key_rot = rotate(key, cos_tab, sin_tab).astype(jnp.bfloat16)
    values = values.astype(jnp.bfloat16)
    scores = jnp.einsum('qhd,khd->hqk', query_rot, key_rot, preferred_element_type=jnp.float32)
    key_valid = jnp.arange(seq_len)[None, None, :] < length
    probs_bf = jax.nn.softmax(jnp.where(key_valid, scores, NEG_BIG), axis=-1).astype(jnp.bfloat16)
    context = jnp.einsum('hqk,khd->qhd', probs_bf, values, preferred_element_type=jnp.float32)
    context = context.astype(jnp.bfloat16).reshape(seq_len, -1)
    x_mid = (x_f32 + dot(context, w_attn[3]) + b_attn[3]).astype(jnp.bfloat16)
    mid_f32 = x_mid.astype(jnp.float32)
    h_two = norm_fwd(mid_f32, ln_par[2], ln_par[3]).astype(jnp.bfloat16)
    pre_act = dot(h_two, w_up) + b_up
    act_bf = jax.nn.gelu(pre_act, approximate=False).astype(jnp.bfloat16)
    y_out = None
    if not last:
        y_out = (mid_f32 + dot(act_bf, w_down) + b_down).astype(jnp.bfloat16)
    return y_out, (x, h_one, query_rot, key_rot, values, probs_bf, context, x_mid, h_two, pre_act, act_bf)


def layer_backward(d_out, saved_acts, weights, tables):
    w_attn, w_up, w_down, b_attn, ln_par, b_up, b_down = weights
    cos_tab, sin_tab = tables
    x, h_one, query_rot, key_rot, values, probs_bf, context, x_mid, h_two, pre_act, act_bf = saved_acts
    seq_len = x.shape[0]
    gb_down = jnp.sum(d_out, axis=0, dtype=jnp.float32)
    d_pre = dot_t(d_out, w_down) * gelu_slope(pre_act)
    gb_up = jnp.sum(d_pre, axis=0)
    d_pre_bf = d_pre.astype(jnp.bfloat16)
    d_h_two = dot_t(d_pre_bf, w_up)
    _, norm_pull_two = jax.vjp(norm_fwd, x_mid.astype(jnp.float32), ln_par[2], ln_par[3])
    d_mid_norm, g_gain_two, g_shift_two = norm_pull_two(d_h_two)
    d_mid = (d_out.astype(jnp.float32) + d_mid_norm).astype(jnp.bfloat16)
    gb_out = jnp.sum(d_mid, axis=0, dtype=jnp.float32)
    d_context = heads(dot_t(d_mid, w_attn[3]).astype(jnp.bfloat16))
    d_probs = jnp.einsum('qhd,khd->hqk', d_context, values, preferred_element_type=jnp.float32)
    d_values = jnp.einsum('hqk,qhd->khd', probs_bf, d_context, preferred_element_type=jnp.float32)
    probs_f32 = probs_bf.astype(jnp.float32)
    d_scores = (probs_f32 * (d_probs - jnp.sum(d_probs * probs_f32, axis=-1, keepdims=True))).astype(jnp.bfloat16)
    d_query = jnp.einsum('hqk,khd->qhd', d_scores, key_rot, preferred_element_type=jnp.float32)
    d_key = jnp.einsum('hqk,qhd->khd', d_scores, query_rot, preferred_element_type=jnp.float32)
    d_proj = jnp.concatenate([
        (rotate_back(d_query, cos_tab, sin_tab) * (HEAD_DIM ** -0.5)).astype(jnp.bfloat16).reshape(seq_len, -1),
        rotate_back(d_key, cos_tab, sin_tab).astype(jnp.bfloat16).reshape(seq_len, -1),
        d_values.astype(jnp.bfloat16).reshape(seq_len, -1)], axis=1)
    gb_qkv = jnp.sum(d_proj, axis=0, dtype=jnp.float32)
    d_h_one = sum(dot_t(d_proj[:, 1024 * i:1024 * i + 1024], w_attn[i]) for i in range(3))
    _, norm_pull_one = jax.vjp(norm_fwd, x.astype(jnp.float32), ln_par[0], ln_par[1])
    d_x_norm, g_gain_one, g_shift_one = norm_pull_one(d_h_one)
    d_x = (d_mid.astype(jnp.float32) + d_x_norm).astype(jnp.bfloat16)
    small = (jnp.concatenate([gb_qkv, gb_out]).reshape(4, -1),
             jnp.stack([g_gain_one, g_shift_one, g_gain_two, g_shift_two]), gb_up, gb_down)
    return d_x, (h_one, context, h_two, act_bf, d_proj, d_mid, d_pre_bf, d_out), small


def pack_small(b_attn, ln_par, b_up, b_down):
    rows = [b_attn.reshape(2, 128), ln_par.reshape(2, 128), b_up, jnp.pad(b_down, ((0, 0), (0, 96)))]
    return jnp.stack(rows, axis=1).reshape(8, 128)


def unpack_small(gathered):
    rows = gathered.reshape(32, 2, 4, 128).astype(jnp.float32)

    def fours(row):
        return row.reshape(32, 4, 32).transpose(1, 0, 2).reshape(4, 1024)

    return [(fours(rows[:, l, 0]), fours(rows[:, l, 1]), rows[:, l, 2].reshape(4096), rows[:, l, 3, :32].reshape(1024))
            for l in range(2)]


def solution(mesh):
    axis_name = mesh.axis_names[0]
    batch_spec = P(axis_name)
    weight_specs = (P(None, None, axis_name, None), P(None, None, axis_name), P(None, None, axis_name),
                    P(None, axis_name, None), P(None, axis_name), P(None, axis_name, None), P(None, axis_name))

    def device_step(x, lengths, d_y, w_attn, b_attn, ln_par, w_up, b_up, w_down, b_down):
        tables = rotary_tables(x.shape[1])
        fa, fu, fd, fs = gather_weights(w_attn, w_up, w_down, pack_small(b_attn, ln_par, b_up, b_down))
        smalls = unpack_small(fs)
        weights = [(fa[l], fu[l], fd[4096 * l:4096 * l + 4096]) + smalls[l] for l in range(2)]
        hidden, saved = x[0], []
        for l in range(2):
            hidden, acts = layer_forward(hidden, weights[l], lengths[0], tables, l == 1)
            saved.append(acts)
        grad, big, tiny = d_y[0], [None] * 2, [None] * 2
        scatter = functools.partial(lax.psum_scatter, axis_name=axis_name, scatter_dimension=0, tiled=True)
        for l in (1, 0):
            grad, (h1, ctx, h2, act, d_proj, d_mid, d_pre, d_out), small = layer_backward(grad, saved[l], weights[l], tables)
            g_qkv = scatter(dot_g(h1, d_proj))
            g_o = scatter(dot_g(ctx, d_mid))
            big[l] = (jnp.stack([g_qkv[:, :1024], g_qkv[:, 1024:2048], g_qkv[:, 2048:], g_o]),
                      scatter(dot_g(h2, d_pre)), scatter(dot_g(act, d_out)))
            gb, gl, gu, gd = small
            tiny[l] = jnp.concatenate([gb.reshape(4, 32, 32).transpose(1, 0, 2).reshape(32, 128),
                                       gl.reshape(4, 32, 32).transpose(1, 0, 2).reshape(32, 128),
                                       gu.reshape(32, 128), gd.reshape(32, 32)], axis=1)
        tiny = scatter(jnp.concatenate(tiny, axis=1)).reshape(2, 416)
        return (grad[None], jnp.stack([big[0][0], big[1][0]]), tiny[:, :128].reshape(2, 4, 32),
                tiny[:, 128:256].reshape(2, 4, 32), jnp.stack([big[0][1], big[1][1]]), tiny[:, 256:384],
                jnp.stack([big[0][2], big[1][2]]), tiny[:, 384:])

    return jax.shard_map(device_step, mesh=mesh,
                         in_specs=(batch_spec, batch_spec, batch_spec) + weight_specs,
                         out_specs=(batch_spec,) + weight_specs,
                         check_vma=False)
```

```python
import functools
import math
import jax
import jax.numpy as jnp
from jax import lax
from jax.experimental import pallas as pl
from jax.experimental.pallas import tpu as pltpu
from jax.sharding import PartitionSpec as P

LINE = 4
PLANE = 8
HEADS = 16
SHARD = 32
HEAD_DIM = 64
HALF_SEQ = 96
TILE = 128
SEQ = 192
SPREAD = 224
BAND = 256
WIDE = 512
DIM = 1024
FAR = 1344
FFN = 4096

MESH = pl.DeviceIdType.MESH
LAYERS = 2
ORDERS = (("b", 0, 1), ("b", 1, 0), ("a", 0, 1), ("a", 1, 0), ("b", 0, 1), ("b", 1, 0))
UNITS = [(layer, piece) for layer in range(LAYERS) for piece in range(6)] + [(0, 6)]
STAGE_LAG = (0, 0, 1, 3)
AHEAD = 2


def gather_kernel(wa, wu, wd, sm, fa, fu, fd, fs, va, vu, vd, vs, load_sem, own_sem, xy_sem, z_sem,
                  push_send, push_recv, recv_sem):
    me = lax.axis_index("fsdp")
    core, xc, yc, zc = me % 2, (me // 2) % 2, (me // LINE) % 2, me // PLANE
    partner = me + 1 - 2 * core
    near = (me + 2 - LINE * xc, me + LINE - PLANE * yc)
    up, down = me + PLANE, me - PLANE
    has_up, has_down = zc < 3, zc > 0

    def full(u, src):
        layer, piece = UNITS[u]
        if piece < 2:
            return fa.at[layer, pl.ds(2 * piece, 2), pl.ds(pl.multiple_of(SHARD * src, SHARD), SHARD), :]
        if piece < LINE:
            return fu.at[layer, pl.ds(pl.multiple_of(SHARD * src + HEADS * (piece - 2), HEADS), HEADS), :]
        if piece < 6:
            return fd.at[pl.ds(pl.multiple_of(FFN * layer + TILE * src + HEAD_DIM * (piece - LINE), HEAD_DIM), HEAD_DIM), :]
        return fs.at[pl.ds(pl.multiple_of(PLANE * src, PLANE), PLANE), :]

    def own(u):
        layer, piece = UNITS[u]
        if piece < 2:
            return va.at[layer, pl.ds(2 * piece, 2)]
        if piece < LINE:
            return vu.at[layer, pl.ds(HEADS * (piece - 2), HEADS), :]
        if piece < 6:
            return vd.at[layer, pl.ds(HEAD_DIM * (piece - LINE), HEAD_DIM), :]
        return vs

    def kind(u):
        return (UNITS[u][1] + 0) // 2

    def order(u):
        return ORDERS[UNITS[u][1] % 6]

    def tiny(u):
        return 1 if UNITS[u][1] == 6 else 0

    barrier = pltpu.get_barrier_semaphore()
    for peer in (partner,) + near:
        pl.semaphore_signal(barrier, inc=1, device_id=(peer,), device_id_type=MESH)

    @pl.when(has_up)
    def _():
        pl.semaphore_signal(barrier, inc=1, device_id=(up,), device_id_type=MESH)

    @pl.when(has_down)
    def _():
        pl.semaphore_signal(barrier, inc=1, device_id=(down,), device_id_type=MESH)

    loads = [pltpu.make_async_copy(src, dst, load_sem.at[i])
             for i, (src, dst) in enumerate(((wa, va), (wu, vu), (wd, vd), (sm, vs)))]
    for load in loads:
        load.start()
    for load in loads:
        load.wait()
    pl.semaphore_wait(barrier, 3 + has_up.astype(jnp.int32) + has_down.astype(jnp.int32))

    def remote(u, src_ref, src, send, recv, dev):
        return pltpu.make_async_remote_copy(src_ref=src_ref, dst_ref=full(u, src), send_sem=send, recv_sem=recv,
                                            device_id=(dev,), device_id_type=MESH)

    def send_z(u, src_ref, src, slot, above, below):
        if above is not None:
            @pl.when(above)
            def _():
                remote(u, src_ref, src, z_sem.at[tiny(u)], recv_sem.at[u, slot], up).start()
        if below is not None:
            @pl.when(below)
            def _():
                remote(u, src_ref, src, z_sem.at[tiny(u)], recv_sem.at[u, slot], down).start()

    def send_xy(u, src_ref, src, dim, slot):
        remote(u, src_ref, src, xy_sem.at[tiny(u)], recv_sem.at[u, slot], near[dim]).start()

    def push(u, src_ref, src):
        remote(u, src_ref, src, push_send.at[kind(u)], push_recv.at[kind(u)], partner).start()

    def column(flip_p, p):
        base = me - PLANE * zc
        if flip_p:
            base = base + (near[p] - me)
        return base

    def arrived(u, src, slot):
        remote(u, full(u, src), src, xy_sem.at[tiny(u)], recv_sem.at[u, slot], me).wait_recv()
        return full(u, src)

    def stage0(u):
        col, p, q = order(u)
        mine = own(u)
        send_z(u, mine, me, zc, has_up, has_down)
        send_xy(u, mine, me, p, LINE + zc)
        send_xy(u, mine, me, q, PLANE)
        push(u, mine, me)
        pltpu.make_async_copy(mine, full(u, me), own_sem.at[kind(u)]).start()

    def z_arrivals(u, flips, send_p):
        col, p, q = order(u)
        for dz in (1, 2, 3):
            for step in (-1, 1):
                for flip_p in flips:
                    zs = zc + step * dz
                    src = column(flip_p, p) + PLANE * zs
                    slot = LINE * flip_p + zs
                    present = (zc >= dz) if step < 0 else (zc <= 3 - dz)

                    @pl.when(present)
                    def _(src=src, slot=slot, step=step):
                        ref = arrived(u, src, slot)
                        send_z(u, ref, src, slot, has_up if step < 0 else None, has_down if step > 0 else None)
                        if send_p:
                            send_xy(u, ref, src, p, LINE + slot)
                        send_xy(u, ref, src, q, PLANE)
                        push(u, ref, src)

    def stage1(u):
        col, p, q = order(u)
        if col == "a":
            z_arrivals(u, (0,), True)
        else:
            src = near[p]
            ref = arrived(u, src, LINE + zc)
            send_z(u, ref, src, LINE + zc, has_up, has_down)
            send_xy(u, ref, src, q, PLANE)
            push(u, ref, src)

    def stage2(u):
        col, p, q = order(u)
        if col == "a":
            for hop in range(LINE):
                zs = lax.rem(zc + hop, LINE)
                src = column(1, p) + PLANE * zs
                ref = arrived(u, src, LINE + zs)
                send_xy(u, ref, src, q, PLANE)
                push(u, ref, src)
        else:
            z_arrivals(u, (0, 1), False)

    def stage3(u):
        col, p, q = order(u)
        rows = fs.at[pl.ds(0, HEAD_DIM), :] if tiny(u) else fd.at[pl.ds(0, WIDE), :]
        pltpu.make_async_copy(rows, rows, recv_sem.at[u, PLANE]).wait()
        for flip_p in (0, 1):
            base = column(flip_p, p) + (near[q] - me)

            def body(zs, carry, base=base):
                src = base + PLANE * zs
                push(u, full(u, src), src)
                return carry

            lax.fori_loop(0, LINE, body, 0)

    stages = (stage0, stage1, stage2, stage3)
    count = len(UNITS)
    for rnd in range(count + STAGE_LAG[3]):
        for k in range(LINE):
            if k == 0:
                todo = range(AHEAD + 1) if rnd == 0 else [rnd + AHEAD]
            else:
                todo = [rnd - STAGE_LAG[k]]
            for u in todo:
                if 0 <= u < count:
                    stages[k](u)

    def drain(ref, sem):
        pltpu.make_async_copy(ref, ref, sem).wait()

    per_layer = HEAD_DIM * LAYERS
    drain(fd.at[pl.ds(0, 60 * per_layer), :], xy_sem.at[0])
    drain(fs.at[pl.ds(0, 9 * PLANE), :], xy_sem.at[1])
    ends = jnp.logical_or(zc == 0, zc == 3)

    @pl.when(ends)
    def _():
        drain(fd.at[pl.ds(0, 10 * per_layer), :], z_sem.at[0])
        drain(fs.at[pl.ds(0, 2 * PLANE), :], z_sem.at[1])

    @pl.when(jnp.logical_not(ends))
    def _():
        drain(fd.at[pl.ds(0, 50 * per_layer), :], z_sem.at[0])
        drain(fs.at[pl.ds(0, 10 * PLANE), :], z_sem.at[1])

    halves = (fa.at[0], fu.at[0], fd.at[pl.ds(0, FFN), :], fs.at[pl.ds(0, TILE), :])
    for i, half in enumerate(halves):
        drain(half, push_send.at[i])
        drain(half, push_recv.at[i])
    for i, ref in enumerate((va, vu, vd, vs)):
        drain(ref, own_sem.at[i])


def gather_weights(w_attn, w_up, w_down, small):
    shapes = (w_attn.shape, w_up.shape, w_down.shape, small.shape)
    dt = jnp.bfloat16
    return pl.pallas_call(
        gather_kernel,
        out_shape=(jax.ShapeDtypeStruct((LAYERS, LINE, DIM, DIM), dt), jax.ShapeDtypeStruct((LAYERS, DIM, FFN), dt),
                   jax.ShapeDtypeStruct((LAYERS * FFN, DIM), dt), jax.ShapeDtypeStruct((SHARD * PLANE, TILE), dt)),
        in_specs=[pl.BlockSpec(memory_space=pltpu.HBM)] * LINE,
        out_specs=[pl.BlockSpec(memory_space=pltpu.HBM)] * LINE,
        scratch_shapes=[pltpu.VMEM(s, dt) for s in shapes] + [
            pltpu.SemaphoreType.DMA((LINE,)), pltpu.SemaphoreType.DMA((LINE,)), pltpu.SemaphoreType.DMA((2,)),
            pltpu.SemaphoreType.DMA((2,)), pltpu.SemaphoreType.DMA((LINE,)), pltpu.SemaphoreType.DMA((LINE,)),
            pltpu.SemaphoreType.DMA((len(UNITS), 9))],
        compiler_params=pltpu.CompilerParams(collective_id=0, has_side_effects=True),
        name="gather_weights",
    )(w_attn, w_up, w_down, small)


EPS = 1e-5
THETA = 10000.0
NEG_BIG = -1e30


def rotary_tables(seq_len):
    half_dim = HEAD_DIM // 2
    inv_freq = 1.0 / (THETA ** (jnp.arange(half_dim, dtype=jnp.float32) * (2.0 / HEAD_DIM)))
    angles = jnp.arange(seq_len, dtype=jnp.float32)[:, None] * inv_freq[None, :]
    return jnp.cos(angles)[:, None, :], jnp.sin(angles)[:, None, :]


def rotate(tensor, cos_tab, sin_tab):
    half_dim = HEAD_DIM // 2
    first_half = tensor[..., :half_dim]
    second_half = tensor[..., half_dim:]
    return jnp.concatenate([first_half * cos_tab - second_half * sin_tab, second_half * cos_tab + first_half * sin_tab], axis=-1)


def rotate_back(tensor, cos_tab, sin_tab):
    return rotate(tensor, cos_tab, -sin_tab)


def norm_fwd(x_in, gain, shift):
    row_mean = jnp.mean(x_in, axis=-1, keepdims=True)
    centered = x_in - row_mean
    variance = jnp.mean(centered * centered, axis=-1, keepdims=True)
    return centered * lax.rsqrt(variance + EPS) * gain + shift


def gelu_slope(pre_act):
    normal_cdf = 0.5 * (1.0 + lax.erf(pre_act * (1.0 / math.sqrt(2.0))))
    density = jnp.exp(-0.5 * pre_act * pre_act) * (1.0 / math.sqrt(2.0 * math.pi))
    return normal_cdf + pre_act * density


def dot(a, b):
    return jnp.dot(a, b, preferred_element_type=jnp.float32)


def dot_t(a, b):
    return lax.dot_general(a, b, (((1,), (1,)), ((), ())), preferred_element_type=jnp.float32)


def dot_g(a, b):
    return lax.dot_general(a, b, (((0,), (0,)), ((), ())), preferred_element_type=jnp.float32)


def heads(tensor):
    return tensor.reshape(tensor.shape[0], -1, HEAD_DIM)


def layer_forward(x, weights, length, tables, last):
    w_attn, w_up, w_down, b_attn, ln_par, b_up, b_down = weights
    cos_tab, sin_tab = tables
    seq_len = x.shape[0]
    x_f32 = x.astype(jnp.float32)
    h_one = norm_fwd(x_f32, ln_par[0], ln_par[1]).astype(jnp.bfloat16)
    query, key, values = (heads(dot(h_one, w_attn[i]) + b_attn[i]) for i in range(3))
    query_rot = rotate(query * (HEAD_DIM ** -0.5), cos_tab, sin_tab).astype(jnp.bfloat16)
    key_rot = rotate(key, cos_tab, sin_tab).astype(jnp.bfloat16)
    values = values.astype(jnp.bfloat16)
    scores = jnp.einsum('qhd,khd->hqk', query_rot, key_rot, preferred_element_type=jnp.float32)
    key_valid = jnp.arange(seq_len)[None, None, :] < length
    probs_bf = jax.nn.softmax(jnp.where(key_valid, scores, NEG_BIG), axis=-1).astype(jnp.bfloat16)
    context = jnp.einsum('hqk,khd->qhd', probs_bf, values, preferred_element_type=jnp.float32)
    context = context.astype(jnp.bfloat16).reshape(seq_len, -1)
    x_mid = (x_f32 + dot(context, w_attn[3]) + b_attn[3]).astype(jnp.bfloat16)
    mid_f32 = x_mid.astype(jnp.float32)
    h_two = norm_fwd(mid_f32, ln_par[2], ln_par[3]).astype(jnp.bfloat16)
    pre_act = dot(h_two, w_up) + b_up
    act_bf = jax.nn.gelu(pre_act, approximate=False).astype(jnp.bfloat16)
    y_out = None
    if not last:
        y_out = (mid_f32 + dot(act_bf, w_down) + b_down).astype(jnp.bfloat16)
    return y_out, (x, h_one, query_rot, key_rot, values, probs_bf, context, x_mid, h_two, pre_act, act_bf)


def layer_backward(d_out, saved_acts, weights, tables):
    w_attn, w_up, w_down, b_attn, ln_par, b_up, b_down = weights
    cos_tab, sin_tab = tables
    x, h_one, query_rot, key_rot, values, probs_bf, context, x_mid, h_two, pre_act, act_bf = saved_acts
    seq_len = x.shape[0]
    gb_down = jnp.sum(d_out, axis=0, dtype=jnp.float32)
    d_pre = dot_t(d_out, w_down) * gelu_slope(pre_act)
    gb_up = jnp.sum(d_pre, axis=0)
    d_pre_bf = d_pre.astype(jnp.bfloat16)
    d_h_two = dot_t(d_pre_bf, w_up)
    _, norm_pull_two = jax.vjp(norm_fwd, x_mid.astype(jnp.float32), ln_par[2], ln_par[3])
    d_mid_norm, g_gain_two, g_shift_two = norm_pull_two(d_h_two)
    d_mid = (d_out.astype(jnp.float32) + d_mid_norm).astype(jnp.bfloat16)
    gb_out = jnp.sum(d_mid, axis=0, dtype=jnp.float32)
    d_context = heads(dot_t(d_mid, w_attn[3]).astype(jnp.bfloat16))
    d_probs = jnp.einsum('qhd,khd->hqk', d_context, values, preferred_element_type=jnp.float32)
    d_values = jnp.einsum('hqk,qhd->khd', probs_bf, d_context, preferred_element_type=jnp.float32)
    probs_f32 = probs_bf.astype(jnp.float32)
    d_scores = (probs_f32 * (d_probs - jnp.sum(d_probs * probs_f32, axis=-1, keepdims=True))).astype(jnp.bfloat16)
    d_query = jnp.einsum('hqk,khd->qhd', d_scores, key_rot, preferred_element_type=jnp.float32)
    d_key = jnp.einsum('hqk,qhd->khd', d_scores, query_rot, preferred_element_type=jnp.float32)
    d_proj = jnp.concatenate([
        (rotate_back(d_query, cos_tab, sin_tab) * (HEAD_DIM ** -0.5)).astype(jnp.bfloat16).reshape(seq_len, -1),
        rotate_back(d_key, cos_tab, sin_tab).astype(jnp.bfloat16).reshape(seq_len, -1),
        d_values.astype(jnp.bfloat16).reshape(seq_len, -1)], axis=1)
    gb_qkv = jnp.sum(d_proj, axis=0, dtype=jnp.float32)
    d_h_one = sum(dot_t(d_proj[:, DIM * i:DIM * i + DIM], w_attn[i]) for i in range(3))
    _, norm_pull_one = jax.vjp(norm_fwd, x.astype(jnp.float32), ln_par[0], ln_par[1])
    d_x_norm, g_gain_one, g_shift_one = norm_pull_one(d_h_one)
    d_x = (d_mid.astype(jnp.float32) + d_x_norm).astype(jnp.bfloat16)
    small = (jnp.concatenate([gb_qkv, gb_out]).reshape(LINE, -1),
             jnp.stack([g_gain_one, g_shift_one, g_gain_two, g_shift_two]), gb_up, gb_down)
    return d_x, (h_one, context, h_two, act_bf, d_proj, d_mid, d_pre_bf, d_out), small


def pack_small(b_attn, ln_par, b_up, b_down):
    rows = [b_attn.reshape(2, TILE), ln_par.reshape(2, TILE), b_up, jnp.pad(b_down, ((0, 0), (0, HALF_SEQ)))]
    return jnp.stack(rows, axis=1).reshape(PLANE, TILE)


def unpack_small(gathered):
    rows = gathered.reshape(SHARD, 2, LINE, TILE).astype(jnp.float32)

    def fours(row):
        return row.reshape(SHARD, LINE, SHARD).transpose(1, 0, 2).reshape(LINE, DIM)

    return [(fours(rows[:, l, 0]), fours(rows[:, l, 1]), rows[:, l, 2].reshape(FFN), rows[:, l, 3, :SHARD].reshape(DIM))
            for l in range(2)]


PIECES = [(layer, name) for layer in (1, 0) for name in "DUOQ"]
WIDTH = {"D": WIDE, "U": WIDE, "O": TILE, "Q": 384}
ROWS = SEQ
LAG = (1, 2, 3)


def acc_shape(name):
    return (WIDE, DIM) if name == "D" else (DIM, WIDTH[name])


def grad_kernel(*refs):
    n = len(PIECES)
    bc_in, sl_in, sums = refs[:n], refs[n:2 * n], refs[2 * n]
    refs = refs[2 * n + 1:]
    g_attn, g_up, g_down, g_small, bc_far = refs[:5]
    sl_far = refs[5:5 + n]
    refs = refs[5 + n:]
    bc_v, sl_v = refs[:2]
    acc, got = refs[2:2 + n], refs[2 + n:2 + 2 * n]
    sum_v, sum_got, sum_line = refs[2 + 2 * n:5 + 2 * n]
    (bc_send, bc_recv, push_send, push_recv, sl_send, sl_recv, load_sem, rs_send, rs_recv, out_send, out_recv, own_sem,
     sum_send, sum_recv) = refs[5 + 2 * n:]

    me = lax.axis_index("fsdp")
    core, xc, yc, zc = me % 2, (me // 2) % 2, (me // LINE) % 2, me // PLANE
    place = me % PLANE

    def peer(r):
        out = me
        if r & 1:
            out = out + 1 - 2 * core
        if r & 2:
            out = out + 2 - LINE * xc
        if r & LINE:
            out = out + LINE - PLANE * yc
        return out

    def line(k):
        return place + PLANE * lax.rem(zc + k, LINE)

    def remote(src, dst, send, recv, dev):
        return pltpu.make_async_remote_copy(src_ref=src, dst_ref=dst, send_sem=send, recv_sem=recv,
                                            device_id=(dev,), device_id_type=MESH)

    def local(src, dst, sem):
        return pltpu.make_async_copy(src, dst, sem)

    def drain(ref, sem):
        local(ref, ref, sem).wait()

    barrier = pltpu.get_barrier_semaphore()
    for r in range(1, PLANE):
        pl.semaphore_signal(barrier, inc=1, device_id=(peer(r),), device_id_type=MESH)
    for k in range(1, LINE):
        pl.semaphore_signal(barrier, inc=1, device_id=(line(k),), device_id_type=MESH)
    local(sums, sum_v, load_sem.at[0]).start()
    drain(sum_v, load_sem.at[0])
    pl.semaphore_wait(barrier, 10)

    def far(u, r, half=None):
        start = FAR * u + SEQ * (r - 1)
        return bc_far.at[pl.ds(start, SEQ), :] if half is None else bc_far.at[pl.ds(start + HALF_SEQ * half, HALF_SEQ), :]

    def blocks(u, where):
        name = PIECES[u][1]
        if name == "D":
            return [(pl.multiple_of(DIM * i + TILE * where, TILE), TILE * i, TILE) for i in range(LINE)]
        if name == "Q":
            return [(pl.multiple_of(DIM * i + TILE * where, TILE), TILE * i, TILE) for i in range(3)]
        return [(pl.multiple_of(WIDTH[name] * where, TILE), 0, WIDTH[name])]

    def send_bc(u):
        for r in (2, LINE):
            for half in (0, 1):
                slot = (0 if r == 2 else 2) + half
                remote(bc_in[u].at[pl.ds(HALF_SEQ * half, HALF_SEQ), :], far(u, r, half), bc_send, bc_recv.at[u, slot], peer(r)).start()
        remote(bc_in[u], far(u, 1), push_send, push_recv.at[u], peer(1)).start()

    def send_sl(u):
        for r in (2, 6, LINE, 3, 7, 5, 1):
            for src, dst, width in blocks(u, peer(r) % PLANE):
                remote(sl_in[u].at[:, pl.ds(src, width)], sl_far[u].at[pl.ds(SEQ * (r - 1), SEQ), pl.ds(dst, width)],
                       sl_send.at[u], sl_recv.at[u], peer(r)).start()

    def push(u, r, half):
        remote(far(u, r, half), far(u, r + 1, half), push_send, push_recv.at[u], peer(1)).start()

    def relay_bc(u):
        for slot, r, half, onward in ((0, 2, 0, LINE), (3, LINE, 1, 2), (1, 2, 1, None), (2, LINE, 0, None)):
            drain(far(u, r, half), bc_recv.at[u, slot])
            if onward is not None:
                remote(far(u, r, half), far(u, 6, half), bc_send, bc_recv.at[u, LINE + half], peer(onward)).start()
            push(u, r, half)

    def collect(u):
        name = PIECES[u][1]
        own = [local(bc_in[u], bc_v.at[pl.ds(0, SEQ), :], load_sem.at[0])]
        for i, (src, dst, width) in enumerate(blocks(u, place)):
            own.append(local(sl_in[u].at[:, pl.ds(src, width)], sl_v.at[pl.ds(0, SEQ), pl.ds(dst, width)],
                             load_sem.at[1 + i]))
        for c in own:
            c.start()
        for half in (0, 1):
            drain(far(u, 6, half), bc_recv.at[u, LINE + half])
            push(u, 6, half)
        drain(sl_far[u], sl_recv.at[u])
        drain(bc_far.at[pl.ds(0, 768), :], push_recv.at[u])
        rest = [local(bc_far.at[pl.ds(FAR * u, FAR), :], bc_v.at[pl.ds(SEQ, FAR), :], load_sem.at[5]),
                local(sl_far[u], sl_v.at[pl.ds(SEQ, FAR), pl.ds(0, WIDTH[name])], load_sem.at[6])]
        for c in rest:
            c.start()
        for c in own + rest:
            c.wait()

    def piece_rows(u):
        return acc_shape(PIECES[u][1])[0] // LINE

    def piece(ref, u, d):
        pr = piece_rows(u)
        return ref.at[pl.ds(pl.multiple_of(pr * d, pr), pr), :]

    def step_down_line(u, d, up):
        side = jnp.where(up, 0, 1)
        dst = got[u].at[side, pl.ds(pl.multiple_of(piece_rows(u) * d, piece_rows(u)), piece_rows(u)), :]
        remote(piece(acc[u], u, d), dst, rs_send.at[u], rs_recv.at[u, side, d], me + jnp.where(up, PLANE, -PLANE)).start()

    def add_piece(u, side, d):
        pr = piece_rows(u)
        drain(piece(acc[u], u, d), rs_recv.at[u, side, d])
        rows = SHARD

        def body(i, carry):
            at = pl.ds(pl.multiple_of(pr * d + rows * i, rows), rows)
            acc[u][at, :] = acc[u][at, :] + got[u][side, at, :]
            return carry

        lax.fori_loop(0, pr // rows, body, 0)

    def product(u):
        name = PIECES[u][1]
        pr, width = piece_rows(u), WIDTH[name]

        def body(d, carry):
            at = pl.ds(pl.multiple_of(pr * d, pr), pr)
            if name == "D":
                lhs, rhs = sl_v[:, at], bc_v[...]
            else:
                lhs, rhs = bc_v[:, at], sl_v[:, pl.ds(0, width)]
            acc[u][at, :] = lax.dot_general(lhs, rhs, (((0,), (0,)), ((), ())), preferred_element_type=jnp.float32)
            return carry

        lax.fori_loop(0, LINE, body, 0)

        @pl.when(jnp.logical_or(zc == 0, zc == 3))
        def _():
            for hop in range(3):
                step_down_line(u, jnp.where(zc == 0, 3 - hop, hop), zc == 0)

    def second_hop(u):
        @pl.when(jnp.logical_or(zc == 1, zc == 2))
        def _():
            for hop in range(2):
                d = jnp.where(zc == 1, 3 - hop, hop)
                add_piece(u, jnp.where(zc == 1, 0, 1), d)
                step_down_line(u, d, zc == 1)

    def third_hop(u):
        @pl.when(jnp.logical_or(zc == 1, zc == 2))
        def _():
            d = jnp.where(zc == 1, 0, 3)
            add_piece(u, jnp.where(zc == 1, 1, 0), d)
            step_down_line(u, d, zc == 2)

    def finish(u):
        layer, name = PIECES[u]

        @pl.when(zc > 0)
        def _():
            add_piece(u, 0, zc)

        @pl.when(zc < 3)
        def _():
            add_piece(u, 1, zc)

        if name == "D":
            local(piece(acc[u], u, zc), g_down.at[layer], own_sem.at[u]).start()
            return
        for r in range(PLANE):
            at = pl.ds(pl.multiple_of(BAND * zc + SHARD * (peer(r) % PLANE), SHARD), SHARD)
            if name == "U":
                pairs = [(acc[u].at[at, :], g_up.at[layer, :, pl.ds(pl.multiple_of(WIDE * place, WIDE), WIDE)])]
            else:
                mats = (3,) if name == "O" else (0, 1, 2)
                pairs = [(acc[u].at[at, pl.ds(TILE * i, TILE)],
                          g_attn.at[layer, m, :, pl.ds(pl.multiple_of(TILE * place, TILE), TILE)]) for i, m in enumerate(mats)]
            for src, dst in pairs:
                if r == 0:
                    local(src, dst, own_sem.at[u]).start()
                else:
                    remote(src, dst, out_send.at[u], out_recv.at[u], peer(r)).start()

    def sums_plane():
        for r in range(1, PLANE):
            remote(sum_v.at[pl.ds(pl.multiple_of(SHARD * (peer(r) % PLANE), SHARD), SHARD), :], sum_got.at[pl.ds(SHARD * (r - 1), SHARD), :],
                   sum_send.at[0], sum_recv.at[0], peer(r)).start()

    def sums_line():
        drain(sum_got, sum_recv.at[0])
        total = sum_v[pl.ds(pl.multiple_of(SHARD * place, SHARD), SHARD), :]
        for r in range(1, PLANE):
            total = total + sum_got[pl.ds(SHARD * (r - 1), SHARD), :]
        sum_line[pl.ds(0, SHARD), :] = total
        for k in range(1, LINE):
            remote(sum_line.at[pl.ds(pl.multiple_of(PLANE * lax.rem(zc + k, LINE), PLANE), PLANE), :],
                   sum_line.at[pl.ds(SHARD + PLANE * (k - 1), PLANE), :], sum_send.at[1], sum_recv.at[1], line(k)).start()

    def sums_end():
        drain(sum_line.at[pl.ds(0, 24), :], sum_recv.at[1])
        total = sum_line[pl.ds(pl.multiple_of(PLANE * zc, PLANE), PLANE), :]
        for k in range(1, LINE):
            total = total + sum_line[pl.ds(SHARD + PLANE * (k - 1), PLANE), :]
        g_small[...] = total

    send_bc(0)
    relay_bc(0)
    send_sl(0)
    sums_plane()
    send_bc(1)
    for s in range(n + LAG[2]):
        if s < n:
            if s + 1 < n:
                relay_bc(s + 1)
                send_sl(s + 1)
            if s + 2 < n:
                send_bc(s + 2)
            collect(s)
            product(s)
        for lag, hop in zip(LAG, (second_hop, third_hop, finish)):
            if 0 <= s - lag < n:
                hop(s - lag)
        if s == 0:
            sums_line()
        if s == 1:
            sums_end()

    drain(bc_far.at[pl.ds(0, n * 576), :], bc_send)
    drain(bc_far.at[pl.ds(0, n * 768), :], push_send)
    drain(sum_got, sum_send.at[0])
    drain(sum_line.at[pl.ds(0, 24), :], sum_send.at[1])
    for u in range(n):
        name = PIECES[u][1]
        drain(sl_far[u], sl_send.at[u])
        drain(acc[u].at[pl.ds(0, 3 * piece_rows(u)), :], rs_send.at[u])
        if name == "D":
            drain(acc[u].at[pl.ds(0, TILE), :], own_sem.at[u])
        else:
            drain(acc[u].at[pl.ds(0, SHARD), :], own_sem.at[u])
            drain(acc[u].at[pl.ds(0, SPREAD), :], out_send.at[u])
            drain(acc[u].at[pl.ds(0, SPREAD), :], out_recv.at[u])


def reduce_grads(bc, sl, sums):
    n = len(PIECES)
    f32, bf16, dma = jnp.float32, jnp.bfloat16, pltpu.SemaphoreType.DMA
    hbm = pl.BlockSpec(memory_space=pltpu.HBM)
    shape = jax.ShapeDtypeStruct
    outs = pl.pallas_call(
        grad_kernel,
        out_shape=[shape((2, LINE, SHARD, DIM), f32), shape((2, SHARD, FFN), f32), shape((2, TILE, DIM), f32), shape((PLANE, TILE), f32),
                   shape((n * FAR, DIM), bf16)] + [shape((FAR, WIDTH[name]), bf16) for _, name in PIECES],
        in_specs=[hbm] * (2 * n + 1),
        out_specs=[hbm] * 3 + [pl.BlockSpec(memory_space=pltpu.VMEM)] + [hbm] * (n + 1),
        scratch_shapes=[pltpu.VMEM((1536, DIM), bf16), pltpu.VMEM((1536, WIDE), bf16)]
        + [pltpu.VMEM(acc_shape(name), f32) for _, name in PIECES]
        + [pltpu.VMEM((2,) + acc_shape(name), f32) for _, name in PIECES]
        + [pltpu.VMEM((BAND, TILE), f32), pltpu.VMEM((SPREAD, TILE), f32), pltpu.VMEM((56, TILE), f32)]
        + [dma, dma((n, 6)), dma, dma((n,)), dma((n,)), dma((n,)), dma((7,)), dma((n,)), dma((n, 2, LINE)),
           dma((n,)), dma((n,)), dma((n,)), dma((2,)), dma((2,))],
        compiler_params=pltpu.CompilerParams(collective_id=1, has_side_effects=True, vmem_limit_bytes=58 * DIM * DIM),
        name="reduce_grads",
    )(*bc, *sl, sums)
    return outs[:LINE]


def solution(mesh):
    axis_name = mesh.axis_names[0]
    batch_spec = P(axis_name)
    weight_specs = (P(None, None, axis_name, None), P(None, None, axis_name), P(None, None, axis_name),
                    P(None, axis_name, None), P(None, axis_name), P(None, axis_name, None), P(None, axis_name))

    def device_step(x, lengths, d_y, w_attn, b_attn, ln_par, w_up, b_up, w_down, b_down):
        tables = rotary_tables(x.shape[1])
        fa, fu, fd, fs = gather_weights(w_attn, w_up, w_down, pack_small(b_attn, ln_par, b_up, b_down))
        smalls = unpack_small(fs)
        weights = [(fa[l], fu[l], fd[FFN * l:FFN * l + FFN]) + smalls[l] for l in range(2)]
        hidden, saved = x[0], []
        for l in range(2):
            hidden, acts = layer_forward(hidden, weights[l], lengths[0], tables, l == 1)
            saved.append(acts)
        grad, bc, sl, tiny = d_y[0], [], [], [None] * 2
        for l in (1, 0):
            grad, (h1, ctx, h2, act, d_proj, d_mid, d_pre, d_out), small = layer_backward(grad, saved[l], weights[l], tables)
            bc += [d_out, h2, ctx, h1]
            sl += [act, d_pre, d_mid, d_proj]
            gb, gl, gu, gd = small
            tiny[l] = jnp.concatenate([gb.reshape(LINE, SHARD, SHARD).transpose(1, 0, 2).reshape(SHARD, TILE),
                                       gl.reshape(LINE, SHARD, SHARD).transpose(1, 0, 2).reshape(SHARD, TILE),
                                       gu.reshape(SHARD, TILE), gd.reshape(SHARD, SHARD), jnp.zeros((SHARD, HALF_SEQ), jnp.float32)], axis=1)
        sums = jnp.concatenate(tiny, axis=1).reshape(LINE, PLANE, PLANE, TILE).transpose(1, 0, 2, 3).reshape(BAND, TILE)
        g_attn, g_up, g_down, g_small = reduce_grads(bc, sl, sums)
        rows = g_small.reshape(2, LINE, TILE)
        return (grad[None], g_attn, rows[:, 0].reshape(2, LINE, SHARD), rows[:, 1].reshape(2, LINE, SHARD), g_up, rows[:, 2],
                g_down, rows[:, 3, :SHARD])

    return jax.shard_map(device_step, mesh=mesh,
                         in_specs=(batch_spec, batch_spec, batch_spec) + weight_specs,
                         out_specs=(batch_spec,) + weight_specs,
                         check_vma=False)
```

```python
import functools
import math
import jax
import jax.numpy as jnp
import numpy as np
from jax import lax
from jax.experimental import pallas as pl
from jax.experimental.pallas import tpu as pltpu
from jax.sharding import PartitionSpec as P

PAIR = 2
TRIO = 3
LINE = 4
PLANE = 8
HEADS = 16
SHARD = 32
HEAD_DIM = 64
HALF_SEQ = 96
TILE = 128
SEQ = 192
SPREAD = 224
BAND = 256
WIDE = 512
DIM = 1024
FAR = 1344
FFN = 4096

MESH = pl.DeviceIdType.MESH
EPS = 1e-5
THETA = 10000.0
NEG_BIG = -1e30
SQRT_HALF = math.sqrt(0.5)
DENSITY = 1.0 / math.sqrt(2.0 * math.pi)
SCALE = HEAD_DIM ** -0.5
F32, BF16 = jnp.float32, jnp.bfloat16
DMA = pltpu.SemaphoreType.DMA


def dot(a, b, ca=1, cb=0, precision=None):
    return lax.dot_general(a, b, (((ca,), (cb,)), ((), ())), preferred_element_type=F32, precision=precision)


def span(index, size):
    return pl.ds(pl.multiple_of(size * index, size), size)


def repeat(count, body):
    def step(i, carry):
        body(i)
        return carry

    lax.fori_loop(0, count, step, 0)


def local(src, dst, sem):
    return pltpu.make_async_copy(src, dst, sem)


def drain(ref, sem):
    local(ref, ref, sem).wait()


def remote(src, dst, send, recv, dev):
    return pltpu.make_async_remote_copy(src_ref=src, dst_ref=dst, send_sem=send, recv_sem=recv,
                                        device_id=(dev,), device_id_type=MESH)


def rotary_tables():
    lane = np.arange(TILE)
    angles = np.arange(SEQ)[:, None] * THETA ** (-(lane % SHARD) / SHARD)[None, :]
    sign = np.where(lane % HEAD_DIM < SHARD, -1.0, 1.0)
    return np.cos(angles).astype(np.float32), (np.sin(angles) * sign).astype(np.float32)


def rotate(block, cos, sin):
    lane = lax.broadcasted_iota(jnp.int32, block.shape, 1)
    return block * cos + jnp.where((lane & SHARD) == 0, pltpu.roll(block, HALF_SEQ, 1), pltpu.roll(block, SHARD, 1)) * sin


def head_masks(block):
    lane = lax.broadcasted_iota(jnp.int32, block.shape, 1)
    zero = jnp.zeros_like(block)
    return jnp.where(lane < HEAD_DIM, block, zero), jnp.where(lane < HEAD_DIM, zero, block)


def row_mean(x):
    return jnp.mean(x, axis=-1, keepdims=True)


def row_sum(x):
    return jnp.sum(x, axis=-1, keepdims=True)


def column_sum(x):
    return jnp.sum(x, axis=0, keepdims=True)


def normed(x):
    centered = x - row_mean(x)
    inv = lax.rsqrt(row_mean(centered * centered) + EPS)
    return centered * inv, inv


def pick(kind):
    shape = (TILE, DIM)
    return lax.broadcasted_iota(jnp.int32, shape, 0) == SHARD * kind + (lax.broadcasted_iota(jnp.int32, shape, 1) & 31)


def owned(swap):
    shape = (SHARD, DIM)
    row = lax.broadcasted_iota(jnp.int32, shape, 0)
    if swap:
        row = (row & TRIO) * PLANE + (row >> PAIR)
    return row == lax.broadcasted_iota(jnp.int32, shape, 1) >> 5


def unpack_vectors(small, vec):
    for l in range(PAIR):
        for t in (0, 1, TRIO):
            rows = small[pl.ds(LINE * l + t, SHARD, stride=PLANE), :].astype(BF16)
            for kind in range(1 if t == TRIO else LINE):
                spread = dot(rows, pick(kind).astype(BF16))
                at = 24 + l if t == TRIO else PLANE * l + LINE * t + kind
                vec[pl.ds(at, 1), :] = column_sum(jnp.where(owned(False), spread, 0.0))
        for d in range(SHARD):
            vec[pl.ds(HEADS + LINE * l + d // PLANE, 1), pl.ds(d % PLANE * TILE, TILE)] = small[pl.ds(PLANE * d + LINE * l + PAIR, 1), :]


def pack_vectors(vec, packed):
    for l in range(PAIR):
        for t in (0, 1, TRIO):
            total = None
            for kind in range(1 if t == TRIO else LINE):
                at = 24 + l if t == TRIO else PLANE * l + LINE * t + kind
                mine = jnp.where(owned(True), vec[pl.ds(at, 1), :], 0.0)
                part = dot(mine, pick(kind).astype(F32), 1, 1, lax.Precision.HIGHEST)
                total = part if total is None else total + part
            packed[pl.ds(LINE * l + t, SHARD, stride=PLANE), :] = total
        for d in range(SHARD):
            packed[pl.ds(SHARD * (d % PLANE) + PLANE * (d // PLANE) + LINE * l + PAIR, 1), :] = vec[pl.ds(HEADS + LINE * l + d // PLANE, 1),
                                                                              pl.ds(d % PLANE * TILE, TILE)]


def norm_stage(src, vec, at, dst):
    def body(i):
        rows = span(i, SHARD)
        unit, _ = normed(src[rows, :].astype(F32))
        dst[rows, :] = (unit * vec[pl.ds(at, 1), :] + vec[pl.ds(at + 1, 1), :]).astype(BF16)

    repeat(6, body)


def project_stage(l, h, w, vec, cos, sin, qkv):
    for kind in range(TRIO):
        def body(n, kind=kind):
            cols = span(n, BAND)
            out = dot(h[...], w[pl.ds(DIM * kind, DIM), cols]) + vec[pl.ds(PLANE * l + kind, 1), cols]
            if kind == 0:
                out = out * SCALE
            if kind < PAIR:
                out = jnp.concatenate([rotate(out[:, :TILE], cos[...], sin[...]), rotate(out[:, TILE:], cos[...], sin[...])], axis=1)
            qkv[:, pl.ds(pl.multiple_of(DIM * kind + BAND * n, BAND), BAND)] = out.astype(BF16)

        repeat(LINE, body)


def attend_stage(qkv, keep, probs, ctx):
    def body(p):
        query = qkv[:, span(p, TILE)]
        keys = head_masks(qkv[:, span(p + PLANE, TILE)])
        vals = head_masks(qkv[:, span(p + HEADS, TILE)])
        out = None
        for h in range(PAIR):
            scores = jnp.where(keep[...] > 0.5, dot(query, keys[h], 1, 1), NEG_BIG)
            grown = jnp.exp(scores - jnp.max(scores, axis=-1, keepdims=True))
            weight = (grown / row_sum(grown)).astype(BF16)
            probs[PAIR * p + h] = weight
            part = dot(weight, vals[h])
            out = part if out is None else out + part
        ctx[:, span(p, TILE)] = out.astype(BF16)

    repeat(PLANE, body)


def residual_stage(a, w, base, bias, vec, dst):
    def body(n):
        cols = span(n, BAND)
        dst[:, cols] = (base[:, cols].astype(F32) + dot(a[...], w[:, cols]) + vec[pl.ds(bias, 1), cols]).astype(BF16)

    repeat(LINE, body)


def up_stage(l, h, w, vec, act, slope):
    def body(c):
        part, n = lax.div(c, LINE), lax.rem(c, LINE)
        cols = span(c, BAND)
        pre = dot(h[...], w[span(part, DIM), span(n, BAND)]) + vec[pl.ds(HEADS + LINE * l + part, 1), span(n, BAND)]
        cdf = 0.5 * (1.0 + lax.erf(pre * SQRT_HALF))
        act[:, cols] = (pre * cdf).astype(BF16)
        slope[:, cols] = cdf + pre * (jnp.exp(-0.5 * pre * pre) * DENSITY)

    repeat(HEADS, body)


def fold(block):
    return sum(block[PLANE * i:PLANE * i + PLANE] for i in range(block.shape[0] // PLANE))


def act_grad_stage(part, d_out, w, slope, d_pre, vec, row):
    def body(n):
        cols, local_cols = span(LINE * part + n, BAND), span(n, BAND)
        grad = dot(d_out[...], w[span(n, BAND), :], 1, 1) * slope[:, local_cols]
        d_pre[:, cols] = grad.astype(BF16)
        vec[pl.ds(row + part, 1), local_cols] = column_sum(grad)

    repeat(LINE, body)


def norm_grad_stage(src, d_h, d_res, gain, vec, row_gain, row_out, row_res, dst):
    zero = jnp.zeros((PLANE, DIM), F32)

    def body(i, carry):
        rows = span(i, SHARD)
        unit, inv = normed(src[rows, :].astype(F32))
        grad = d_h[rows, :]
        scaled = grad * gain
        inner = scaled - row_mean(scaled) - unit * row_mean(scaled * unit)
        res = d_res[rows, :].astype(F32)
        out = (res + inv * inner).astype(BF16)
        dst[rows, :] = out
        return tuple(c + fold(v) for c, v in zip(carry, (grad * unit, grad, out.astype(F32), res)))

    sums = lax.fori_loop(0, 6, body, (zero,) * LINE)
    for at, value in zip((row_gain, row_gain + 1, row_out, row_res), sums):
        if at is not None:
            vec[pl.ds(at, 1), :] = column_sum(value)


def attend_grad_stage(l, qkv, probs, d_ctx, cos, sin, d_proj, vec):
    def body(p):
        keys = head_masks(qkv[:, span(p + PLANE, TILE)])
        queries = head_masks(qkv[:, span(p, TILE)])
        vals = qkv[:, span(p + HEADS, TILE)]
        outs = head_masks(d_ctx[:, span(p, TILE)])
        d_q = d_k = d_v = 0.0
        for h in range(PAIR):
            weight = probs[PAIR * p + h]
            wide = weight.astype(F32)
            d_weight = dot(outs[h], vals, 1, 1)
            d_score = (wide * (d_weight - row_sum(d_weight * wide))).astype(BF16)
            d_v = d_v + dot(weight, outs[h], 0, 0)
            d_q = d_q + dot(d_score, keys[h])
            d_k = d_k + dot(d_score, queries[h], 0, 0)
        d_q = rotate(d_q, cos[...], -sin[...]) * SCALE
        d_k = rotate(d_k, cos[...], -sin[...])
        for kind, grad in enumerate((d_q, d_k, d_v)):
            grad = grad.astype(BF16)
            d_proj[:, span(p + PLANE * kind, TILE)] = grad
            vec[pl.ds(PLANE * l + kind, 1), span(p, TILE)] = column_sum(grad.astype(F32))

    repeat(PLANE, body)
LAYERS = PAIR
ORDERS = (("b", 0, 1), ("b", 1, 0), ("a", 0, 1), ("a", 1, 0), ("b", 0, 1), ("b", 1, 0))
UNITS = [(0, 6)] + [(layer, piece) for layer in range(LAYERS) for piece in range(6)]
STAGE_LAG = (0, 0, 1, TRIO)
AHEAD = PAIR


SAVED = ("h1", "qkv", "probs", "ctx", "mid", "h2", "act", "slope")
SAVED_SHAPES = {"h1": (SEQ, DIM), "qkv": (SEQ, 3072), "probs": (HEADS, SEQ, SEQ), "ctx": (SEQ, DIM), "mid": (SEQ, DIM),
                "h2": (SEQ, DIM), "act": (SEQ, FFN), "slope": (SEQ, FFN)}


def saved_type(name):
    return F32 if name == "slope" else BF16


def forward_kernel(*refs):
    (wa, wu, wd, sm, x, keep, cos, sin), refs = refs[:PLANE], refs[PLANE:]
    (fa, fu, fd, fs, out_vec, out_mid), refs = refs[:6], refs[6:]
    saved = [dict(zip(SAVED, refs[PLANE * l:PLANE * l + PLANE])) for l in range(LAYERS)]
    refs = refs[HEADS:]
    (va, vu, vd, vs), refs = refs[:LINE], refs[LINE:]
    acts = [dict(zip(SAVED, refs[PLANE * l:PLANE * l + PLANE])) for l in range(LAYERS)]
    refs = refs[HEADS:]
    (y, vec, small_in, small, w_even, w_odd, load_sem, save_sem, own_sem, xy_sem, z_sem, push_send, push_recv,
     recv_sem) = refs
    me = lax.axis_index("fsdp")
    core, xc, yc, zc = me % PAIR, (me // PAIR) % PAIR, (me // LINE) % PAIR, me // PLANE
    partner = me + 1 - PAIR * core
    near = (me + PAIR - LINE * xc, me + LINE - PLANE * yc)
    up, down = me + PLANE, me - PLANE
    has_up, has_down = zc < TRIO, zc > 0

    def full(u, src):
        layer, piece = UNITS[u]
        if piece < PAIR:
            return fa.at[layer, pl.ds(PAIR * piece, PAIR), pl.ds(pl.multiple_of(SHARD * src, SHARD), SHARD), :]
        if piece < LINE:
            return fu.at[layer, pl.ds(pl.multiple_of(SHARD * src + HEADS * (piece - PAIR), HEADS), HEADS), :]
        if piece < 6:
            return fd.at[pl.ds(pl.multiple_of(FFN * layer + TILE * src + HEAD_DIM * (piece - LINE), HEAD_DIM), HEAD_DIM), :]
        return fs.at[pl.ds(pl.multiple_of(PLANE * src, PLANE), PLANE), :]

    def own(u):
        layer, piece = UNITS[u]
        if piece < PAIR:
            return va.at[layer, pl.ds(PAIR * piece, PAIR)]
        if piece < LINE:
            return vu.at[layer, pl.ds(HEADS * (piece - PAIR), HEADS), :]
        if piece < 6:
            return vd.at[layer, pl.ds(HEAD_DIM * (piece - LINE), HEAD_DIM), :]
        return vs

    def kind(u):
        return (UNITS[u][1] + 0) // PAIR

    def order(u):
        return ORDERS[UNITS[u][1] % 6]

    def tiny(u):
        return 1 if UNITS[u][1] == 6 else 0

    barrier = pltpu.get_barrier_semaphore()
    for peer in (partner,) + near:
        pl.semaphore_signal(barrier, inc=1, device_id=(peer,), device_id_type=MESH)

    @pl.when(has_up)
    def _():
        pl.semaphore_signal(barrier, inc=1, device_id=(up,), device_id_type=MESH)

    @pl.when(has_down)
    def _():
        pl.semaphore_signal(barrier, inc=1, device_id=(down,), device_id_type=MESH)

    loads = [local(src, dst, load_sem.at[i])
             for i, (src, dst) in enumerate(((wa, va), (wu, vu), (wd, vd), (sm, vs)))]
    for load in loads:
        load.start()
    for load in loads:
        load.wait()
    pl.semaphore_wait(barrier, TRIO + has_up.astype(jnp.int32) + has_down.astype(jnp.int32))

    def slab(u, src_ref, src, send, recv, dev):
        return remote(src_ref, full(u, src), send, recv, dev)

    def send_z(u, src_ref, src, slot, above, below):
        if above is not None:
            @pl.when(above)
            def _():
                slab(u, src_ref, src, z_sem.at[tiny(u)], recv_sem.at[u, slot], up).start()
        if below is not None:
            @pl.when(below)
            def _():
                slab(u, src_ref, src, z_sem.at[tiny(u)], recv_sem.at[u, slot], down).start()

    def send_xy(u, src_ref, src, dim, slot):
        slab(u, src_ref, src, xy_sem.at[tiny(u)], recv_sem.at[u, slot], near[dim]).start()

    def push(u, src_ref, src):
        slab(u, src_ref, src, push_send.at[kind(u)], push_recv.at[u], partner).start()

    def column(flip_p, p):
        base = me - PLANE * zc
        if flip_p:
            base = base + (near[p] - me)
        return base

    def arrived(u, src, slot):
        slab(u, full(u, src), src, xy_sem.at[tiny(u)], recv_sem.at[u, slot], me).wait_recv()
        return full(u, src)

    def stage0(u):
        col, p, q = order(u)
        mine = own(u)
        send_z(u, mine, me, zc, has_up, has_down)
        send_xy(u, mine, me, p, LINE + zc)
        send_xy(u, mine, me, q, PLANE)
        push(u, mine, me)
        local(mine, full(u, me), own_sem.at[u]).start()

    def z_arrivals(u, flips, send_p):
        col, p, q = order(u)
        for dz in (1, PAIR, TRIO):
            for step in (-1, 1):
                for flip_p in flips:
                    zs = zc + step * dz
                    src = column(flip_p, p) + PLANE * zs
                    slot = LINE * flip_p + zs
                    present = (zc >= dz) if step < 0 else (zc <= TRIO - dz)

                    @pl.when(present)
                    def _(src=src, slot=slot, step=step):
                        ref = arrived(u, src, slot)
                        send_z(u, ref, src, slot, has_up if step < 0 else None, has_down if step > 0 else None)
                        if send_p:
                            send_xy(u, ref, src, p, LINE + slot)
                        send_xy(u, ref, src, q, PLANE)
                        push(u, ref, src)

    def stage1(u):
        col, p, q = order(u)
        if col == "a":
            z_arrivals(u, (0,), True)
        else:
            src = near[p]
            ref = arrived(u, src, LINE + zc)
            send_z(u, ref, src, LINE + zc, has_up, has_down)
            send_xy(u, ref, src, q, PLANE)
            push(u, ref, src)

    def stage2(u):
        col, p, q = order(u)
        if col == "a":
            for hop in range(LINE):
                zs = lax.rem(zc + hop, LINE)
                src = column(1, p) + PLANE * zs
                ref = arrived(u, src, LINE + zs)
                send_xy(u, ref, src, q, PLANE)
                push(u, ref, src)
        else:
            z_arrivals(u, (0, 1), False)

    def stage3(u):
        col, p, q = order(u)
        rows = fs.at[pl.ds(0, HEAD_DIM), :] if tiny(u) else fd.at[pl.ds(0, WIDE), :]
        drain(rows, recv_sem.at[u, PLANE])
        for flip_p in (0, 1):
            base = column(flip_p, p) + (near[q] - me)

            def body(zs, carry, base=base):
                src = base + PLANE * zs
                push(u, full(u, src), src)
                return carry

            lax.fori_loop(0, LINE, body, 0)

    def ready(*units):
        for u in units:
            drain(fs.at[pl.ds(0, TILE), :] if tiny(u) else fd.at[pl.ds(0, DIM), :], push_recv.at[u])
            drain(own(u), own_sem.at[u])

    def fetch(l, what, buf):
        for i in range(LINE):
            src = {"a": lambda: fa.at[l, i], "u": lambda: fu.at[l, :, pl.ds(DIM * i, DIM)],
                   "d": lambda: fd.at[pl.ds(FFN * l + DIM * i, DIM), :]}[what]()
            local(src, buf.at[pl.ds(DIM * i, DIM), :], load_sem.at[i]).start()

    def fetched(buf):
        for i in range(LINE):
            drain(buf.at[pl.ds(DIM * i, DIM), :], load_sem.at[i])

    def save(l, *names):
        for name in names:
            local(acts[l][name], saved[l][name], save_sem.at[l, SAVED.index(name)]).start()

    def source(l):
        return y if l else x

    def begin():
        ready(0)
        local(fs, small_in, load_sem.at[0]).start()
        drain(small_in, load_sem.at[0])
        small[...] = small_in[...].astype(F32)
        unpack_vectors(small, vec)
        local(vec, out_vec, save_sem.at[0, PLANE]).start()
        norm_stage(x, vec, LINE, acts[0]["h1"])
        save(0, "h1")

    def project(l, buf):
        fetched(buf)
        project_stage(l, acts[l]["h1"], buf, vec, cos, sin, acts[l]["qkv"])
        save(l, "qkv")

    def attend(l, buf):
        got = acts[l]
        attend_stage(got["qkv"], keep, got["probs"], got["ctx"])
        residual_stage(got["ctx"], buf.at[pl.ds(3072, DIM), :], source(l), PLANE * l + TRIO, vec, got["mid"])
        norm_stage(got["mid"], vec, PLANE * l + 6, got["h2"])
        save(l, "probs", "ctx", "mid", "h2")

    def grow(l, buf):
        fetched(buf)
        up_stage(l, acts[l]["h2"], buf, vec, acts[l]["act"], acts[l]["slope"])
        save(l, "act", "slope")

    def shrink(buf):
        fetched(buf)
        residual_stage(acts[0]["act"], buf, acts[0]["mid"], 24, vec, y)
        local(y, out_mid, save_sem.at[1, PLANE]).start()
        norm_stage(y, vec, 12, acts[1]["h1"])
        save(1, "h1")

    def need(l, pair, what, buf):
        def go():
            first = 1 + 6 * l + PAIR * pair
            ready(first, first + 1)
            fetch(l, what, buf)
        return go

    before = {6: need(0, 0, "a", w_even), PLANE: need(0, 1, "u", w_odd), 10: need(0, PAIR, "d", w_even),
              12: need(1, 0, "a", w_odd), 14: need(1, 1, "u", w_even)}
    after = {5: begin, 6: lambda: project(0, w_even), 7: lambda: attend(0, w_even), PLANE: lambda: grow(0, w_odd),
             10: lambda: shrink(w_even), 12: lambda: project(1, w_odd), 13: lambda: attend(1, w_odd),
             14: lambda: grow(1, w_even)}
    stages = (stage0, stage1, stage2, stage3)
    count = len(UNITS)
    for rnd in range(count + STAGE_LAG[TRIO]):
        before.get(rnd, lambda: None)()
        for k in range(LINE):
            if k == 0:
                todo = range(AHEAD + 1) if rnd == 0 else [rnd + AHEAD]
            else:
                todo = [rnd - STAGE_LAG[k]]
            for u in todo:
                if 0 <= u < count:
                    stages[k](u)
        after.get(rnd, lambda: None)()
    ready(count - PAIR, count - 1)

    per_layer = HEAD_DIM * LAYERS
    drain(fd.at[pl.ds(0, 60 * per_layer), :], xy_sem.at[0])
    drain(fs.at[pl.ds(0, 9 * PLANE), :], xy_sem.at[1])
    ends = jnp.logical_or(zc == 0, zc == TRIO)

    @pl.when(ends)
    def _():
        drain(fd.at[pl.ds(0, 10 * per_layer), :], z_sem.at[0])
        drain(fs.at[pl.ds(0, PAIR * PLANE), :], z_sem.at[1])

    @pl.when(jnp.logical_not(ends))
    def _():
        drain(fd.at[pl.ds(0, 50 * per_layer), :], z_sem.at[0])
        drain(fs.at[pl.ds(0, 10 * PLANE), :], z_sem.at[1])

    halves = (fa.at[0], fu.at[0], fd.at[pl.ds(0, FFN), :], fs.at[pl.ds(0, TILE), :])
    for i, half in enumerate(halves):
        drain(half, push_send.at[i])
    for l in range(LAYERS):
        for i, name in enumerate(SAVED):
            drain(saved[l][name], save_sem.at[l, i])
    drain(out_vec, save_sem.at[0, PLANE])
    drain(out_mid, save_sem.at[1, PLANE])


def forward(w_attn, w_up, w_down, small, x, keep, cos, sin):
    shape, hbm, vmem = jax.ShapeDtypeStruct, pl.BlockSpec(memory_space=pltpu.HBM), pl.BlockSpec(memory_space=pltpu.VMEM)
    kept = [shape(SAVED_SHAPES[name], saved_type(name)) for name in SAVED] * LAYERS
    outs = pl.pallas_call(
        forward_kernel,
        out_shape=[shape((LAYERS, LINE, DIM, DIM), BF16), shape((LAYERS, DIM, FFN), BF16),
                   shape((LAYERS * FFN, DIM), BF16), shape((BAND, TILE), BF16), shape((SHARD, DIM), F32),
                   shape((SEQ, DIM), BF16)] + kept,
        in_specs=[hbm] * LINE + [vmem] * LINE,
        out_specs=[hbm] * (6 + len(kept)),
        scratch_shapes=[pltpu.VMEM(w.shape, BF16) for w in (w_attn, w_up, w_down, small)]
        + [pltpu.VMEM(k.shape, k.dtype) for k in kept]
        + [pltpu.VMEM((SEQ, DIM), BF16), pltpu.VMEM((SHARD, DIM), F32), pltpu.VMEM((BAND, TILE), BF16),
           pltpu.VMEM((BAND, TILE), F32), pltpu.VMEM((FFN, DIM), BF16), pltpu.VMEM((FFN, DIM), BF16),
           DMA((LINE,)), DMA((PAIR, 9)), DMA((len(UNITS),)), DMA((PAIR,)), DMA((PAIR,)), DMA((LINE,)), DMA((len(UNITS),)),
           DMA((len(UNITS), 9))],
        compiler_params=pltpu.CompilerParams(collective_id=0, has_side_effects=True, vmem_limit_bytes=60 * DIM * DIM),
        name="forward",
    )(w_attn, w_up, w_down, small, x, keep, cos, sin)
    return outs[:TRIO], outs[LINE], outs[5], [dict(zip(SAVED, outs[6 + PLANE * l:14 + PLANE * l])) for l in range(LAYERS)]


PIECES = [(layer, name) for layer in (1, 0) for name in "DUOQ"]
WIDTH = {"D": WIDE, "U": WIDE, "O": TILE, "Q": 384}
ROWS = SEQ
LAG = (1, PAIR, TRIO)


def acc_shape(name):
    return (WIDE, DIM) if name == "D" else (DIM, WIDTH[name])


def backward_kernel(*refs):
    n = len(PIECES)
    (fa, fu, fd, vec, cos, sin, x_in, y_in, d_y), refs = refs[:9], refs[9:]
    saved = [dict(zip(SAVED, refs[PLANE * l:PLANE * l + PLANE])) for l in range(LAYERS)]
    refs = refs[HEADS:]
    (g_attn, g_up, g_down, g_small, d_x, bc_far), refs = refs[:6], refs[6:]
    sl_far, refs = refs[:n], refs[n:]
    (d_pre_far, d_mid_far, d_proj_far, d_top), refs = refs[:LINE], refs[LINE:]
    (bc_v, sl_v), refs = refs[:PAIR], refs[PAIR:]
    acc, got, refs = refs[:n], refs[n:PAIR * n], refs[PAIR * n:]
    (sum_v, sum_got, sum_line, square, wide, slope_v, qkv_v, probs_v, mid_v, x_v, d_out, d_pre, d_mid, d_proj, d_ctx, d_h,
     g_vec), refs = refs[:17], refs[17:]
    (bc_send, bc_recv, push_send, push_recv, sl_send, sl_recv, load_sem, rs_send, rs_recv, out_send, out_recv, own_sem,
     sum_send, sum_recv, square_sem, slope_sem, wide_sem, act_sem, spill_sem) = refs
    d_outs = (d_top, d_y)
    bc_in = [{"D": d_outs[l], "U": saved[l]["h2"], "O": saved[l]["ctx"], "Q": saved[l]["h1"]}[name] for l, name in PIECES]
    sl_in = [{"D": saved[l]["act"], "U": d_pre_far.at[l], "O": d_mid_far.at[l], "Q": d_proj_far.at[l]}[name]
             for l, name in PIECES]

    me = lax.axis_index("fsdp")
    core, xc, yc, zc = me % PAIR, (me // PAIR) % PAIR, (me // LINE) % PAIR, me // PLANE
    place = me % PLANE

    def peer(r):
        out = me
        if r & 1:
            out = out + 1 - PAIR * core
        if r & PAIR:
            out = out + PAIR - LINE * xc
        if r & LINE:
            out = out + LINE - PLANE * yc
        return out

    def line(k):
        return place + PLANE * lax.rem(zc + k, LINE)

    barrier = pltpu.get_barrier_semaphore()
    for r in range(1, PLANE):
        pl.semaphore_signal(barrier, inc=1, device_id=(peer(r),), device_id_type=MESH)
    for k in range(1, LINE):
        pl.semaphore_signal(barrier, inc=1, device_id=(line(k),), device_id_type=MESH)
    pl.semaphore_wait(barrier, 10)

    def far(u, r, half=None):
        start = FAR * u + SEQ * (r - 1)
        return bc_far.at[pl.ds(start, SEQ), :] if half is None else bc_far.at[pl.ds(start + HALF_SEQ * half, HALF_SEQ), :]

    def blocks(u, where):
        name = PIECES[u][1]
        if name == "D":
            return [(pl.multiple_of(DIM * i + TILE * where, TILE), TILE * i, TILE) for i in range(LINE)]
        if name == "Q":
            return [(pl.multiple_of(DIM * i + TILE * where, TILE), TILE * i, TILE) for i in range(TRIO)]
        return [(pl.multiple_of(WIDTH[name] * where, TILE), 0, WIDTH[name])]

    def send_bc(u):
        for r in (PAIR, LINE):
            for half in (0, 1):
                slot = (0 if r == PAIR else PAIR) + half
                remote(bc_in[u].at[pl.ds(HALF_SEQ * half, HALF_SEQ), :], far(u, r, half), bc_send, bc_recv.at[u, slot], peer(r)).start()
        remote(bc_in[u], far(u, 1), push_send, push_recv.at[u], peer(1)).start()

    def send_sl(u):
        for r in (PAIR, 6, LINE, TRIO, 7, 5, 1):
            for src, dst, width in blocks(u, peer(r) % PLANE):
                remote(sl_in[u].at[:, pl.ds(src, width)], sl_far[u].at[pl.ds(SEQ * (r - 1), SEQ), pl.ds(dst, width)],
                       sl_send.at[u], sl_recv.at[u], peer(r)).start()

    def push(u, r, half):
        remote(far(u, r, half), far(u, r + 1, half), push_send, push_recv.at[u], peer(1)).start()

    def relay_bc(u):
        for slot, r, half, onward in ((0, PAIR, 0, LINE), (TRIO, LINE, 1, PAIR), (1, PAIR, 1, None), (PAIR, LINE, 0, None)):
            drain(far(u, r, half), bc_recv.at[u, slot])
            if onward is not None:
                remote(far(u, r, half), far(u, 6, half), bc_send, bc_recv.at[u, LINE + half], peer(onward)).start()
            push(u, r, half)

    def collect(u):
        name = PIECES[u][1]
        own = [local(bc_in[u], bc_v.at[pl.ds(0, SEQ), :], load_sem.at[0])]
        for i, (src, dst, width) in enumerate(blocks(u, place)):
            own.append(local(sl_in[u].at[:, pl.ds(src, width)], sl_v.at[pl.ds(0, SEQ), pl.ds(dst, width)],
                             load_sem.at[1 + i]))
        for c in own:
            c.start()
        for half in (0, 1):
            drain(far(u, 6, half), bc_recv.at[u, LINE + half])
            push(u, 6, half)
        drain(sl_far[u], sl_recv.at[u])
        drain(bc_far.at[pl.ds(0, 768), :], push_recv.at[u])
        rest = [local(bc_far.at[pl.ds(FAR * u, FAR), :], bc_v.at[pl.ds(SEQ, FAR), :], load_sem.at[5]),
                local(sl_far[u], sl_v.at[pl.ds(SEQ, FAR), pl.ds(0, WIDTH[name])], load_sem.at[6])]
        for c in rest:
            c.start()
        for c in own + rest:
            c.wait()

    def piece_rows(u):
        return acc_shape(PIECES[u][1])[0] // LINE

    def piece(ref, u, d):
        pr = piece_rows(u)
        return ref.at[pl.ds(pl.multiple_of(pr * d, pr), pr), :]

    def step_down_line(u, d, up):
        side = jnp.where(up, 0, 1)
        dst = got[u].at[side, span(d - 1 + side, piece_rows(u)), :]
        remote(piece(acc[u], u, d), dst, rs_send.at[u], rs_recv.at[u, side, d], me + jnp.where(up, PLANE, -PLANE)).start()

    def add_piece(u, side, d):
        pr = piece_rows(u)
        drain(piece(acc[u], u, d), rs_recv.at[u, side, d])
        rows = SHARD

        def body(i, carry):
            at = pl.ds(pl.multiple_of(pr * d + rows * i, rows), rows)
            there = pl.ds(pl.multiple_of(pr * (d - 1 + side) + rows * i, rows), rows)
            acc[u][at, :] = acc[u][at, :] + got[u][side, there, :]
            return carry

        lax.fori_loop(0, pr // rows, body, 0)

    def product(u):
        name = PIECES[u][1]
        pr, width = piece_rows(u), WIDTH[name]

        def body(d, carry):
            at = pl.ds(pl.multiple_of(pr * d, pr), pr)
            if name == "D":
                lhs, rhs = sl_v[:, at], bc_v[...]
            else:
                lhs, rhs = bc_v[:, at], sl_v[:, pl.ds(0, width)]
            acc[u][at, :] = lax.dot_general(lhs, rhs, (((0,), (0,)), ((), ())), preferred_element_type=jnp.float32)
            return carry

        lax.fori_loop(0, LINE, body, 0)

        @pl.when(jnp.logical_or(zc == 0, zc == TRIO))
        def _():
            for hop in range(TRIO):
                step_down_line(u, jnp.where(zc == 0, TRIO - hop, hop), zc == 0)

    def second_hop(u):
        @pl.when(jnp.logical_or(zc == 1, zc == PAIR))
        def _():
            for hop in range(PAIR):
                d = jnp.where(zc == 1, TRIO - hop, hop)
                add_piece(u, jnp.where(zc == 1, 0, 1), d)
                step_down_line(u, d, zc == 1)

    def third_hop(u):
        @pl.when(jnp.logical_or(zc == 1, zc == PAIR))
        def _():
            d = jnp.where(zc == 1, 0, TRIO)
            add_piece(u, jnp.where(zc == 1, 1, 0), d)
            step_down_line(u, d, zc == PAIR)

    def finish(u):
        layer, name = PIECES[u]

        @pl.when(zc > 0)
        def _():
            add_piece(u, 0, zc)

        @pl.when(zc < TRIO)
        def _():
            add_piece(u, 1, zc)

        if name == "D":
            local(piece(acc[u], u, zc), g_down.at[layer], own_sem.at[u]).start()
            return
        for r in range(PLANE):
            at = pl.ds(pl.multiple_of(BAND * zc + SHARD * (peer(r) % PLANE), SHARD), SHARD)
            if name == "U":
                pairs = [(acc[u].at[at, :], g_up.at[layer, :, pl.ds(pl.multiple_of(WIDE * place, WIDE), WIDE)])]
            else:
                mats = (TRIO,) if name == "O" else (0, 1, PAIR)
                pairs = [(acc[u].at[at, pl.ds(TILE * i, TILE)],
                          g_attn.at[layer, m, :, pl.ds(pl.multiple_of(TILE * place, TILE), TILE)]) for i, m in enumerate(mats)]
            for src, dst in pairs:
                if r == 0:
                    local(src, dst, own_sem.at[u]).start()
                else:
                    remote(src, dst, out_send.at[u], out_recv.at[u], peer(r)).start()

    def sums_plane():
        for r in range(1, PLANE):
            remote(sum_v.at[pl.ds(pl.multiple_of(SHARD * (peer(r) % PLANE), SHARD), SHARD), :], sum_got.at[pl.ds(SHARD * (r - 1), SHARD), :],
                   sum_send.at[0], sum_recv.at[0], peer(r)).start()

    def sums_line():
        drain(sum_got, sum_recv.at[0])
        total = sum_v[pl.ds(pl.multiple_of(SHARD * place, SHARD), SHARD), :]
        for r in range(1, PLANE):
            total = total + sum_got[pl.ds(SHARD * (r - 1), SHARD), :]
        sum_line[pl.ds(0, SHARD), :] = total
        for k in range(1, LINE):
            remote(sum_line.at[pl.ds(pl.multiple_of(PLANE * lax.rem(zc + k, LINE), PLANE), PLANE), :],
                   sum_line.at[pl.ds(SHARD + PLANE * (k - 1), PLANE), :], sum_send.at[1], sum_recv.at[1], line(k)).start()

    def sums_end():
        drain(sum_line.at[pl.ds(0, 24), :], sum_recv.at[1])
        total = sum_line[pl.ds(pl.multiple_of(PLANE * zc, PLANE), PLANE), :]
        for k in range(1, LINE):
            total = total + sum_line[pl.ds(SHARD + PLANE * (k - 1), PLANE), :]
        g_small[...] = total

    squares = [(l, k) for l in (1, 0) for k in range(PLANE)]
    wides = [(l, k) for l in (1, 0) for k in range(LINE)]
    taken = [0, 0]

    def fetch_square(i):
        if i < len(squares):
            l, k = squares[i]
            src = fd.at[pl.ds(FFN * l + DIM * k, DIM), :] if k < LINE else fa.at[l, (TRIO, 0, 1, PAIR)[k - LINE]]
            local(src, square.at[i % PAIR], square_sem.at[i % PAIR]).start()
            if k < LINE:
                local(saved[l]["slope"].at[:, pl.ds(DIM * k, DIM)], slope_v.at[i % PAIR], slope_sem.at[i % PAIR]).start()

    def fetch_wide(i):
        if i < len(wides):
            l, k = wides[i]
            local(fu.at[l, pl.ds(BAND * k, BAND), :], wide.at[i % PAIR], wide_sem.at[i % PAIR]).start()

    def with_square(body):
        i = taken[0]
        drain(square.at[i % PAIR], square_sem.at[i % PAIR])
        if squares[i][1] < LINE:
            drain(slope_v.at[i % PAIR], slope_sem.at[i % PAIR])
        body(square.at[i % PAIR], slope_v.at[i % PAIR])
        fetch_square(i + PAIR)
        taken[0] += 1

    def with_wide(body):
        i = taken[1]
        drain(wide.at[i % PAIR], wide_sem.at[i % PAIR])
        body(wide.at[i % PAIR])
        fetch_wide(i + PAIR)
        taken[1] += 1

    def loads(l):
        pairs = [(saved[l]["qkv"], qkv_v), (saved[l]["probs"], probs_v), (saved[l]["mid"], mid_v), ((x_in, y_in)[l], x_v)]
        return [local(src, dst, act_sem.at[i]) for i, (src, dst) in enumerate(pairs)]

    def spill(src, dst, i):
        local(src, dst, spill_sem.at[i]).start()
        drain(src, spill_sem.at[i])

    def chain_act(l):
        for c in loads(l):
            c.start()
        for part in range(LINE):
            with_square(lambda w, sl: act_grad_stage(part, d_out, w, sl, d_pre, g_vec, HEADS + LINE * l))
        spill(d_pre, d_pre_far.at[l], 0)

    def chain_mid(l):
        for part in range(LINE):
            def body(w, part=part):
                d_h[:, pl.ds(BAND * part, BAND)] = dot(d_pre[...], w[...], 1, 1)

            with_wide(body)
        for c in loads(l):
            c.wait()
        norm_grad_stage(mid_v, d_h, d_out, vec[pl.ds(PLANE * l + 6, 1), :], g_vec, PLANE * l + 6, PLANE * l + TRIO, 24 + l, d_mid)
        spill(d_mid, d_mid_far.at[l], 0)

    def chain_attend(l):
        def to_ctx(w, _):
            def body(i):
                d_ctx[:, span(i, BAND)] = dot(d_mid[...], w[span(i, BAND), :], 1, 1).astype(BF16)

            repeat(LINE, body)

        with_square(to_ctx)
        attend_grad_stage(l, qkv_v, probs_v, d_ctx, cos, sin, d_proj, g_vec)
        spill(d_proj, d_proj_far.at[l], 0)

    def chain_norm(l):
        for kind in range(TRIO):
            def to_h(w, _, kind=kind):
                def body(i):
                    part = dot(d_proj[:, pl.ds(DIM * kind, DIM)], w[span(i, BAND), :], 1, 1)
                    d_h[:, span(i, BAND)] = d_h[:, span(i, BAND)] + part if kind else part

                repeat(LINE, body)

            with_square(to_h)
        norm_grad_stage(x_v, d_h, d_mid, vec[pl.ds(PLANE * l + LINE, 1), :], g_vec, PLANE * l + LINE, None, None, d_out)
        spill(d_out, (d_x, d_top)[l], 0)

    for i in (0, 1):
        fetch_square(i)
        fetch_wide(i)
    send_bc(0)
    send_sl(0)
    local(d_y, d_out, load_sem.at[0]).start()
    g_vec[...] = jnp.zeros_like(g_vec)
    drain(d_out, load_sem.at[0])
    chain_act(1)
    relay_bc(0)
    send_bc(1)
    chain_mid(1)
    chain = (lambda: chain_attend(1), lambda: chain_norm(1), lambda: chain_act(0), lambda: chain_mid(0),
             lambda: chain_attend(0), lambda: chain_norm(0))
    for s in range(n + LAG[PAIR]):
        if s < n:
            if s + 1 < n:
                relay_bc(s + 1)
                send_sl(s + 1)
            if s + PAIR < n:
                send_bc(s + PAIR)
            if s < len(chain):
                chain[s]()
            collect(s)
            product(s)
        for lag, hop in zip(LAG, (second_hop, third_hop, finish)):
            if 0 <= s - lag < n:
                hop(s - lag)
        if s == len(chain):
            pack_vectors(g_vec, sum_v)
            sums_plane()
        if s == len(chain) + 1:
            sums_line()
    sums_end()

    drain(bc_far.at[pl.ds(0, n * 576), :], bc_send)
    drain(bc_far.at[pl.ds(0, n * 768), :], push_send)
    drain(sum_got, sum_send.at[0])
    drain(sum_line.at[pl.ds(0, 24), :], sum_send.at[1])
    for u in range(n):
        name = PIECES[u][1]
        drain(sl_far[u], sl_send.at[u])
        drain(acc[u].at[pl.ds(0, TRIO * piece_rows(u)), :], rs_send.at[u])
        if name == "D":
            drain(acc[u].at[pl.ds(0, TILE), :], own_sem.at[u])
        else:
            drain(acc[u].at[pl.ds(0, SHARD), :], own_sem.at[u])
            drain(acc[u].at[pl.ds(0, SPREAD), :], out_send.at[u])
            drain(acc[u].at[pl.ds(0, SPREAD), :], out_recv.at[u])


def backward(weights, vec, cos, sin, x_in, y_in, d_y, saved):
    n = len(PIECES)
    shape, hbm, vmem = jax.ShapeDtypeStruct, pl.BlockSpec(memory_space=pltpu.HBM), pl.BlockSpec(memory_space=pltpu.VMEM)
    wide = lambda cols: (SEQ, cols)
    outs = pl.pallas_call(
        backward_kernel,
        out_shape=[shape((PAIR, LINE, SHARD, DIM), F32), shape((PAIR, SHARD, FFN), F32), shape((PAIR, TILE, DIM), F32), shape((PLANE, TILE), F32),
                   shape(wide(DIM), BF16), shape((n * FAR, DIM), BF16)]
        + [shape((FAR, WIDTH[name]), BF16) for _, name in PIECES]
        + [shape((LAYERS, SEQ, cols), BF16) for cols in (FFN, DIM, 3072)] + [shape(wide(DIM), BF16)],
        in_specs=[hbm] * TRIO + [vmem] * TRIO + [hbm] * (TRIO + PAIR * len(SAVED)),
        out_specs=[hbm] * TRIO + [vmem] + [hbm] * (n + 6),
        scratch_shapes=[pltpu.VMEM((1536, DIM), BF16), pltpu.VMEM((1536, WIDE), BF16)]
        + [pltpu.VMEM(acc_shape(name), F32) for _, name in PIECES]
        + [pltpu.VMEM((PAIR, TRIO * acc_shape(name)[0] // LINE, acc_shape(name)[1]), F32) for _, name in PIECES]
        + [pltpu.VMEM((BAND, TILE), F32), pltpu.VMEM((SPREAD, TILE), F32), pltpu.VMEM((56, TILE), F32),
           pltpu.VMEM((PAIR, DIM, DIM), BF16), pltpu.VMEM((PAIR, BAND, FFN), BF16), pltpu.VMEM((PAIR, SEQ, DIM), F32)]
        + [pltpu.VMEM(s, BF16) for s in (wide(3072), (HEADS, SEQ, SEQ), wide(DIM), wide(DIM), wide(DIM), wide(FFN),
                                         wide(DIM), wide(3072), wide(DIM))]
        + [pltpu.VMEM(wide(DIM), F32), pltpu.VMEM((SHARD, DIM), F32)]
        + [DMA, DMA((n, 6)), DMA, DMA((n,)), DMA((n,)), DMA((n,)), DMA((7,)), DMA((n,)), DMA((n, PAIR, LINE)),
           DMA((n,)), DMA((n,)), DMA((n,)), DMA((PAIR,)), DMA((PAIR,)), DMA((PAIR,)), DMA((PAIR,)), DMA((PAIR,)), DMA((LINE,)), DMA((1,))],
        compiler_params=pltpu.CompilerParams(collective_id=1, has_side_effects=True, vmem_limit_bytes=67043328),
        name="backward",
    )(*weights, vec, cos, sin, x_in, y_in, d_y, *[saved[l][name] for l in range(LAYERS) for name in SAVED])
    return outs[:5]


def pack_small(b_attn, ln_par, b_up, b_down):
    rows = [b_attn.reshape(PAIR, TILE), ln_par.reshape(PAIR, TILE), b_up, jnp.pad(b_down, ((0, 0), (0, HALF_SEQ)))]
    return jnp.stack(rows, axis=1).reshape(PLANE, TILE)


def solution(mesh):
    axis_name = mesh.axis_names[0]
    batch_spec = P(axis_name)
    weight_specs = (P(None, None, axis_name, None), P(None, None, axis_name), P(None, None, axis_name),
                    P(None, axis_name, None), P(None, axis_name), P(None, axis_name, None), P(None, axis_name))

    def device_step(x, lengths, d_y, w_attn, b_attn, ln_par, w_up, b_up, w_down, b_down):
        cos, sin = rotary_tables()
        keep = (jnp.arange(SEQ)[None] < lengths[0]).astype(F32)
        weights, vec, y, saved = forward(w_attn, w_up, w_down, pack_small(b_attn, ln_par, b_up, b_down), x[0], keep, cos, sin)
        g_attn, g_up, g_down, g_small, d_x = backward(weights, vec, cos, sin, x[0], y, d_y[0], saved)
        rows = g_small.reshape(PAIR, LINE, TILE)
        return (d_x[None], g_attn, rows[:, 0].reshape(PAIR, LINE, SHARD), rows[:, 1].reshape(PAIR, LINE, SHARD), g_up, rows[:, PAIR],
                g_down, rows[:, TRIO, :SHARD])

    return jax.shard_map(device_step, mesh=mesh,
                         in_specs=(batch_spec, batch_spec, batch_spec) + weight_specs,
                         out_specs=(batch_spec,) + weight_specs,
                         check_vma=False)
```

```python
import functools
import math
import jax
import jax.numpy as jnp
import numpy as np
from jax import lax
from jax.experimental import pallas as pl
from jax.experimental.pallas import tpu as pltpu
from jax.sharding import PartitionSpec as P

PAIR = 2
TRIO = 3
LINE = 4
FIVE = 5
SIX = 6
PEERS = 7
PLANE = 8
HEADS = 16
DOWN_ROW = 24
SHARD = 32
HEAD_DIM = 64
HALF_SEQ = 96
TILE = 128
SEQ = 192
SPREAD = 224
BAND = 256
WIDE = 512
DIM = 1024
FAR = 1344
QKV_COLS = 3072
FFN = 4096

MESH = pl.DeviceIdType.MESH
EPS = 1e-5
THETA = 10000.0
NEG_BIG = -1e30
SQRT_HALF = math.sqrt(0.5)
DENSITY = 1.0 / math.sqrt(2.0 * math.pi)
SCALE = HEAD_DIM ** -0.5
F32, BF16 = jnp.float32, jnp.bfloat16
DMA = pltpu.SemaphoreType.DMA


def dot(a, b, ca=1, cb=0, precision=None):
    return lax.dot_general(a, b, (((ca,), (cb,)), ((), ())), preferred_element_type=F32, precision=precision)


def span(index, size):
    return pl.ds(pl.multiple_of(size * index, size), size)


def repeat(count, body):
    def step(i, carry):
        body(i)
        return carry

    lax.fori_loop(0, count, step, 0)


def head(ref, rows):
    return ref.at[pl.ds(0, rows), :]


def local(src, dst, sem):
    return pltpu.make_async_copy(src, dst, sem)


def drain(ref, sem):
    local(ref, ref, sem).wait()


def remote(src, dst, send, recv, dev):
    return pltpu.make_async_remote_copy(src_ref=src, dst_ref=dst, send_sem=send, recv_sem=recv,
                                        device_id=(dev,), device_id_type=MESH)


def rotary_tables():
    lane = np.arange(TILE)
    angles = np.arange(SEQ)[:, None] * THETA ** (-(lane % SHARD) / SHARD)[None, :]
    sign = np.where(lane % HEAD_DIM < SHARD, -1.0, 1.0)
    return np.cos(angles).astype(np.float32), (np.sin(angles) * sign).astype(np.float32)


def rotate(block, cos, sin):
    lane = lax.broadcasted_iota(jnp.int32, block.shape, 1)
    return block * cos + jnp.where((lane & SHARD) == 0, pltpu.roll(block, HALF_SEQ, 1), pltpu.roll(block, SHARD, 1)) * sin


def head_masks(block):
    lane = lax.broadcasted_iota(jnp.int32, block.shape, 1)
    zero = jnp.zeros_like(block)
    return jnp.where(lane < HEAD_DIM, block, zero), jnp.where(lane < HEAD_DIM, zero, block)


def row_mean(x):
    return jnp.mean(x, axis=-1, keepdims=True)


def row_sum(x):
    return jnp.sum(x, axis=-1, keepdims=True)


def column_sum(x):
    return jnp.sum(x, axis=0, keepdims=True)


def normed(x):
    centered = x - row_mean(x)
    inv = lax.rsqrt(row_mean(centered * centered) + EPS)
    return centered * inv, inv


def pick(kind):
    shape = (TILE, DIM)
    return lax.broadcasted_iota(jnp.int32, shape, 0) == SHARD * kind + (lax.broadcasted_iota(jnp.int32, shape, 1) & 31)


def owned(swap):
    shape = (SHARD, DIM)
    row = lax.broadcasted_iota(jnp.int32, shape, 0)
    if swap:
        row = (row & TRIO) * PLANE + (row >> PAIR)
    return row == lax.broadcasted_iota(jnp.int32, shape, 1) >> FIVE


def unpack_vectors(small, vec):
    for l in range(PAIR):
        for t in (0, 1, TRIO):
            rows = small[pl.ds(LINE * l + t, SHARD, stride=PLANE), :].astype(BF16)
            for kind in range(1 if t == TRIO else LINE):
                spread = dot(rows, pick(kind).astype(BF16))
                at = DOWN_ROW + l if t == TRIO else PLANE * l + LINE * t + kind
                vec[pl.ds(at, 1), :] = column_sum(jnp.where(owned(False), spread, 0.0))
        for d in range(SHARD):
            vec[pl.ds(HEADS + LINE * l + d // PLANE, 1), pl.ds(d % PLANE * TILE, TILE)] = small[pl.ds(PLANE * d + LINE * l + PAIR, 1), :]


def pack_vectors(vec, packed):
    for l in range(PAIR):
        for t in (0, 1, TRIO):
            total = None
            for kind in range(1 if t == TRIO else LINE):
                at = DOWN_ROW + l if t == TRIO else PLANE * l + LINE * t + kind
                mine = jnp.where(owned(True), vec[pl.ds(at, 1), :], 0.0)
                part = dot(mine, pick(kind).astype(F32), 1, 1, lax.Precision.HIGHEST)
                total = part if total is None else total + part
            packed[pl.ds(LINE * l + t, SHARD, stride=PLANE), :] = total
        for d in range(SHARD):
            packed[pl.ds(SHARD * (d % PLANE) + PLANE * (d // PLANE) + LINE * l + PAIR, 1), :] = vec[pl.ds(HEADS + LINE * l + d // PLANE, 1),
                                                                              pl.ds(d % PLANE * TILE, TILE)]


def norm_stage(src, vec, at, dst):
    def body(i):
        rows = span(i, SHARD)
        unit, _ = normed(src[rows, :].astype(F32))
        dst[rows, :] = (unit * vec[pl.ds(at, 1), :] + vec[pl.ds(at + 1, 1), :]).astype(BF16)

    repeat(SIX, body)


def project_stage(l, h, w, vec, cos, sin, qkv, kind):
    def body(n):
        cols = span(n, BAND)
        out = dot(h[...], w[pl.ds(DIM * kind, DIM), cols]) + vec[pl.ds(PLANE * l + kind, 1), cols]
        if kind == 0:
            out = out * SCALE
        if kind < PAIR:
            out = jnp.concatenate([rotate(out[:, :TILE], cos[...], sin[...]), rotate(out[:, TILE:], cos[...], sin[...])], axis=1)
        qkv[:, pl.ds(pl.multiple_of(DIM * kind + BAND * n, BAND), BAND)] = out.astype(BF16)

    repeat(LINE, body)


def attend_stage(qkv, keep, probs, ctx, first, count):
    def body(i):
        p = first + i
        query = qkv[:, span(p, TILE)]
        keys = head_masks(qkv[:, span(p + PLANE, TILE)])
        vals = head_masks(qkv[:, span(p + HEADS, TILE)])
        out = None
        for h in range(PAIR):
            scores = jnp.where(keep[...] > 0.5, dot(query, keys[h], 1, 1), NEG_BIG)
            grown = jnp.exp(scores - jnp.max(scores, axis=-1, keepdims=True))
            weight = (grown / row_sum(grown)).astype(BF16)
            probs[PAIR * p + h] = weight
            part = dot(weight, vals[h])
            out = part if out is None else out + part
        ctx[:, span(p, TILE)] = out.astype(BF16)

    repeat(count, body)


def residual_stage(a, w, base, bias, vec, dst, first=0, count=LINE):
    def body(i):
        cols = span(first + i, BAND)
        dst[:, cols] = (base[:, cols].astype(F32) + dot(a[...], w[:, cols]) + vec[pl.ds(bias, 1), cols]).astype(BF16)

    repeat(count, body)


def gelu(pre):
    cdf = 0.5 * (1.0 + lax.erf(pre * SQRT_HALF))
    return pre * cdf, cdf + pre * (jnp.exp(-0.5 * pre * pre) * DENSITY)


def up_stage(l, h, w, vec, act, slope, part):
    def body(n):
        cols, here = span(LINE * part + n, BAND), span(n, BAND)
        pre = dot(h[...], w[pl.ds(DIM * part, DIM), here]) + vec[pl.ds(HEADS + LINE * l + part, 1), here]
        out, slope[:, cols] = gelu(pre)
        act[:, cols] = out.astype(BF16)

    repeat(LINE, body)


def fold(block):
    return sum(block[PLANE * i:PLANE * i + PLANE] for i in range(block.shape[0] // PLANE))


def act_grad_stage(part, d_out, w, slope, d_pre, vec, row):
    def body(n):
        cols, local_cols = span(LINE * part + n, BAND), span(n, BAND)
        grad = dot(d_out[...], w[span(n, BAND), :], 1, 1) * slope[:, local_cols]
        d_pre[:, cols] = grad.astype(BF16)
        vec[pl.ds(row + part, 1), local_cols] = column_sum(grad)

    repeat(LINE, body)


def norm_grad_stage(src, d_h, d_res, gain, vec, row_gain, row_out, row_res, dst):
    zero = jnp.zeros((PLANE, DIM), F32)

    def body(i, carry):
        rows = span(i, SHARD)
        unit, inv = normed(src[rows, :].astype(F32))
        grad = d_h[rows, :]
        scaled = grad * gain
        inner = scaled - row_mean(scaled) - unit * row_mean(scaled * unit)
        res = d_res[rows, :].astype(F32)
        out = (res + inv * inner).astype(BF16)
        dst[rows, :] = out
        return tuple(c + fold(v) for c, v in zip(carry, (grad * unit, grad, out.astype(F32), res)))

    sums = lax.fori_loop(0, SIX, body, (zero,) * LINE)
    for at, value in zip((row_gain, row_gain + 1, row_out, row_res), sums):
        if at is not None:
            vec[pl.ds(at, 1), :] = column_sum(value)


def attend_grad_stage(l, qkv, probs, d_ctx, cos, sin, d_proj, vec):
    def body(p):
        keys = head_masks(qkv[:, span(p + PLANE, TILE)])
        queries = head_masks(qkv[:, span(p, TILE)])
        vals = qkv[:, span(p + HEADS, TILE)]
        outs = head_masks(d_ctx[:, span(p, TILE)])
        d_q = d_k = d_v = 0.0
        for h in range(PAIR):
            weight = probs[PAIR * p + h]
            wide = weight.astype(F32)
            d_weight = dot(outs[h], vals, 1, 1)
            d_score = (wide * (d_weight - row_sum(d_weight * wide))).astype(BF16)
            d_v = d_v + dot(weight, outs[h], 0, 0)
            d_q = d_q + dot(d_score, keys[h])
            d_k = d_k + dot(d_score, queries[h], 0, 0)
        d_q = rotate(d_q, cos[...], -sin[...]) * SCALE
        d_k = rotate(d_k, cos[...], -sin[...])
        for kind, grad in enumerate((d_q, d_k, d_v)):
            grad = grad.astype(BF16)
            d_proj[:, span(p + PLANE * kind, TILE)] = grad
            vec[pl.ds(PLANE * l + kind, 1), span(p, TILE)] = column_sum(grad.astype(F32))

    repeat(PLANE, body)


FORWARD_ORDER = (
    "O0", "O1", "O2", "P1_0", "P0_0", "O3", "O4", "O5", "O6", "Z4_1", "Z0_1m", "P3_0", "O7", "P2_0", "P4_0", "O8",
    "Z4_2", "Z8_1", "Z0_1p", "Z2_1m", "Z1_1m", "Z2_1p", "Z3_1", "Z4_3", "Z1_1p", "Z8_2", "Z1_2m", "P7_0", "Z7_1",
    "Z0_2m", "aua", "Z3_2", "Z0_2p", "Z1_2p", "Z8_3", "P8_0", "Z1_3m", "P5_0", "P6_0", "Z3_3", "Z2_2m", "Z2_2p",
    "Z0_3m", "Z5_1m", "P3_1", "Z2_3m", "Z6_1m", "Z0_3p", "Z6_1p", "P4_1", "Z2_3p", "P4_2", "P3_2", "P3_3", "Q0",
    "Z1_3p", "Z5_1p", "N0", "P4_3", "Z7_2", "Z5_2m", "Q2", "Z7_3", "Q1", "Z5_2p", "PJ0", "PJ1", "Z6_2m", "Z6_2p",
    "wua", "Szu", "PJ2", "AT0", "Z6_3m", "Z6_3p", "P8_1", "AT1", "Q4", "Z5_3m", "Szd", "Q3", "Z5_3p", "P8_2", "AT2",
    "AT3", "P7_1", "RE0", "UP0", "UP1", "P7_2", "Q6", "P8_3", "Q5", "zd_1", "P7_3", "UP2", "UP3", "DN0", "DN1",
    "Bdy", "Q8", "Q7", "DN2", "zu_1", "DN3", "pj0", "pj1", "pj2", "at0", "Rdy", "at1", "at2", "at3", "re0", "Bh2",
    "zd_2", "zu_2", "Rh2", "Ldy", "Lh2", "zd_3", "zu_3", "G",
)
BACKWARD_ORDER = (
    "B2", "X1", "X1d", "P0", "X1x", "R2", "P1", "B3", "Y1", "S2", "C2", "R3", "L2", "C3", "S3", "L3", "H0a", "C4",
    "P2", "S4", "H1a", "B4", "C5", "P3", "R4", "S5", "H3a", "H2a", "L4", "P4", "B5", "I0", "S6", "H0b", "H4a",
    "H1b", "R5", "C6", "B6", "I4", "I3", "L5", "B7", "I1", "H4b", "P5", "H3b", "H5a", "R6", "R7", "I2", "S7", "H5b",
    "L7", "L6", "I5", "P6", "P7", "H6a", "H2b", "H6b", "H7a", "F5", "F3", "F2", "I6", "H7b", "F6", "I7", "F4", "F0",
    "C7", "F7", "F1", "END",
)


LAYERS = PAIR
UNITS = [(0, SIX)] + [(0, piece) for piece in range(SIX)] + [(1, 0), (1, 1)]
ROUTES = [("b", 0, 1)] + [("b", 0, 1), ("b", 1, 0), ("a", 0, 1), ("a", 1, 0)] * LAYERS


SAVED = ("h1", "qkv", "probs", "ctx", "mid", "h2", "act", "slope")
KEPT = [(l, name) for l in range(LAYERS) for name in SAVED[:PLANE - PAIR * l]]
SAVED_SHAPES = {"h1": (SEQ, DIM), "qkv": (SEQ, QKV_COLS), "probs": (HEADS, SEQ, SEQ), "ctx": (SEQ, DIM), "mid": (SEQ, DIM),
                "h2": (SEQ, DIM), "act": (SEQ, FFN), "slope": (SEQ, FFN)}


def saved_type(name):
    return F32 if name == "slope" else BF16


def plane_cast(peer, far, sems):
    send, recv, push_send, push_recv = sems

    def block(r, half):
        return far.at[pl.ds(SEQ * (r - 1) + HALF_SEQ * half, HALF_SEQ), :]

    def push(r, half):
        remote(block(r, half), block(r + 1, half), push_send, push_recv, peer(1)).start()

    def start(src):
        for r in (PAIR, LINE):
            for half in (0, 1):
                remote(src.at[pl.ds(HALF_SEQ * half, HALF_SEQ), :], block(r, half), send, recv.at[r - PAIR + half], peer(r)).start()
        remote(src, head(far, SEQ), push_send, push_recv, peer(1)).start()

    def relay():
        for r, half, onward in ((PAIR, 0, LINE), (LINE, 1, PAIR), (PAIR, 1, None), (LINE, 0, None)):
            drain(block(r, half), recv.at[r - PAIR + half])
            if onward is not None:
                remote(block(r, half), block(SIX, half), send, recv.at[LINE + half], peer(onward)).start()
            push(r, half)

    def last():
        for half in (0, 1):
            drain(block(SIX, half), recv.at[LINE + half])
            push(SIX, half)

    def arrived():
        drain(head(far, 768), push_recv)

    def sent():
        drain(head(far, 576), send)
        drain(head(far, 768), push_send)

    return start, relay, last, arrived, sent


def plane_peer(me, core, xc, yc):
    def peer(r):
        out = me
        if r & 1:
            out = out + 1 - PAIR * core
        if r & PAIR:
            out = out + PAIR - LINE * xc
        if r & LINE:
            out = out + LINE - PLANE * yc
        return out

    return peer


def in_order(order, tasks):
    assert sorted(order) == sorted(tasks)
    for name in order:
        tasks[name]()


def forward_kernel(*refs):
    (wa, wu, wd, sm, x, keep, cos, sin, d_y), refs = refs[:9], refs[9:]
    (fa, fu, fd, fs, fu_mine, fd_mine, h_far, dy_far, out_vec, out_mid), refs = refs[:10], refs[10:]
    saved, refs = dict(zip(KEPT, refs)), refs[len(KEPT):]
    (va, vu, vd, vs), refs = refs[:LINE], refs[LINE:]
    acts, refs = dict(zip(KEPT, refs)), refs[len(KEPT):]
    (y, vec, small_in, small, w_even, w_odd, load_sem, save_sem, own_sem, xy_sem, z_sem, push_send, push_recv,
     recv_sem, line_send, line_recv, spread_send, spread_recv, mine_sem, bc_send, bc_recv, bp_send, bp_recv) = refs
    me = lax.axis_index("fsdp")
    core, xc, yc, zc = me % PAIR, (me // PAIR) % PAIR, (me // LINE) % PAIR, me // PLANE
    partner = me + 1 - PAIR * core
    near = (me + PAIR - LINE * xc, me + LINE - PLANE * yc)
    up, down = me + PLANE, me - PLANE
    has_up, has_down = zc < TRIO, zc > 0

    def full(u, src):
        layer, piece = UNITS[u]
        if piece < PAIR:
            return fa.at[layer, pl.ds(PAIR * piece, PAIR), pl.ds(pl.multiple_of(SHARD * src, SHARD), SHARD), :]
        if piece < LINE:
            return fu.at[pl.ds(pl.multiple_of(SHARD * src + HEADS * (piece - PAIR), HEADS), HEADS), :]
        if piece < SIX:
            return fd.at[pl.ds(pl.multiple_of(TILE * src + HEAD_DIM * (piece - LINE), HEAD_DIM), HEAD_DIM), :]
        return fs.at[pl.ds(pl.multiple_of(PLANE * src, PLANE), PLANE), :]

    def own(u):
        layer, piece = UNITS[u]
        if piece < PAIR:
            return va.at[layer, pl.ds(PAIR * piece, PAIR)]
        if piece < LINE:
            return vu.at[layer, pl.ds(HEADS * (piece - PAIR), HEADS), :]
        if piece < SIX:
            return vd.at[layer, pl.ds(HEAD_DIM * (piece - LINE), HEAD_DIM), :]
        return vs

    def kind(u):
        return UNITS[u][1] // PAIR

    def order(u):
        return ROUTES[u]

    def tiny(u):
        return 1 if UNITS[u][1] == SIX else 0

    peer = plane_peer(me, core, xc, yc)
    barrier = pltpu.get_barrier_semaphore()
    for r in range(1, PLANE):
        pl.semaphore_signal(barrier, inc=1, device_id=(peer(r),), device_id_type=MESH)

    @pl.when(has_up)
    def _():
        pl.semaphore_signal(barrier, inc=1, device_id=(up,), device_id_type=MESH)

    @pl.when(has_down)
    def _():
        pl.semaphore_signal(barrier, inc=1, device_id=(down,), device_id_type=MESH)

    loads = [local(src, dst, load_sem.at[i])
             for i, (src, dst) in enumerate(((wa, va), (wu, vu), (wd, vd), (sm, vs)))]
    for load in loads:
        load.start()
    for load in loads:
        load.wait()
    pl.semaphore_wait(barrier, PEERS + has_up.astype(jnp.int32) + has_down.astype(jnp.int32))

    def slab(u, src_ref, src, send, recv, dev):
        return remote(src_ref, full(u, src), send, recv, dev)

    def send_z(u, src_ref, src, slot, above, below):
        if above is not None:
            @pl.when(above)
            def _():
                slab(u, src_ref, src, z_sem.at[u], recv_sem.at[u, slot], up).start()
        if below is not None:
            @pl.when(below)
            def _():
                slab(u, src_ref, src, z_sem.at[u], recv_sem.at[u, slot], down).start()

    def send_xy(u, src_ref, src, dim, slot):
        slab(u, src_ref, src, xy_sem.at[u], recv_sem.at[u, slot], near[dim]).start()

    def push(u, src_ref, src):
        slab(u, src_ref, src, push_send.at[kind(u)], push_recv.at[u], partner).start()

    def column(flip_p, p):
        base = me - PLANE * zc
        if flip_p:
            base = base + (near[p] - me)
        return base

    def arrived(u, src, slot):
        slab(u, full(u, src), src, xy_sem.at[u], recv_sem.at[u, slot], me).wait_recv()
        return full(u, src)

    def stage0(u):
        col, p, q = order(u)
        mine = own(u)
        send_z(u, mine, me, zc, has_up, has_down)
        send_xy(u, mine, me, p, LINE + zc)
        send_xy(u, mine, me, q, PLANE)
        push(u, mine, me)
        local(mine, full(u, me), own_sem.at[u]).start()

    def z_arrival(u, dz, steps, flips, send_p):
        col, p, q = order(u)
        for step in steps:
            for flip_p in flips:
                zs = zc + step * dz
                src = column(flip_p, p) + PLANE * zs
                slot = LINE * flip_p + zs
                present = (zc >= dz) if step < 0 else (zc <= TRIO - dz)

                @pl.when(present)
                def _(src=src, slot=slot, step=step):
                    ref = arrived(u, src, slot)
                    send_z(u, ref, src, slot, has_up if step < 0 else None, has_down if step > 0 else None)
                    if send_p:
                        send_xy(u, ref, src, p, LINE + slot)
                    send_xy(u, ref, src, q, PLANE)
                    push(u, ref, src)

    def p_arrival(u, hop):
        col, p, q = order(u)
        zs = lax.rem(zc + hop, LINE)
        src = column(1, p) + PLANE * zs
        ref = arrived(u, src, LINE + zs)
        if col == "b":
            send_z(u, ref, src, LINE + zs, has_up, has_down)
        send_xy(u, ref, src, q, PLANE)
        push(u, ref, src)

    def q_arrivals(u):
        col, p, q = order(u)
        rows = head(fs, HEAD_DIM) if tiny(u) else head(fd, WIDE)
        drain(rows, recv_sem.at[u, PLANE])
        for flip_p in (0, 1):
            base = column(flip_p, p) + (near[q] - me)

            def body(zs, base=base):
                src = base + PLANE * zs
                push(u, full(u, src), src)

            repeat(LINE, body)

    place = me % PLANE

    def mine_cols(where):
        return [(pl.multiple_of(DIM * i + TILE * where, TILE), TILE * i) for i in range(LINE)]

    def spread():
        rows = pl.ds(pl.multiple_of(SHARD * me, SHARD), SHARD)
        for r in (SIX, PAIR, LINE, PEERS, TRIO, FIVE, 1):
            for src, dst in mine_cols(peer(r) % PLANE):
                remote(vu.at[1, :, pl.ds(src, TILE)], fu_mine.at[rows, pl.ds(dst, TILE)], spread_send, spread_recv, peer(r)).start()
        for src, dst in mine_cols(place):
            local(vu.at[1, :, pl.ds(src, TILE)], fu_mine.at[rows, pl.ds(dst, TILE)], mine_sem.at[1]).start()
        local(vd.at[1], fd_mine.at[pl.ds(pl.multiple_of(TILE * zc, TILE), TILE), :], mine_sem.at[0]).start()

    def spread_done():
        drain(head(fu_mine, SPREAD), spread_recv)
        drain(head(fu_mine, SHARD), mine_sem.at[1])

    def line_block(k, zs):
        size = BAND if k else TILE
        return (fu_mine if k else fd_mine).at[pl.ds(pl.multiple_of(size * zs, size), size), :]

    def line_send_on(k, src, zs, above, below):
        for want, dev in ((above, up), (below, down)):
            if want is not None:
                @pl.when(want)
                def _(dev=dev):
                    remote(src, line_block(k, zs), line_send.at[k], line_recv.at[k, zs], dev).start()

    def line_start(k):
        line_send_on(k, line_block(1, zc) if k else vd.at[1], zc, has_up, has_down)

    def line_hop(k, dz):
        for step in (-1, 1):
            zs = zc + step * dz

            @pl.when((zc >= dz) if step < 0 else (zc <= TRIO - dz))
            def _(zs=zs, step=step):
                drain(line_block(k, zs), line_recv.at[k, zs])
                line_send_on(k, line_block(k, zs), zs, has_up if step < 0 else None, has_down if step > 0 else None)

    casts = [plane_cast(peer, far, (bc_send.at[i], bc_recv.at[i], bp_send.at[i], bp_recv.at[i]))
             for i, far in enumerate((dy_far, h_far))]

    def ready(*units):
        for u in units:
            drain(head(fs, TILE) if tiny(u) else head(fd, DIM), push_recv.at[u])
            drain(own(u), own_sem.at[u])

    def fetch(l, what, buf):
        for i in range(LINE):
            src = {"a": lambda: fa.at[l, i], "u": lambda: fu.at[:, pl.ds(DIM * i, DIM)],
                   "d": lambda: fd.at[pl.ds(DIM * i, DIM), :]}[what]()
            local(src, buf.at[pl.ds(DIM * i, DIM), :], load_sem.at[i]).start()

    def fetched(buf, *chunks):
        for i in chunks:
            drain(buf.at[pl.ds(DIM * i, DIM), :], load_sem.at[i])

    def save(l, *names):
        for name in names:
            local(acts[l, name], saved[l, name], save_sem.at[l, SAVED.index(name)]).start()

    def source(l):
        return y if l else x

    def begin():
        ready(0)
        local(fs, small_in, load_sem.at[0]).start()
        drain(small_in, load_sem.at[0])
        small[...] = small_in[...].astype(F32)
        unpack_vectors(small, vec)
        local(vec, out_vec, save_sem.at[0, PLANE]).start()
        norm_stage(x, vec, LINE, acts[0, "h1"])
        save(0, "h1")

    def project(l, buf, kind):
        if kind == 0:
            first = 1 + SIX * l
            ready(first, first + 1)
            fetch(l, "a", buf)
        fetched(buf, kind)
        project_stage(l, acts[l, "h1"], buf, vec, cos, sin, acts[l, "qkv"], kind)
        if kind == PAIR:
            save(l, "qkv")

    def attend(l, part):
        attend_stage(acts[l, "qkv"], keep, acts[l, "probs"], acts[l, "ctx"], PAIR * part, PAIR)

    def settle(l, buf):
        save(l, "probs", "ctx")
        fetched(buf, TRIO)
        residual_stage(acts[l, "ctx"], buf.at[pl.ds(QKV_COLS, DIM), :], source(l), PLANE * l + TRIO, vec, acts[l, "mid"])
        norm_stage(acts[l, "mid"], vec, PLANE * l + SIX, acts[l, "h2"])
        save(l, "mid", "h2")

    def grow(buf, part):
        if part == 0:
            ready(TRIO, LINE)
            fetch(0, "u", buf)
        fetched(buf, part)
        up_stage(0, acts[0, "h2"], buf, vec, acts[0, "act"], acts[0, "slope"], part)
        if part == TRIO:
            save(0, "act", "slope")

    def shrink(buf, n):
        if n == 0:
            ready(FIVE, SIX)
            fetch(0, "d", buf)
            fetched(buf, 0, 1, PAIR, TRIO)
        residual_stage(acts[0, "act"], buf, acts[0, "mid"], DOWN_ROW, vec, y, n, 1)
        if n == TRIO:
            local(y, out_mid, save_sem.at[1, PLANE]).start()
            norm_stage(y, vec, 12, acts[1, "h1"])
            save(1, "h1")

    def gathered():
        for cast in casts:
            cast[TRIO]()

    tasks = {"N0": begin, "RE0": lambda: settle(0, w_even), "re0": lambda: settle(1, w_odd), "aua": spread, "wua": spread_done,
             "Szd": lambda: line_start(0), "Szu": lambda: line_start(1), "Bdy": lambda: casts[0][0](d_y),
             "Bh2": lambda: casts[1][0](acts[1, "h2"]), "Rdy": casts[0][1], "Rh2": casts[1][1], "Ldy": casts[0][PAIR],
             "Lh2": casts[1][PAIR], "G": gathered}
    for i in range(TRIO):
        tasks[f"PJ{i}"] = functools.partial(project, 0, w_even, i)
        tasks[f"pj{i}"] = functools.partial(project, 1, w_odd, i)
        for k, name in enumerate(("zd", "zu")):
            tasks[f"{name}_{i + 1}"] = functools.partial(line_hop, k, i + 1)
    for i in range(LINE):
        tasks[f"AT{i}"] = functools.partial(attend, 0, i)
        tasks[f"at{i}"] = functools.partial(attend, 1, i)
        tasks[f"UP{i}"] = functools.partial(grow, w_odd, i)
        tasks[f"DN{i}"] = functools.partial(shrink, w_even, i)
    for u in range(len(UNITS)):
        tasks[f"O{u}"] = functools.partial(stage0, u)
        tasks[f"Q{u}"] = functools.partial(q_arrivals, u)
        for dz in (1, PAIR, TRIO):
            if order(u)[0] == "a":
                tasks[f"Z{u}_{dz}"] = functools.partial(z_arrival, u, dz, (-1, 1), (0,), True)
            else:
                tasks[f"Z{u}_{dz}m"] = functools.partial(z_arrival, u, dz, (-1,), (0, 1), False)
                tasks[f"Z{u}_{dz}p"] = functools.partial(z_arrival, u, dz, (1,), (0, 1), False)
        for hop in range(LINE if order(u)[0] == "a" else 1):
            tasks[f"P{u}_{hop}"] = functools.partial(p_arrival, u, hop)
    in_order(FORWARD_ORDER, tasks)

    ends = jnp.logical_or(zc == 0, zc == TRIO)
    middle = jnp.logical_not(ends)

    def rows_of(u, units):
        return head(fs, PLANE * units) if tiny(u) else head(fd, HEAD_DIM * units)

    for u in range(len(UNITS)):
        straight = order(u)[0] == "a"
        drain(rows_of(u, 12 if straight else 9), xy_sem.at[u])
        for case, units in ((ends, 1), (middle, FIVE)):
            @pl.when(case)
            def _(u=u, units=units, straight=straight):
                drain(rows_of(u, units if straight else PAIR * units), z_sem.at[u])
    for k in range(PAIR):
        for case, units in ((ends, 1), (middle, FIVE)):
            @pl.when(case)
            def _(k=k, units=units):
                drain(head(fd, TILE * units), line_send.at[k])
    drain(head(fu_mine, SPREAD), spread_send)
    drain(head(fd_mine, TILE), mine_sem.at[0])
    for cast in casts:
        cast[LINE]()
    halves = (fa.at[0], head(fu, WIDE), head(fd, 2048), head(fs, TILE))
    for i, half in enumerate(halves):
        drain(half, push_send.at[i])
    for l, name in KEPT:
        drain(saved[l, name], save_sem.at[l, SAVED.index(name)])
    drain(out_vec, save_sem.at[0, PLANE])
    drain(out_mid, save_sem.at[1, PLANE])


def forward(w_attn, w_up, w_down, small, x, keep, cos, sin, d_y):
    shape, hbm, vmem = jax.ShapeDtypeStruct, pl.BlockSpec(memory_space=pltpu.HBM), pl.BlockSpec(memory_space=pltpu.VMEM)
    kept = [shape(SAVED_SHAPES[name], saved_type(name)) for _, name in KEPT]
    outs = pl.pallas_call(
        forward_kernel,
        out_shape=[shape((LAYERS, LINE, DIM, DIM), BF16), shape((DIM, FFN), BF16), shape((FFN, DIM), BF16),
                   shape((BAND, TILE), BF16), shape((DIM, WIDE), BF16), shape((WIDE, DIM), BF16), shape((FAR, DIM), BF16),
                   shape((FAR, DIM), BF16), shape((SHARD, DIM), F32), shape((SEQ, DIM), BF16)] + kept,
        in_specs=[hbm] * LINE + [vmem] * LINE + [hbm],
        out_specs=[hbm] * (10 + len(kept)),
        scratch_shapes=[pltpu.VMEM(w.shape, BF16) for w in (w_attn, w_up, w_down, small)]
        + [pltpu.VMEM(k.shape, k.dtype) for k in kept]
        + [pltpu.VMEM((SEQ, DIM), BF16), pltpu.VMEM((SHARD, DIM), F32), pltpu.VMEM((BAND, TILE), BF16),
           pltpu.VMEM((BAND, TILE), F32), pltpu.VMEM((FFN, DIM), BF16), pltpu.VMEM((FFN, DIM), BF16),
           DMA((LINE,)), DMA((PAIR, 9)), DMA((len(UNITS),)), DMA((len(UNITS),)), DMA((len(UNITS),)), DMA((LINE,)), DMA((len(UNITS),)),
           DMA((len(UNITS), 9)), DMA((PAIR,)), DMA((PAIR, LINE)), DMA, DMA, DMA((PAIR,)), DMA((PAIR,)), DMA((PAIR, SIX)), DMA((PAIR,)), DMA((PAIR,))],
        compiler_params=pltpu.CompilerParams(collective_id=0, has_side_effects=True, vmem_limit_bytes=60 * DIM * DIM),
        name="forward",
    )(w_attn, w_up, w_down, small, x, keep, cos, sin, d_y)
    return outs[:TRIO], outs[LINE:PLANE], outs[PLANE], outs[9], dict(zip(KEPT, outs[10:]))


PIECES = [(1, name) for name in "UDOQ"] + [(0, name) for name in "DUOQ"]
WIDTH = {"D": WIDE, "U": WIDE, "O": TILE, "Q": 384}
ROWS = SEQ


def acc_shape(name):
    return (WIDE, DIM) if name == "D" else (DIM, WIDTH[name])


def backward_kernel(*refs):
    n = len(PIECES)
    (fa, fu, fd, vec, cos, sin, x_in, y_in, d_y, fu_mine, fd_mine, h_far, dy_far), refs = refs[:13], refs[13:]
    saved, refs = dict(zip(KEPT, refs)), refs[len(KEPT):]
    (g_attn, g_up, g_down, g_small, d_x), refs = refs[:FIVE], refs[FIVE:]
    bc_far, sl_far, refs = (None, None) + refs[:n - PAIR], (None, None) + refs[n - PAIR:PAIR * n - LINE], refs[PAIR * n - LINE:]
    (d_pre_far, d_mid_far, d_proj_far, d_top, pair_far, cross_far), refs = refs[:SIX], refs[SIX:]
    (bc_v, sl_v, sl_w), refs = refs[:TRIO], refs[TRIO:]
    acc, got, refs = refs[:n], refs[n:PAIR * n], refs[PAIR * n:]
    (sum_v, sum_got, sum_line, square, wide, slope_v, qkv_v, probs_v, mid_v, x_v, d_out, d_pre, d_mid, d_proj, d_ctx, d_h,
     g_vec, up_v, down_v, odd_v, even_v), refs = refs[:21], refs[21:]
    (bc_send, bc_recv, push_send, push_recv, sl_send, sl_recv, load_sem, rs_send, rs_recv, out_send, out_recv, own_sem,
     sum_send, sum_recv, square_sem, slope_sem, wide_sem, act_sem, spill_sem, pair_send, pair_recv, cross_send,
     cross_recv) = refs
    bc_in = [None, None, saved[1, "ctx"], saved[1, "h1"], d_top, saved[0, "h2"], saved[0, "ctx"], saved[0, "h1"]]
    sl_in = [None, None, d_mid_far.at[1], d_proj_far.at[1], saved[0, "act"], d_pre_far, d_mid_far.at[0], d_proj_far.at[0]]

    me = lax.axis_index("fsdp")
    core, xc, yc, zc = me % PAIR, (me // PAIR) % PAIR, (me // LINE) % PAIR, me // PLANE
    place = me % PLANE

    peer = plane_peer(me, core, xc, yc)

    def line(k):
        return place + PLANE * lax.rem(zc + k, LINE)

    barrier = pltpu.get_barrier_semaphore()
    for r in range(1, PLANE):
        pl.semaphore_signal(barrier, inc=1, device_id=(peer(r),), device_id_type=MESH)
    for k in range(1, LINE):
        pl.semaphore_signal(barrier, inc=1, device_id=(line(k),), device_id_type=MESH)
    pl.semaphore_wait(barrier, 10)

    casts = [None, None] + [plane_cast(peer, bc_far[u], (bc_send.at[u], bc_recv.at[u], push_send.at[u], push_recv.at[u]))
                            for u in range(PAIR, n)]

    def blocks(u, where):
        name = PIECES[u][1]
        if name == "D":
            return [(pl.multiple_of(DIM * i + TILE * where, TILE), TILE * i, TILE) for i in range(LINE)]
        if name == "Q":
            return [(pl.multiple_of(DIM * i + TILE * where, TILE), TILE * i, TILE) for i in range(TRIO)]
        return [(pl.multiple_of(WIDTH[name] * where, TILE), 0, WIDTH[name])]

    def send_sl(u):
        for r in (PAIR, SIX, LINE, TRIO, PEERS, FIVE, 1):
            for src, dst, width in blocks(u, peer(r) % PLANE):
                remote(sl_in[u].at[:, pl.ds(src, width)], sl_far[u].at[pl.ds(SEQ * (r - 1), SEQ), pl.ds(dst, width)],
                       sl_send.at[u], sl_recv.at[u], peer(r)).start()

    def collect(u):
        name = PIECES[u][1]
        own = [local(bc_in[u], head(bc_v, SEQ), load_sem.at[0])]
        for i, (src, dst, width) in enumerate(blocks(u, place)):
            own.append(local(sl_in[u].at[:, pl.ds(src, width)], sl_v.at[pl.ds(0, SEQ), pl.ds(dst, width)],
                             load_sem.at[1 + i]))
        for c in own:
            c.start()
        drain(sl_far[u], sl_recv.at[u])
        casts[u][TRIO]()
        rest = [local(bc_far[u], bc_v.at[pl.ds(SEQ, FAR), :], load_sem.at[FIVE]),
                local(sl_far[u], sl_v.at[pl.ds(SEQ, FAR), pl.ds(0, WIDTH[name])], load_sem.at[SIX])]
        for c in rest:
            c.start()
        for c in own + rest:
            c.wait()

    def piece_rows(u):
        return acc_shape(PIECES[u][1])[0] // LINE

    def piece(ref, u, d):
        pr = piece_rows(u)
        return ref.at[pl.ds(pl.multiple_of(pr * d, pr), pr), :]

    def step_down_line(u, d, up):
        side = jnp.where(up, 0, 1)
        dst = got[u].at[side, span(d - 1 + side, piece_rows(u)), :]
        remote(piece(acc[u], u, d), dst, rs_send.at[u], rs_recv.at[u, side, d], me + jnp.where(up, PLANE, -PLANE)).start()

    def add_piece(u, side, d):
        pr = piece_rows(u)
        drain(piece(acc[u], u, d), rs_recv.at[u, side, d])
        rows = SHARD

        def body(i, carry):
            at = pl.ds(pl.multiple_of(pr * d + rows * i, rows), rows)
            there = pl.ds(pl.multiple_of(pr * (d - 1 + side) + rows * i, rows), rows)
            acc[u][at, :] = acc[u][at, :] + got[u][side, there, :]
            return carry

        lax.fori_loop(0, pr // rows, body, 0)

    def product(u):
        if u > 1:
            collect(u)
        if u == 1:
            load_all(d_y, dy_far)
        name = PIECES[u][1]
        pr, width = piece_rows(u), WIDTH[name]
        cols_v = sl_w if u == 0 else sl_v

        def body(d, carry):
            at = pl.ds(pl.multiple_of(pr * d, pr), pr)
            if name == "D":
                lhs, rhs = cols_v[:, at], bc_v[...]
            else:
                lhs, rhs = bc_v[:, at], cols_v[:, pl.ds(0, width)]
            acc[u][at, :] = lax.dot_general(lhs, rhs, (((0,), (0,)), ((), ())), preferred_element_type=jnp.float32)
            return carry

        lax.fori_loop(0, LINE, body, 0)

        @pl.when(jnp.logical_or(zc == 0, zc == TRIO))
        def _():
            for hop in range(TRIO):
                step_down_line(u, jnp.where(zc == 0, TRIO - hop, hop), zc == 0)

    def second_hop(u, hop):
        @pl.when(jnp.logical_or(zc == 1, zc == PAIR))
        def _():
            d = jnp.where(zc == 1, TRIO - hop, hop)
            add_piece(u, jnp.where(zc == 1, 0, 1), d)
            step_down_line(u, d, zc == 1)

    def third_hop(u):
        @pl.when(jnp.logical_or(zc == 1, zc == PAIR))
        def _():
            d = jnp.where(zc == 1, 0, TRIO)
            add_piece(u, jnp.where(zc == 1, 1, 0), d)
            step_down_line(u, d, zc == PAIR)

    def finish(u):
        layer, name = PIECES[u]

        @pl.when(zc > 0)
        def _():
            add_piece(u, 0, zc)

        @pl.when(zc < TRIO)
        def _():
            add_piece(u, 1, zc)

        if name == "D":
            local(piece(acc[u], u, zc), g_down.at[layer], own_sem.at[u]).start()
            return
        for r in range(PLANE):
            at = pl.ds(pl.multiple_of(BAND * zc + SHARD * (peer(r) % PLANE), SHARD), SHARD)
            if name == "U" and layer:
                pairs = [(acc[u].at[at, pl.ds(TILE * i, TILE)],
                          g_up.at[layer, :, pl.ds(pl.multiple_of(DIM * i + TILE * place, TILE), TILE)]) for i in range(LINE)]
            elif name == "U":
                pairs = [(acc[u].at[at, :], g_up.at[layer, :, pl.ds(pl.multiple_of(WIDE * place, WIDE), WIDE)])]
            else:
                mats = (TRIO,) if name == "O" else (0, 1, PAIR)
                pairs = [(acc[u].at[at, pl.ds(TILE * i, TILE)],
                          g_attn.at[layer, m, :, pl.ds(pl.multiple_of(TILE * place, TILE), TILE)]) for i, m in enumerate(mats)]
            for src, dst in pairs:
                if r == 0:
                    local(src, dst, own_sem.at[u]).start()
                else:
                    remote(src, dst, out_send.at[u], out_recv.at[u], peer(r)).start()

    def sums_plane():
        for r in range(1, PLANE):
            remote(sum_v.at[pl.ds(pl.multiple_of(SHARD * (peer(r) % PLANE), SHARD), SHARD), :], sum_got.at[pl.ds(SHARD * (r - 1), SHARD), :],
                   sum_send.at[0], sum_recv.at[0], peer(r)).start()

    def sums_line():
        drain(sum_got, sum_recv.at[0])
        total = sum_v[pl.ds(pl.multiple_of(SHARD * place, SHARD), SHARD), :]
        for r in range(1, PLANE):
            total = total + sum_got[pl.ds(SHARD * (r - 1), SHARD), :]
        sum_line[pl.ds(0, SHARD), :] = total
        for i in range(LINE):
            at = pl.ds(PLANE * i + SIX, 1)
            sum_line[at, :] = sum_line[at, :] + g_vec[pl.ds(30, 1), pl.ds(TILE * i, TILE)]
        for k in range(1, LINE):
            remote(sum_line.at[pl.ds(pl.multiple_of(PLANE * lax.rem(zc + k, LINE), PLANE), PLANE), :],
                   sum_line.at[pl.ds(SHARD + PLANE * (k - 1), PLANE), :], sum_send.at[1], sum_recv.at[1], line(k)).start()

    def sums_end():
        drain(head(sum_line, DOWN_ROW), sum_recv.at[1])
        total = sum_line[pl.ds(pl.multiple_of(PLANE * zc, PLANE), PLANE), :]
        for k in range(1, LINE):
            total = total + sum_line[pl.ds(SHARD + PLANE * (k - 1), PLANE), :]
        g_small[...] = total

    squares = [(1, k) for k in range(LINE, PLANE)] + [(0, k) for k in range(PLANE)]
    taken = [0, 0]

    def fetch_square(i):
        if i < len(squares):
            l, k = squares[i]
            src = fd.at[pl.ds(DIM * k, DIM), :] if k < LINE else fa.at[l, (TRIO, 0, 1, PAIR)[k - LINE]]
            local(src, square.at[i % PAIR], square_sem.at[i % PAIR]).start()
            if k < LINE:
                local(saved[0, "slope"].at[:, pl.ds(DIM * k, DIM)], slope_v.at[i % PAIR], slope_sem.at[i % PAIR]).start()

    def fetch_wide(i):
        if i < PLANE:
            local(fu.at[pl.ds(TILE * i, TILE), :], wide.at[i % PAIR], wide_sem.at[i % PAIR]).start()

    def with_square(body):
        i = taken[0]
        drain(square.at[i % PAIR], square_sem.at[i % PAIR])
        if squares[i][1] < LINE:
            drain(slope_v.at[i % PAIR], slope_sem.at[i % PAIR])
        body(square.at[i % PAIR], slope_v.at[i % PAIR])
        fetch_square(i + PAIR)
        taken[0] += 1

    def with_wide(body):
        i = taken[1]
        drain(wide.at[i % PAIR], wide_sem.at[i % PAIR])
        body(wide.at[i % PAIR])
        fetch_wide(i + PAIR)
        taken[1] += 1

    def loads(l):
        pairs = [(saved[l, "qkv"], qkv_v), (saved[l, "probs"], probs_v), (saved[l, "mid"], mid_v), ((x_in, y_in)[l], x_v)]
        return [local(src, dst, act_sem.at[i]) for i, (src, dst) in enumerate(pairs)]

    def spill(src, dst):
        local(src, dst, spill_sem).start()
        drain(src, spill_sem)

    def load_all(mine, others):
        both = [local(mine, head(bc_v, SEQ), load_sem.at[0]), local(others, bc_v.at[pl.ds(SEQ, FAR), :], load_sem.at[FIVE])]
        for c in both:
            c.start()
        for c in both:
            c.wait()

    spare = (x_v, mid_v)

    def token_load(i, r):
        src = d_y if r == 0 else dy_far.at[pl.ds(SEQ * (r - 1), SEQ), :]
        return local(src, spare[i % PAIR], act_sem.at[i % PAIR])

    def token_block(i, r, dst):
        token_load(i, r).wait()
        rows = pl.ds(SEQ * r, SEQ)
        for half in (0, 1):
            cols = pl.ds(BAND * half, BAND)
            out, slope = gelu(dot(bc_v[rows, :], up_v[:, cols]) + g_vec[pl.ds(31, 1), cols])
            grad = dot(spare[i % PAIR][...], down_v[cols, :], 1, 1) * slope
            sl_v[rows, cols] = out.astype(BF16)
            sl_w[rows, cols] = grad.astype(BF16)
            g_vec[pl.ds(30, 1), cols] = g_vec[pl.ds(30, 1), cols] + column_sum(grad)

        def body(k):
            dst[:, span(k, BAND)] = dot(sl_w[rows, :], up_v[span(k, BAND), :], 1, 1)

        repeat(LINE, body)

    BLOCKS = (PEERS, FIVE, TRIO, 1, SIX, PAIR, LINE, 0)

    def even(r):
        return even_v.at[r // PAIR - 1] if r else d_h

    def tokens():
        weights = [local(fu_mine, up_v, square_sem.at[0]), local(fd_mine, down_v, square_sem.at[1])]
        for c in weights:
            c.start()
        token_load(0, BLOCKS[0]).start()
        load_all(saved[1, "h2"], h_far)
        for c in weights:
            c.wait()
        for i in range(LINE):
            g_vec[pl.ds(31, 1), pl.ds(TILE * i, TILE)] = vec[pl.ds(20 + i, 1), pl.ds(pl.multiple_of(TILE * place, TILE), TILE)]
        for i, r in enumerate(BLOCKS):
            if i + 1 < len(BLOCKS):
                token_load(i + 1, BLOCKS[i + 1]).start()
            if r % PAIR:
                buf = odd_v.at[i % PAIR]
                if i > 1:
                    drain(buf, pair_send.at[i - PAIR])
                token_block(i, r, buf)
                remote(buf, pair_far.at[pl.ds(SEQ * (r // PAIR), SEQ), :], pair_send.at[i], pair_recv.at[r // PAIR], peer(1)).start()
            else:
                token_block(i, r, even(r))
        for i in (0, 1):
            drain(odd_v.at[i], pair_send.at[i + PAIR])
            fetch_square(i)
            fetch_wide(i)
        for c in loads(1):
            c.start()

    def add_rows(dst, src):
        def body(i):
            at = span(i, SHARD)
            dst[at, :] = dst[at, :] + src[at, :]

        repeat(SIX, body)

    def pair_add(r):
        buf = odd_v.at[0]
        block = pair_far.at[pl.ds(SEQ * (r // PAIR), SEQ), :]
        drain(block, pair_recv.at[r // PAIR])
        local(block, buf, load_sem.at[0]).start()
        drain(buf, load_sem.at[0])
        add_rows(even(r), buf)
        if r:
            i = r // PAIR - 1
            remote(even(r), cross_far.at[pl.ds(SEQ * i, SEQ), :], cross_send.at[i], cross_recv.at[i], peer(r)).start()

    def cross_end():
        pair_add(0)
        for i in (PAIR, 0, 1):
            block, buf = cross_far.at[pl.ds(SEQ * i, SEQ), :], odd_v.at[i % PAIR]
            drain(block, cross_recv.at[i])
            local(block, buf, load_sem.at[i % PAIR]).start()
            drain(buf, load_sem.at[i % PAIR])
            add_rows(d_h, buf)
        for c in loads(1):
            c.wait()
        local(d_y, d_out, load_sem.at[0]).start()
        drain(d_out, load_sem.at[0])
        norm_mid(1)

    def norm_mid(l):
        norm_grad_stage(mid_v, d_h, d_out, vec[pl.ds(PLANE * l + SIX, 1), :], g_vec, PLANE * l + SIX, PLANE * l + TRIO, DOWN_ROW + l, d_mid)
        spill(d_mid, d_mid_far.at[l])

    def chain_act():
        for c in loads(0):
            c.start()
        for part in range(LINE):
            with_square(lambda w, sl: act_grad_stage(part, d_out, w, sl, d_pre, g_vec, HEADS))
        spill(d_pre, d_pre_far)

    def chain_mid():
        for part in range(PLANE):
            def body(w, part=part):
                d_h[:, pl.ds(TILE * part, TILE)] = dot(d_pre[...], w[...], 1, 1)

            with_wide(body)
        for c in loads(0):
            c.wait()
        norm_mid(0)

    def chain_attend(l):
        def to_ctx(w, _):
            def body(i):
                d_ctx[:, span(i, BAND)] = dot(d_mid[...], w[span(i, BAND), :], 1, 1).astype(BF16)

            repeat(LINE, body)

        with_square(to_ctx)
        attend_grad_stage(l, qkv_v, probs_v, d_ctx, cos, sin, d_proj, g_vec)
        spill(d_proj, d_proj_far.at[l])

    def chain_norm(l):
        for kind in range(TRIO):
            def to_h(w, _, kind=kind):
                def body(i):
                    part = dot(d_proj[:, pl.ds(DIM * kind, DIM)], w[span(i, BAND), :], 1, 1)
                    d_h[:, span(i, BAND)] = d_h[:, span(i, BAND)] + part if kind else part

                repeat(LINE, body)

            with_square(to_h)
        norm_grad_stage(x_v, d_h, d_mid, vec[pl.ds(PLANE * l + LINE, 1), :], g_vec, PLANE * l + LINE, None, None, d_out)
        spill(d_out, (d_x, d_top)[l])
        if l == 0:
            pack_vectors(g_vec, sum_v)
            sums_plane()

    def end():
        sums_line()
        sums_end()

    g_vec[...] = jnp.zeros_like(g_vec)
    tasks = {"X1": tokens, "X1d": lambda: pair_add(SIX), "X1x": lambda: [pair_add(r) for r in (PAIR, LINE)], "Y1": cross_end,
             "C2": lambda: chain_attend(1), "C3": lambda: chain_norm(1), "C4": chain_act, "C5": chain_mid,
             "C6": lambda: chain_attend(0), "C7": lambda: chain_norm(0), "END": end}
    for u in range(n):
        if u > 1:
            tasks[f"B{u}"] = functools.partial(casts[u][0], bc_in[u])
            tasks[f"R{u}"], tasks[f"L{u}"] = casts[u][1], casts[u][PAIR]
            tasks[f"S{u}"] = functools.partial(send_sl, u)
        tasks[f"P{u}"] = functools.partial(product, u)
        for hop, name in enumerate("ab"):
            tasks[f"H{u}{name}"] = functools.partial(second_hop, u, hop)
        tasks[f"I{u}"] = functools.partial(third_hop, u)
        tasks[f"F{u}"] = functools.partial(finish, u)
    in_order(BACKWARD_ORDER, tasks)

    for i in range(TRIO):
        drain(even_v.at[i], cross_send.at[i])
    drain(sum_got, sum_send.at[0])
    drain(head(sum_line, DOWN_ROW), sum_send.at[1])
    for u in range(n):
        name = PIECES[u][1]
        if u > 1:
            casts[u][LINE]()
            drain(sl_far[u], sl_send.at[u])
        drain(head(acc[u], TRIO * piece_rows(u)), rs_send.at[u])
        if name == "D":
            drain(head(acc[u], TILE), own_sem.at[u])
        else:
            drain(head(acc[u], SHARD), own_sem.at[u])
            drain(head(acc[u], SPREAD), out_send.at[u])
            drain(head(acc[u], SPREAD), out_recv.at[u])


def backward(weights, mine, vec, cos, sin, x_in, y_in, d_y, saved):
    n = len(PIECES)
    shape, hbm, vmem = jax.ShapeDtypeStruct, pl.BlockSpec(memory_space=pltpu.HBM), pl.BlockSpec(memory_space=pltpu.VMEM)
    wide = lambda cols: (SEQ, cols)
    far = PIECES[PAIR:]
    outs = pl.pallas_call(
        backward_kernel,
        out_shape=[shape((PAIR, LINE, SHARD, DIM), F32), shape((PAIR, SHARD, FFN), F32), shape((PAIR, TILE, DIM), F32), shape((PLANE, TILE), F32),
                   shape(wide(DIM), BF16)]
        + [shape((FAR, DIM), BF16) for _ in far] + [shape((FAR, WIDTH[name]), BF16) for _, name in far]
        + [shape(wide(FFN), BF16), shape((LAYERS, SEQ, DIM), BF16), shape((LAYERS, SEQ, QKV_COLS), BF16), shape(wide(DIM), BF16),
           shape((768, DIM), F32), shape((576, DIM), F32)],
        in_specs=[hbm] * TRIO + [vmem] * TRIO + [hbm] * (PEERS + len(KEPT)),
        out_specs=[hbm] * TRIO + [vmem] + [hbm] * (PAIR * len(far) + PEERS),
        scratch_shapes=[pltpu.VMEM((1536, DIM), BF16), pltpu.VMEM((1536, WIDE), BF16), pltpu.VMEM((1536, WIDE), BF16)]
        + [pltpu.VMEM(acc_shape(name), F32) for _, name in PIECES]
        + [pltpu.VMEM((PAIR, TRIO * acc_shape(name)[0] // LINE, acc_shape(name)[1]), F32) for _, name in PIECES]
        + [pltpu.VMEM((BAND, TILE), F32), pltpu.VMEM((SPREAD, TILE), F32), pltpu.VMEM((56, TILE), F32),
           pltpu.VMEM((PAIR, DIM, DIM), BF16), pltpu.VMEM((PAIR, TILE, FFN), BF16), pltpu.VMEM((PAIR, SEQ, DIM), F32)]
        + [pltpu.VMEM(s, BF16) for s in (wide(QKV_COLS), (HEADS, SEQ, SEQ), wide(DIM), wide(DIM), wide(DIM), wide(FFN),
                                         wide(DIM), wide(QKV_COLS), wide(DIM))]
        + [pltpu.VMEM(wide(DIM), F32), pltpu.VMEM((SHARD, DIM), F32), pltpu.VMEM((DIM, WIDE), BF16), pltpu.VMEM((WIDE, DIM), BF16),
           pltpu.VMEM((PAIR, SEQ, DIM), F32), pltpu.VMEM((TRIO, SEQ, DIM), F32)]
        + [DMA((n,)), DMA((n, SIX)), DMA((n,)), DMA((n,)), DMA((n,)), DMA((n,)), DMA((PEERS,)), DMA((n,)), DMA((n, PAIR, LINE)),
           DMA((n,)), DMA((n,)), DMA((n,)), DMA((PAIR,)), DMA((PAIR,)), DMA((PAIR,)), DMA((PAIR,)), DMA((PAIR,)), DMA((LINE,)), DMA,
           DMA((LINE,)), DMA((LINE,)), DMA((TRIO,)), DMA((TRIO,))],
        compiler_params=pltpu.CompilerParams(collective_id=1, has_side_effects=True, vmem_limit_bytes=67043328),
        name="backward",
    )(*weights, vec, cos, sin, x_in, y_in, d_y, *mine, *[saved[key] for key in KEPT])
    return outs[:FIVE]


def pack_small(b_attn, ln_par, b_up, b_down):
    rows = [b_attn.reshape(PAIR, TILE), ln_par.reshape(PAIR, TILE), b_up, jnp.pad(b_down, ((0, 0), (0, HALF_SEQ)))]
    return jnp.stack(rows, axis=1).reshape(PLANE, TILE)


def solution(mesh):
    axis_name = mesh.axis_names[0]
    batch_spec = P(axis_name)
    by_row, by_input = P(None, axis_name), P(None, None, axis_name)
    weight_specs = (by_input, by_input, by_input, by_row, by_row, by_row, by_row)

    def device_step(x, lengths, d_y, w_attn, b_attn, ln_par, w_up, b_up, w_down, b_down):
        cos, sin = rotary_tables()
        keep = (jnp.arange(SEQ)[None] < lengths[0]).astype(F32)
        weights, mine, vec, y, saved = forward(w_attn, w_up, w_down, pack_small(b_attn, ln_par, b_up, b_down), x[0], keep,
                                               cos, sin, d_y[0])
        g_attn, g_up, g_down, g_small, d_x = backward(weights, mine, vec, cos, sin, x[0], y, d_y[0], saved)
        rows = g_small.reshape(PAIR, LINE, TILE)
        return (d_x[None], g_attn, rows[:, 0].reshape(PAIR, LINE, SHARD), rows[:, 1].reshape(PAIR, LINE, SHARD), g_up, rows[:, PAIR],
                g_down, rows[:, TRIO, :SHARD])

    return jax.shard_map(device_step, mesh=mesh,
                         in_specs=(batch_spec, batch_spec, batch_spec) + weight_specs,
                         out_specs=(batch_spec,) + weight_specs,
                         check_vma=False)
```

```python
import functools
import math
import jax
import jax.numpy as jnp
import numpy as np
from jax import lax
from jax.experimental import pallas as pl
from jax.experimental.pallas import tpu as pltpu
from jax.sharding import PartitionSpec as P

PAIR = 2
TRIO = 3
LINE = 4
FIVE = 5
SIX = 6
PEERS = 7
PLANE = 8
NINE = 9
DOZEN = 12
FOURTEEN = 14
HEADS = 16
DOWN_ROW = 24
SHARD = 32
HEAD_DIM = 64
HALF_SEQ = 96
TILE = 128
SEQ = 192
SPREAD = 224
BAND = 256
WIDE = 512
HALF_PLANE = 768
DIM = 1024
FAR = 1344
PLANE_SEQ = 1536
QKV_COLS = 3072
FFN = 4096

MESH = pl.DeviceIdType.MESH
EPS = 1e-5
THETA = 10000.0
NEG_BIG = -1e30
SQRT_HALF = math.sqrt(0.5)
DENSITY = 1.0 / math.sqrt(2.0 * math.pi)
KEEP = True
SCALE = HEAD_DIM ** -0.5
F32, BF16 = jnp.float32, jnp.bfloat16
DMA = pltpu.SemaphoreType.DMA


def dot(a, b, ca=1, cb=0, precision=None):
    return lax.dot_general(a, b, (((ca,), (cb,)), ((), ())), preferred_element_type=F32, precision=precision)


def span(index, size):
    return pl.ds(pl.multiple_of(size * index, size), size)


def repeat(count, body):
    def step(i, carry):
        body(i)
        return carry

    lax.fori_loop(0, count, step, 0)


def head(ref, rows):
    return ref.at[pl.ds(0, rows), :]


def local(src, dst, sem):
    return pltpu.make_async_copy(src, dst, sem)


def drain(ref, sem):
    local(ref, ref, sem).wait()


def remote(src, dst, send, recv, dev):
    return pltpu.make_async_remote_copy(src_ref=src, dst_ref=dst, send_sem=send, recv_sem=recv,
                                        device_id=(dev,), device_id_type=MESH)


def rotary_tables():
    lane = np.arange(TILE)
    angles = np.arange(SEQ)[:, None] * THETA ** (-(lane % SHARD) / SHARD)[None, :]
    sign = np.where(lane % HEAD_DIM < SHARD, -1.0, 1.0)
    return np.cos(angles).astype(np.float32), (np.sin(angles) * sign).astype(np.float32)


def rotate(block, cos, sin):
    lane = lax.broadcasted_iota(jnp.int32, block.shape, 1)
    return block * cos + jnp.where((lane & SHARD) == 0, pltpu.roll(block, HALF_SEQ, 1), pltpu.roll(block, SHARD, 1)) * sin


def head_masks(block):
    lane = lax.broadcasted_iota(jnp.int32, block.shape, 1)
    zero = jnp.zeros_like(block)
    return jnp.where(lane < HEAD_DIM, block, zero), jnp.where(lane < HEAD_DIM, zero, block)


def row_mean(x):
    return jnp.mean(x, axis=-1, keepdims=KEEP)


def row_sum(x):
    return jnp.sum(x, axis=-1, keepdims=KEEP)


def column_sum(x):
    return jnp.sum(x, axis=0, keepdims=KEEP)


def normed(x):
    centered = x - row_mean(x)
    inv = lax.rsqrt(row_mean(centered * centered) + EPS)
    return centered * inv, inv


def pick(kind):
    shape = (TILE, DIM)
    return lax.broadcasted_iota(jnp.int32, shape, 0) == SHARD * kind + (lax.broadcasted_iota(jnp.int32, shape, 1) & 31)


def owned(swap):
    shape = (SHARD, DIM)
    row = lax.broadcasted_iota(jnp.int32, shape, 0)
    if swap:
        row = (row & TRIO) * PLANE + (row >> PAIR)
    return row == lax.broadcasted_iota(jnp.int32, shape, 1) >> FIVE


def lane_shift(to):
    shape = (SHARD, TILE)
    return lax.broadcasted_iota(jnp.int32, shape, 0) + to == lax.broadcasted_iota(jnp.int32, shape, 1)


def pack_parameters(b_attn, ln_par, b_up, b_down, wide, out):
    for l in range(PAIR):
        for t, src in enumerate((b_attn, ln_par)):
            wide[pl.ds(LINE * l + t, 1), :] = sum(dot(src[l, pl.ds(k, 1), :], lane_shift(SHARD * k).astype(BF16)) for k in range(LINE))
        wide[pl.ds(LINE * l + PAIR, 1), :] = b_up[pl.ds(l, 1), :].astype(F32)
        wide[pl.ds(LINE * l + TRIO, 1), :] = dot(b_down[pl.ds(l, 1), :], lane_shift(0).astype(BF16))
    out[...] = wide[pl.ds(0, PLANE), :].astype(BF16)


def unpack_vectors(small, vec):
    for l in range(PAIR):
        for t in (0, 1, TRIO):
            rows = small[pl.ds(LINE * l + t, SHARD, stride=PLANE), :].astype(BF16)
            for kind in range(1 if t == TRIO else LINE):
                spread = dot(rows, pick(kind).astype(BF16))
                at = DOWN_ROW + l if t == TRIO else PLANE * l + LINE * t + kind
                vec[pl.ds(at, 1), :] = column_sum(jnp.where(owned(False), spread, 0.0))
        for d in range(SHARD):
            vec[pl.ds(HEADS + LINE * l + d // PLANE, 1), pl.ds(d % PLANE * TILE, TILE)] = small[pl.ds(PLANE * d + LINE * l + PAIR, 1), :]


def pack_vectors(vec, packed):
    for l in range(PAIR):
        for t in (0, 1, TRIO):
            total = None
            for kind in range(1 if t == TRIO else LINE):
                at = DOWN_ROW + l if t == TRIO else PLANE * l + LINE * t + kind
                mine = jnp.where(owned(True), vec[pl.ds(at, 1), :], 0.0)
                part = dot(mine, pick(kind).astype(F32), 1, 1, lax.Precision.HIGHEST)
                total = part if total is None else total + part
            packed[pl.ds(LINE * l + t, SHARD, stride=PLANE), :] = total
        for d in range(SHARD):
            packed[pl.ds(SHARD * (d % PLANE) + PLANE * (d // PLANE) + LINE * l + PAIR, 1), :] = vec[pl.ds(HEADS + LINE * l + d // PLANE, 1),
                                                                              pl.ds(d % PLANE * TILE, TILE)]


def norm_stage(src, vec, at, dst):
    def body(i):
        rows = span(i, SHARD)
        unit, _ = normed(src[rows, :].astype(F32))
        dst[rows, :] = (unit * vec[pl.ds(at, 1), :] + vec[pl.ds(at + 1, 1), :]).astype(BF16)

    repeat(SIX, body)


def project_stage(l, h, w, vec, cos, sin, qkv, kind):
    def body(n):
        cols = span(n, BAND)
        out = dot(h[...], w[pl.ds(DIM * kind, DIM), cols]) + vec[pl.ds(PLANE * l + kind, 1), cols]
        if kind == 0:
            out = out * SCALE
        if kind < PAIR:
            out = jnp.concatenate([rotate(out[:, :TILE], cos[...], sin[...]), rotate(out[:, TILE:], cos[...], sin[...])], axis=1)
        qkv[:, pl.ds(pl.multiple_of(DIM * kind + BAND * n, BAND), BAND)] = out.astype(BF16)

    repeat(LINE, body)


def attend_stage(qkv, keep, probs, ctx, first, count):
    def body(i):
        p = first + i
        query = qkv[:, span(p, TILE)]
        keys = head_masks(qkv[:, span(p + PLANE, TILE)])
        vals = head_masks(qkv[:, span(p + HEADS, TILE)])
        out = None
        for h in range(PAIR):
            scores = jnp.where(keep, dot(query, keys[h], 1, 1), NEG_BIG)
            grown = jnp.exp(scores - jnp.max(scores, axis=-1, keepdims=KEEP))
            weight = (grown / row_sum(grown)).astype(BF16)
            probs[PAIR * p + h] = weight
            part = dot(weight, vals[h])
            out = part if out is None else out + part
        ctx[:, span(p, TILE)] = out.astype(BF16)

    repeat(count, body)


def residual_stage(a, w, base, bias, vec, dst, first=0, count=LINE):
    def body(i):
        cols = span(first + i, BAND)
        dst[:, cols] = (base[:, cols].astype(F32) + dot(a[...], w[:, cols]) + vec[pl.ds(bias, 1), cols]).astype(BF16)

    repeat(count, body)


def gelu(pre):
    cdf = 0.5 * (1.0 + lax.erf(pre * SQRT_HALF))
    return pre * cdf, cdf + pre * (jnp.exp(-0.5 * pre * pre) * DENSITY)


def up_stage(l, h, w, vec, act, slope, part):
    def body(n):
        cols, here = span(LINE * part + n, BAND), span(n, BAND)
        pre = dot(h[...], w[pl.ds(DIM * part, DIM), here]) + vec[pl.ds(HEADS + LINE * l + part, 1), here]
        out, slope[:, cols] = gelu(pre)
        act[:, cols] = out.astype(BF16)

    repeat(LINE, body)


def fold(block):
    return sum(block[PLANE * i:PLANE * i + PLANE] for i in range(block.shape[0] // PLANE))


def act_grad_stage(part, d_out, w, slope, d_pre, vec, row):
    def body(n):
        cols, local_cols = span(LINE * part + n, BAND), span(n, BAND)
        grad = dot(d_out[...], w[span(n, BAND), :], 1, 1) * slope[:, local_cols]
        d_pre[:, cols] = grad.astype(BF16)
        vec[pl.ds(row + part, 1), local_cols] = column_sum(grad)

    repeat(LINE, body)


def norm_grad_stage(src, d_h, d_res, gain, vec, row_gain, row_out, row_res, dst):
    zero = jnp.zeros((PLANE, DIM), F32)

    def body(i, carry):
        rows = span(i, SHARD)
        unit, inv = normed(src[rows, :].astype(F32))
        grad = d_h[rows, :]
        scaled = grad * gain
        inner = scaled - row_mean(scaled) - unit * row_mean(scaled * unit)
        res = d_res[rows, :].astype(F32)
        out = (res + inv * inner).astype(BF16)
        dst[rows, :] = out
        return tuple(c + fold(v) for c, v in zip(carry, (grad * unit, grad, out.astype(F32), res)))

    sums = lax.fori_loop(0, SIX, body, (zero,) * LINE)
    for at, value in zip((row_gain, row_gain + 1, row_out, row_res), sums):
        if at is not None:
            vec[pl.ds(at, 1), :] = column_sum(value)


def attend_grad_stage(l, qkv, probs, d_ctx, cos, sin, d_proj, vec):
    def body(p):
        keys = head_masks(qkv[:, span(p + PLANE, TILE)])
        queries = head_masks(qkv[:, span(p, TILE)])
        vals = qkv[:, span(p + HEADS, TILE)]
        outs = head_masks(d_ctx[:, span(p, TILE)])
        d_q = d_k = d_v = 0.0
        for h in range(PAIR):
            weight = probs[PAIR * p + h]
            wide = weight.astype(F32)
            d_weight = dot(outs[h], vals, 1, 1)
            d_score = (wide * (d_weight - row_sum(d_weight * wide))).astype(BF16)
            d_v = d_v + dot(weight, outs[h], 0, 0)
            d_q = d_q + dot(d_score, keys[h])
            d_k = d_k + dot(d_score, queries[h], 0, 0)
        d_q = rotate(d_q, cos[...], -sin[...]) * SCALE
        d_k = rotate(d_k, cos[...], -sin[...])
        for kind, grad in enumerate((d_q, d_k, d_v)):
            grad = grad.astype(BF16)
            d_proj[:, span(p + PLANE * kind, TILE)] = grad
            vec[pl.ds(PLANE * l + kind, 1), span(p, TILE)] = column_sum(grad.astype(F32))

    repeat(PLANE, body)


FORWARD_ORDER = (
    "O0", "O1", "O2", "O3", "Z11", "O4", "O5", "Z12", "P00", "Z21", "P30", "Z01", "P20", "P10", "Z22", "Z31", "P40",
    "Z23", "Z13", "Y01", "P50", "Z41", "O6", "Z02", "P21", "O7", "Y31", "Y02", "P11", "Y41", "Z42", "P22", "P12",
    "P13", "P60", "O8", "as", "Z03", "Y03", "Z32", "P23", "Y42", "Z61", "Z71", "Z51", "Y32", "Z33", "Q0", "Y33",
    "Q1", "Z81", "Z43", "Y61", "Q2", "Y51", "N0", "Z52", "Z62", "J0", "Y62", "Z82", "Y52", "J1", "Z72", "Z53", "J2",
    "Y43", "A0", "A1", "Z63", "A2", "Sd", "Q3", "A3", "Y63", "Y53", "E0", "Q4", "Z83", "ws", "Z73", "Q6", "Su",
    "U0", "P80", "d0", "Q5", "P70", "P81", "P82", "U1", "P71", "U2", "P83", "U3", "P72", "u0", "P73", "D0", "D1",
    "D2", "By", "D3", "d1", "Q7", "Q8", "u1", "j0", "j1", "j2", "Ry", "a0", "a1", "d2", "a2", "a3", "u2", "e0",
    "Bh", "W", "T1", "Ly", "T0", "Rh", "T4", "T2", "T3", "Lh", "T5", "T7", "T6", "G",
)
BACKWARD_ORDER = (
    "X", "P0", "P1", "B2", "B3", "Y", "R2", "S2", "C2", "L2", "S3", "R3", "C3", "H0a", "C4", "S4", "B4", "H0b",
    "P2", "H1a", "L3", "P3", "R4", "H2a", "H2b", "B5", "L4", "H3a", "P4", "S5", "I2", "C5", "I1", "H3b", "R5", "C6",
    "L5", "I0", "H4a", "H1b", "H4b", "B7", "B6", "P5", "S6", "R6", "I3", "C7", "S7", "H5a", "L6", "F0", "I4", "H5b",
    "R7", "P6", "F2", "F1", "I5", "H6a", "H6b", "L7", "P7", "F5", "F3", "F4", "I6", "H7a", "H7b", "F6", "I7", "F7",
    "END",
)


LAYERS = PAIR
UNITS = [(0, SIX)] + [(0, piece) for piece in range(SIX)] + [(1, 0), (1, 1)]
ROUTES = [("b", 0, 1)] + [(kind, p, 1 - p) for kind in "abba" for p in range(PAIR)]


SAVED = ("h1", "qkv", "probs", "ctx", "mid", "h2", "act", "slope")
KEPT = [(l, name) for l in range(LAYERS) for name in SAVED[:PLANE - PAIR * l]]
SAVED_SHAPES = {"h1": (SEQ, DIM), "qkv": (SEQ, QKV_COLS), "probs": (HEADS, SEQ, SEQ), "ctx": (SEQ, DIM), "mid": (SEQ, DIM),
                "h2": (SEQ, DIM), "act": (SEQ, FFN), "slope": (SEQ, FFN)}


def saved_type(name):
    return F32 if name == "slope" else BF16


def plane_cast(peer, far, sems):
    send, recv, push_send, push_recv = sems

    def block(r, half):
        return far.at[pl.ds(SEQ * (r - 1) + HALF_SEQ * half, HALF_SEQ), :]

    def whole(r):
        return far.at[pl.ds(SEQ * (r - 1), SEQ), :]

    def push(r, half):
        remote(block(r, half), block(r + 1, half), push_send, push_recv.at[r // PAIR], peer(1)).start()

    def start(src):
        for r, half in ((PAIR, 0), (LINE, 1), (PAIR, 1), (LINE, 0)):
            remote(src.at[pl.ds(HALF_SEQ * half, HALF_SEQ), :], block(r, half), send, recv.at[r - PAIR + half], peer(r)).start()
        remote(src, whole(1), push_send, push_recv.at[0], peer(1)).start()

    def relay():
        for r, half, onward in ((PAIR, 0, LINE), (LINE, 1, PAIR), (PAIR, 1, None), (LINE, 0, None)):
            drain(block(r, half), recv.at[r - PAIR + half])
            if onward is not None:
                remote(block(r, half), block(SIX, half), send, recv.at[LINE + half], peer(onward)).start()
            push(r, half)

    def last():
        for half in (0, 1):
            drain(block(SIX, half), recv.at[LINE + half])
            push(SIX, half)

    def arrived(r):
        drain(whole(r), push_recv.at[r // PAIR])

    def sent():
        drain(head(far, 576), send)
        drain(head(far, HALF_PLANE), push_send)

    return start, relay, last, arrived, sent


def plane_peer(me, core, xc, yc):
    def peer(r):
        out = me
        if r & 1:
            out = out + 1 - PAIR * core
        if r & PAIR:
            out = out + PAIR - LINE * xc
        if r & LINE:
            out = out + LINE - PLANE * yc
        return out

    return peer


def in_order(order, tasks):
    assert sorted(order) == sorted(tasks), set(order) ^ set(tasks)
    for name in order:
        tasks[name]()


def token_block(h, d_y, up, down, bias, row, rows, act, d_pre, dst):
    for half in (0, 1):
        cols = pl.ds(BAND * half, BAND)
        out, slope = gelu(dot(h[...], up[:, cols]) + bias[pl.ds(0, 1), cols])
        grad = dot(d_y[...], down[cols, :], 1, 1) * slope
        act[rows, cols] = out.astype(BF16)
        d_pre[rows, cols] = grad.astype(BF16)
        bias[pl.ds(1, 1), cols] = bias[pl.ds(1, 1), cols] + column_sum(grad)

    def body(k):
        dst[:, span(k, BAND)] = dot(d_pre[rows, :], up[span(k, BAND), :], 1, 1)

    repeat(LINE, body)


def add_rows(dst, src):
    def body(i):
        at = span(i, SHARD)
        dst[at, :] = dst[at, :] + src[at, :]

    repeat(SIX, body)


def forward_kernel(*refs):
    (wa, wu, wd, b_attn, ln_par, b_up, b_down, x, length, cos, sin, d_y), refs = refs[:DOZEN], refs[DOZEN:]
    (fa, fu, fd, fs, fu_mine, fd_mine, out_h, out_dy, out_act, out_pre, out_part, out_bias, out_vec, out_mid), refs = (
        refs[:FOURTEEN], refs[FOURTEEN:])
    saved, refs = dict(zip(KEPT, refs)), refs[len(KEPT):]
    (va, vu, vd, vs), refs = refs[:LINE], refs[LINE:]
    acts, refs = dict(zip(KEPT, refs)), refs[len(KEPT):]
    (y, vec, small_in, small, w_even, w_odd, dy_v, h_far, dy_far, up_v, down_v, act_v, pre_v, bias_v, part_v, odd_v, pair_v,
     load_sem, save_sem, own_sem, xy_sem, z_sem, push_send, push_recv, recv_sem, line_send, line_recv, spread_send,
     spread_recv, mine_sem, bc_send, bc_recv, bp_send, bp_recv, pair_send, pair_recv, late_sem) = refs
    keep = lax.broadcasted_iota(jnp.int32, (1, SEQ), 1) < length[0]
    me = lax.axis_index("fsdp")
    core, xc, yc, zc = me % PAIR, (me // PAIR) % PAIR, (me // LINE) % PAIR, me // PLANE
    partner = me + 1 - PAIR * core
    near = (me + PAIR - LINE * xc, me + LINE - PLANE * yc)
    up, down = me + PLANE, me - PLANE
    has_up, has_down = zc < TRIO, zc > 0

    def full(u, src):
        layer, piece = UNITS[u]
        if piece < PAIR:
            return fa.at[layer, pl.ds(PAIR * piece, PAIR), pl.ds(pl.multiple_of(SHARD * src, SHARD), SHARD), :]
        if piece < LINE:
            return fu.at[pl.ds(pl.multiple_of(SHARD * src + HEADS * (piece - PAIR), HEADS), HEADS), :]
        if piece < SIX:
            return fd.at[pl.ds(pl.multiple_of(TILE * src + HEAD_DIM * (piece - LINE), HEAD_DIM), HEAD_DIM), :]
        return fs.at[pl.ds(pl.multiple_of(PLANE * src, PLANE), PLANE), :]

    def own(u):
        layer, piece = UNITS[u]
        if piece < PAIR:
            return va.at[layer, pl.ds(PAIR * piece, PAIR)]
        if piece < LINE:
            return vu.at[layer, pl.ds(HEADS * (piece - PAIR), HEADS), :]
        if piece < SIX:
            return vd.at[layer, pl.ds(HEAD_DIM * (piece - LINE), HEAD_DIM), :]
        return vs

    def kind(u):
        return UNITS[u][1] // PAIR

    def order(u):
        return ROUTES[u]

    def tiny(u):
        return 1 if UNITS[u][1] == SIX else 0

    peer = plane_peer(me, core, xc, yc)
    barrier = pltpu.get_barrier_semaphore()
    for r in range(1, PLANE):
        pl.semaphore_signal(barrier, inc=1, device_id=(peer(r),), device_id_type=MESH)

    @pl.when(has_up)
    def _():
        pl.semaphore_signal(barrier, inc=1, device_id=(up,), device_id_type=MESH)

    @pl.when(has_down)
    def _():
        pl.semaphore_signal(barrier, inc=1, device_id=(down,), device_id_type=MESH)

    loads = [local(src, dst, load_sem.at[i])
             for i, (src, dst) in enumerate(((wa, va), (wu, vu), (wd, vd), (d_y, dy_v)))]
    for load in loads:
        load.start()
    pack_parameters(b_attn, ln_par, b_up, b_down, small, vs)
    bias_v[...] = jnp.zeros_like(bias_v)
    for load in loads:
        load.wait()
    pl.semaphore_wait(barrier, PEERS + has_up.astype(jnp.int32) + has_down.astype(jnp.int32))

    def slab(u, src_ref, src, send, recv, dev):
        return remote(src_ref, full(u, src), send, recv, dev)

    def send_z(u, src_ref, src, slot, above, below):
        if above is not None:
            @pl.when(above)
            def _():
                slab(u, src_ref, src, z_sem.at[u], recv_sem.at[u, slot], up).start()
        if below is not None:
            @pl.when(below)
            def _():
                slab(u, src_ref, src, z_sem.at[u], recv_sem.at[u, slot], down).start()

    def send_xy(u, src_ref, src, dim, slot):
        slab(u, src_ref, src, xy_sem.at[u], recv_sem.at[u, slot], near[dim]).start()

    def push(u, src_ref, src):
        slab(u, src_ref, src, push_send.at[kind(u)], push_recv.at[u], partner).start()

    def column(flip_p, p):
        base = me - PLANE * zc
        if flip_p:
            base = base + (near[p] - me)
        return base

    def arrived(u, src, slot):
        slab(u, full(u, src), src, xy_sem.at[u], recv_sem.at[u, slot], me).wait_recv()
        return full(u, src)

    def stage0(u):
        col, p, q = order(u)
        mine = own(u)
        send_z(u, mine, me, zc, has_up, has_down)
        send_xy(u, mine, me, p, LINE + zc)
        send_xy(u, mine, me, q, PLANE)
        push(u, mine, me)
        local(mine, full(u, me), own_sem.at[u]).start()

    def z_arrival(u, dz, steps, flips, send_p):
        col, p, q = order(u)
        for step in steps:
            for flip_p in flips:
                zs = zc + step * dz
                src = column(flip_p, p) + PLANE * zs
                slot = LINE * flip_p + zs
                present = (zc >= dz) if step < 0 else (zc <= TRIO - dz)

                @pl.when(present)
                def _(src=src, slot=slot, step=step):
                    ref = arrived(u, src, slot)
                    send_z(u, ref, src, slot, has_up if step < 0 else None, has_down if step > 0 else None)
                    if send_p:
                        send_xy(u, ref, src, p, LINE + slot)
                    send_xy(u, ref, src, q, PLANE)
                    push(u, ref, src)

    def p_arrival(u, hop):
        col, p, q = order(u)
        zs = lax.rem(zc + hop, LINE)
        src = column(1, p) + PLANE * zs
        ref = arrived(u, src, LINE + zs)
        if col == "b":
            send_z(u, ref, src, LINE + zs, has_up, has_down)
        send_xy(u, ref, src, q, PLANE)
        push(u, ref, src)

    def q_arrivals(u):
        col, p, q = order(u)
        rows = head(fs, HEAD_DIM) if tiny(u) else head(fd, WIDE)
        drain(rows, recv_sem.at[u, PLANE])
        for flip_p in (0, 1):
            base = column(flip_p, p) + (near[q] - me)

            def body(zs, base=base):
                src = base + PLANE * zs
                push(u, full(u, src), src)

            repeat(LINE, body)

    place = me % PLANE

    def mine_cols(where):
        return [(pl.multiple_of(DIM * i + TILE * where, TILE), TILE * i) for i in range(LINE)]

    def spread():
        rows = pl.ds(pl.multiple_of(SHARD * me, SHARD), SHARD)
        for r in (SIX, PAIR, LINE, PEERS, TRIO, FIVE, 1):
            for src, dst in mine_cols(peer(r) % PLANE):
                remote(vu.at[1, :, pl.ds(src, TILE)], fu_mine.at[rows, pl.ds(dst, TILE)], spread_send.at[0], spread_recv.at[0], peer(r)).start()
        for src, dst in mine_cols(place):
            local(vu.at[1, :, pl.ds(src, TILE)], fu_mine.at[rows, pl.ds(dst, TILE)], mine_sem.at[1]).start()
        local(vd.at[1], fd_mine.at[pl.ds(pl.multiple_of(TILE * zc, TILE), TILE), :], mine_sem.at[0]).start()

    def spread_done():
        drain(head(fu_mine, SPREAD), spread_recv.at[0])
        drain(head(fu_mine, SHARD), mine_sem.at[1])

    def line_block(k, zs):
        size = BAND if k else TILE
        return (fu_mine if k else fd_mine).at[pl.ds(pl.multiple_of(size * zs, size), size), :]

    def line_send_on(k, src, zs, above, below):
        for want, dev in ((above, up), (below, down)):
            if want is not None:
                @pl.when(want)
                def _(dev=dev):
                    remote(src, line_block(k, zs), line_send.at[k], line_recv.at[k, zs], dev).start()

    def line_start(k):
        line_send_on(k, line_block(1, zc) if k else vd.at[1], zc, has_up, has_down)

    def line_hop(k, dz):
        for step in (-1, 1):
            zs = zc + step * dz

            @pl.when((zc >= dz) if step < 0 else (zc <= TRIO - dz))
            def _(zs=zs, step=step):
                drain(line_block(k, zs), line_recv.at[k, zs])
                line_send_on(k, line_block(k, zs), zs, has_up if step < 0 else None, has_down if step > 0 else None)

    casts = [plane_cast(peer, far, (bc_send.at[i], bc_recv.at[i], bp_send.at[i], bp_recv.at[i]))
             for i, far in enumerate((dy_far, h_far))]

    def ready(*units):
        for u in units:
            drain(head(fs, TILE) if tiny(u) else head(fd, DIM), push_recv.at[u])
            drain(own(u), own_sem.at[u])

    def fetch(l, what, buf):
        for i in range(LINE):
            src = {"a": lambda: fa.at[l, i], "u": lambda: fu.at[:, pl.ds(DIM * i, DIM)],
                   "d": lambda: fd.at[pl.ds(DIM * i, DIM), :]}[what]()
            local(src, buf.at[pl.ds(DIM * i, DIM), :], load_sem.at[i]).start()

    def fetched(buf, *chunks):
        for i in chunks:
            drain(buf.at[pl.ds(DIM * i, DIM), :], load_sem.at[i])

    def save(l, *names):
        for name in names:
            local(acts[l, name], saved[l, name], save_sem.at[l, SAVED.index(name)]).start()

    def source(l):
        return y if l else x

    def begin():
        ready(0)
        local(fs, small_in, load_sem.at[0]).start()
        drain(small_in, load_sem.at[0])
        small[...] = small_in[...].astype(F32)
        unpack_vectors(small, vec)
        local(vec, out_vec, save_sem.at[0, PLANE]).start()
        norm_stage(x, vec, LINE, acts[0, "h1"])
        save(0, "h1")

    def project(l, buf, kind):
        if kind == 0:
            first = 1 + SIX * l
            ready(first, first + 1)
            fetch(l, "a", buf)
        fetched(buf, kind)
        project_stage(l, acts[l, "h1"], buf, vec, cos, sin, acts[l, "qkv"], kind)
        if kind == PAIR:
            save(l, "qkv")

    def attend(l, part):
        attend_stage(acts[l, "qkv"], keep, acts[l, "probs"], acts[l, "ctx"], PAIR * part, PAIR)

    def settle(l, buf):
        save(l, "probs", "ctx")
        fetched(buf, TRIO)
        residual_stage(acts[l, "ctx"], buf.at[pl.ds(QKV_COLS, DIM), :], source(l), PLANE * l + TRIO, vec, acts[l, "mid"])
        norm_stage(acts[l, "mid"], vec, PLANE * l + SIX, acts[l, "h2"])
        save(l, "mid", "h2")

    def grow(buf, part):
        if part == 0:
            ready(TRIO, LINE)
            fetch(0, "u", buf)
        fetched(buf, part)
        up_stage(0, acts[0, "h2"], buf, vec, acts[0, "act"], acts[0, "slope"], part)
        if part == TRIO:
            save(0, "act", "slope")

    def shrink(buf, n):
        if n == 0:
            ready(FIVE, SIX)
            fetch(0, "d", buf)
            fetched(buf, 0, 1, PAIR, TRIO)
        residual_stage(acts[0, "act"], buf, acts[0, "mid"], DOWN_ROW, vec, y, n, 1)
        if n == TRIO:
            local(y, out_mid, save_sem.at[1, PLANE]).start()
            norm_stage(y, vec, DOZEN, acts[1, "h1"])
            save(1, "h1")

    def load_mine():
        drain(head(fd_mine, TILE), mine_sem.at[0])
        pairs = [local(fu_mine, up_v, late_sem.at[0]), local(fd_mine, down_v, late_sem.at[1])]
        for c in pairs:
            c.start()
        for c in pairs:
            c.wait()
        for i in range(LINE):
            bias_v[pl.ds(0, 1), pl.ds(TILE * i, TILE)] = vec[pl.ds(20 + i, 1), pl.ds(pl.multiple_of(TILE * place, TILE), TILE)]

    def tokens(r):
        rows = pl.ds(SEQ * r, SEQ)
        there = pl.ds(SEQ * (r - 1), SEQ)
        if r % PAIR:
            for cast in casts:
                cast[TRIO](r)
        h, grad = (h_far.at[there, :], dy_far.at[there, :]) if r else (acts[1, "h2"], dy_v)
        dst = (odd_v if r % PAIR else part_v).at[r // PAIR]
        token_block(h, grad, up_v, down_v, bias_v, 0, rows, act_v, pre_v, dst)
        if r % PAIR:
            remote(dst, pair_v.at[r // PAIR], pair_send.at[r // PAIR], pair_recv.at[r // PAIR], partner).start()

    LATE = ((h_far, out_h), (dy_far, out_dy), (act_v, out_act), (pre_v, out_pre), (bias_v, out_bias))

    def gathered():
        for i, (src, dst) in enumerate(LATE):
            local(src, dst, late_sem.at[i]).start()
        for k in range(LINE):
            drain(pair_v.at[k], pair_recv.at[k])
            add_rows(part_v.at[k], pair_v.at[k])
            local(part_v.at[k], out_part.at[pl.ds(SEQ * k, SEQ), :], late_sem.at[FIVE + k]).start()

    tasks = {"N0": begin, "E0": lambda: settle(0, w_even), "e0": lambda: settle(1, w_odd), "as": spread, "ws": spread_done,
             "Sd": lambda: line_start(0), "Su": lambda: line_start(1), "By": lambda: casts[0][0](dy_v),
             "Bh": lambda: casts[1][0](acts[1, "h2"]), "Ry": casts[0][1], "Rh": casts[1][1], "Ly": casts[0][PAIR],
             "Lh": casts[1][PAIR], "W": load_mine, "G": gathered}
    for r in range(PLANE):
        tasks[f"T{r}"] = functools.partial(tokens, r)
    for i in range(TRIO):
        tasks[f"J{i}"] = functools.partial(project, 0, w_even, i)
        tasks[f"j{i}"] = functools.partial(project, 1, w_odd, i)
        for k, name in enumerate("du"):
            tasks[f"{name}{i}"] = functools.partial(line_hop, k, i + 1)
    for i in range(LINE):
        tasks[f"A{i}"] = functools.partial(attend, 0, i)
        tasks[f"a{i}"] = functools.partial(attend, 1, i)
        tasks[f"U{i}"] = functools.partial(grow, w_odd, i)
        tasks[f"D{i}"] = functools.partial(shrink, w_even, i)
    for u in range(len(UNITS)):
        tasks[f"O{u}"] = functools.partial(stage0, u)
        tasks[f"Q{u}"] = functools.partial(q_arrivals, u)
        for dz in (1, PAIR, TRIO):
            if order(u)[0] == "a":
                tasks[f"Z{u}{dz}"] = functools.partial(z_arrival, u, dz, (-1, 1), (0,), True)
            else:
                tasks[f"Z{u}{dz}"] = functools.partial(z_arrival, u, dz, (-1,), (0, 1), False)
                tasks[f"Y{u}{dz}"] = functools.partial(z_arrival, u, dz, (1,), (0, 1), False)
        for hop in range(LINE if order(u)[0] == "a" else 1):
            tasks[f"P{u}{hop}"] = functools.partial(p_arrival, u, hop)
    in_order(FORWARD_ORDER, tasks)

    ends = jnp.logical_or(zc == 0, zc == TRIO)
    middle = jnp.logical_not(ends)

    def rows_of(u, units):
        return head(fs, PLANE * units) if tiny(u) else head(fd, HEAD_DIM * units)

    for u in range(len(UNITS)):
        straight = order(u)[0] == "a"
        drain(rows_of(u, DOZEN if straight else NINE), xy_sem.at[u])
        for case, units in ((ends, 1), (middle, FIVE)):
            @pl.when(case)
            def _(u=u, units=units, straight=straight):
                drain(rows_of(u, units if straight else PAIR * units), z_sem.at[u])
    for k in range(PAIR):
        for case, units in ((ends, 1), (middle, FIVE)):
            @pl.when(case)
            def _(k=k, units=units):
                drain(head(fd, TILE * units), line_send.at[k])
    drain(head(fu_mine, SPREAD), spread_send.at[0])
    for cast in casts:
        cast[LINE]()
    for i, (src, _) in enumerate(LATE):
        drain(src, late_sem.at[i])
    for k in range(LINE):
        drain(part_v.at[k], late_sem.at[FIVE + k])
        drain(odd_v.at[k], pair_send.at[k])
    halves = (fa.at[0], head(fu, WIDE), head(fd, 2048), head(fs, TILE))
    for i, half in enumerate(halves):
        drain(half, push_send.at[i])
    for l, name in KEPT:
        drain(saved[l, name], save_sem.at[l, SAVED.index(name)])
    drain(out_vec, save_sem.at[0, PLANE])
    drain(out_mid, save_sem.at[1, PLANE])


def forward(w_attn, w_up, w_down, b_attn, ln_par, b_up, b_down, x, lengths, cos, sin, d_y):
    shape, hbm, vmem = jax.ShapeDtypeStruct, pl.BlockSpec(memory_space=pltpu.HBM), pl.BlockSpec(memory_space=pltpu.VMEM)
    kept = [shape(SAVED_SHAPES[name], saved_type(name)) for _, name in KEPT]
    tokens, far, hidden = shape((SEQ, DIM), BF16), shape((FAR, DIM), BF16), shape((PLANE_SEQ, WIDE), BF16)
    up, down, vectors, bias = shape((DIM, WIDE), BF16), shape((WIDE, DIM), BF16), shape((SHARD, DIM), F32), shape((PLANE, WIDE), F32)
    small, blocks = shape((BAND, TILE), BF16), shape((LINE, SEQ, DIM), F32)
    mine = shape((PLANE, TILE), BF16)
    scratch = [w_attn, w_up, w_down, mine] + kept + [tokens, vectors, small, shape((BAND, TILE), F32)]
    scratch += [shape((FFN, DIM), BF16)] * PAIR + [tokens, far, far, up, down, hidden, hidden, bias, blocks, blocks, blocks]
    count = len(UNITS)
    sems = [(LINE,), (PAIR, NINE), (count,), (count,), (count,), (LINE,), (count,), (count, NINE), (PAIR,), (PAIR, LINE), (1,), (1,), (PAIR,), (PAIR,), (PAIR, SIX),
            (PAIR,), (PAIR, LINE), (LINE,), (LINE,), (NINE,)]
    outs = pl.pallas_call(
        forward_kernel,
        out_shape=[shape((LAYERS, LINE, DIM, DIM), BF16), shape((DIM, FFN), BF16), shape((FFN, DIM), BF16), small, up, down,
                   far, far, hidden, hidden, shape((HALF_PLANE, DIM), F32), bias, vectors, tokens] + kept,
        in_specs=[hbm] * TRIO + [vmem] * FIVE + [pl.BlockSpec(memory_space=pltpu.SMEM)] + [vmem] * PAIR + [hbm],
        out_specs=[hbm] * (FOURTEEN + len(kept)),
        scratch_shapes=[pltpu.VMEM(s.shape, s.dtype) for s in scratch] + [DMA(s) for s in sems],
        compiler_params=pltpu.CompilerParams(collective_id=0, has_side_effects=True, vmem_limit_bytes=67043328),
        name="forward",
    )(w_attn, w_up, w_down, b_attn, ln_par, b_up, b_down, x, lengths, cos, sin, d_y)
    return outs[:TRIO], outs[SIX:DOZEN], outs[DOZEN], outs[13], dict(zip(KEPT, outs[FOURTEEN:]))


PIECES = [(1, name) for name in "UDOQ"] + [(0, name) for name in "DUQO"]
WIDTH = {"D": WIDE, "U": WIDE, "O": TILE, "Q": 384}
ROWS = SEQ


def acc_shape(name):
    return (WIDE, DIM) if name == "D" else (DIM, WIDTH[name])


def backward_kernel(*refs):
    n = len(PIECES)
    (fa, fu, fd, vec, cos, sin, x_in, y_in, d_y, h_far, dy_far, act_mine, pre_mine, part_in, bias_in), refs = refs[:15], refs[15:]
    saved, refs = dict(zip(KEPT, refs)), refs[len(KEPT):]
    (g_attn, g_up, g_down, g_small, d_x), refs = refs[:FIVE], refs[FIVE:]
    bc_far, sl_far, refs = (None, None) + refs[:n - PAIR], (None, None) + refs[n - PAIR:PAIR * n - LINE], refs[PAIR * n - LINE:]
    (d_pre_far, d_mid_far, d_proj_far, d_top, cross_far), refs = refs[:FIVE], refs[FIVE:]
    (bc_v, sl_v), refs = refs[:PAIR], refs[PAIR:]
    acc, got, refs = refs[:n], refs[n:PAIR * n], refs[PAIR * n:]
    (sum_v, sum_got, sum_line, square, wide, slope_v, qkv_v, probs_v, mid_v, x_v, d_out, d_pre, d_mid, d_proj, d_ctx, d_h,
     g_vec, odd_v), refs = refs[:18], refs[18:]
    (bc_send, bc_recv, push_send, push_recv, sl_send, sl_recv, load_sem, rs_send, rs_recv, out_send, out_recv, own_sem,
     sum_send, sum_recv, square_sem, slope_sem, wide_sem, act_sem, spill_sem, cross_send, cross_recv, early_sem) = refs
    whole = {(1, "O"): saved[1, "ctx"], (1, "Q"): saved[1, "h1"], (0, "D"): d_top, (0, "U"): saved[0, "h2"],
             (0, "O"): saved[0, "ctx"], (0, "Q"): saved[0, "h1"]}
    sliced = {(1, "O"): d_mid_far.at[1], (1, "Q"): d_proj_far.at[1], (0, "D"): saved[0, "act"], (0, "U"): d_pre_far,
              (0, "O"): d_mid_far.at[0], (0, "Q"): d_proj_far.at[0]}
    bc_in, sl_in = [[where.get(piece) for piece in PIECES] for where in (whole, sliced)]

    me = lax.axis_index("fsdp")
    core, xc, yc, zc = me % PAIR, (me // PAIR) % PAIR, (me // LINE) % PAIR, me // PLANE
    place = me % PLANE

    peer = plane_peer(me, core, xc, yc)

    def line(k):
        return place + PLANE * lax.rem(zc + k, LINE)

    barrier = pltpu.get_barrier_semaphore()
    for r in range(1, PLANE):
        pl.semaphore_signal(barrier, inc=1, device_id=(peer(r),), device_id_type=MESH)
    for k in range(1, LINE):
        pl.semaphore_signal(barrier, inc=1, device_id=(line(k),), device_id_type=MESH)
    pl.semaphore_wait(barrier, 10)

    casts = [None, None] + [plane_cast(peer, bc_far[u], (bc_send.at[u], bc_recv.at[u], push_send.at[u], push_recv.at[u]))
                            for u in range(PAIR, n)]

    def blocks(u, where):
        name = PIECES[u][1]
        if name == "D":
            return [(pl.multiple_of(DIM * i + TILE * where, TILE), TILE * i, TILE) for i in range(LINE)]
        if name == "Q":
            return [(pl.multiple_of(DIM * i + TILE * where, TILE), TILE * i, TILE) for i in range(TRIO)]
        return [(pl.multiple_of(WIDTH[name] * where, TILE), 0, WIDTH[name])]

    def send_sl(u):
        for r in (PAIR, SIX, LINE, TRIO, PEERS, FIVE, 1):
            for src, dst, width in blocks(u, peer(r) % PLANE):
                remote(sl_in[u].at[:, pl.ds(src, width)], sl_far[u].at[pl.ds(SEQ * (r - 1), SEQ), pl.ds(dst, width)],
                       sl_send.at[u], sl_recv.at[u], peer(r)).start()

    def collect(u):
        name = PIECES[u][1]
        own = [local(bc_in[u], head(bc_v, SEQ), load_sem.at[0])]
        for i, (src, dst, width) in enumerate(blocks(u, place)):
            own.append(local(sl_in[u].at[:, pl.ds(src, width)], sl_v.at[pl.ds(0, SEQ), pl.ds(dst, width)],
                             load_sem.at[1 + i]))
        for c in own:
            c.start()
        drain(sl_far[u], sl_recv.at[u])
        for r in (1, TRIO, FIVE, PEERS):
            casts[u][TRIO](r)
        rest = [local(bc_far[u], bc_v.at[pl.ds(SEQ, FAR), :], load_sem.at[FIVE]),
                local(sl_far[u], sl_v.at[pl.ds(SEQ, FAR), pl.ds(0, WIDTH[name])], load_sem.at[SIX])]
        for c in rest:
            c.start()
        for c in own + rest:
            c.wait()

    def piece_rows(u):
        return acc_shape(PIECES[u][1])[0] // LINE

    def piece(ref, u, d):
        pr = piece_rows(u)
        return ref.at[pl.ds(pl.multiple_of(pr * d, pr), pr), :]

    def step_down_line(u, d, up):
        side = jnp.where(up, 0, 1)
        dst = got[u].at[side, span(d - 1 + side, piece_rows(u)), :]
        remote(piece(acc[u], u, d), dst, rs_send.at[u], rs_recv.at[u, side, d], me + jnp.where(up, PLANE, -PLANE)).start()

    def add_piece(u, side, d):
        pr = piece_rows(u)
        drain(piece(acc[u], u, d), rs_recv.at[u, side, d])
        rows = SHARD

        def body(i, carry):
            at = pl.ds(pl.multiple_of(pr * d + rows * i, rows), rows)
            there = pl.ds(pl.multiple_of(pr * (d - 1 + side) + rows * i, rows), rows)
            acc[u][at, :] = acc[u][at, :] + got[u][side, there, :]
            return carry

        lax.fori_loop(0, pr // rows, body, 0)

    def product(u):
        if u > 1:
            collect(u)
        elif u == 0:
            load_all(saved[1, "h2"], h_far, pre_mine)
        else:
            load_all(d_y, dy_far, act_mine)
        name = PIECES[u][1]
        pr, width = piece_rows(u), WIDTH[name]

        def body(d, carry):
            at = pl.ds(pl.multiple_of(pr * d, pr), pr)
            if name == "D":
                lhs, rhs = sl_v[:, at], bc_v[...]
            else:
                lhs, rhs = bc_v[:, at], sl_v[:, pl.ds(0, width)]
            acc[u][at, :] = lax.dot_general(lhs, rhs, (((0,), (0,)), ((), ())), preferred_element_type=jnp.float32)
            return carry

        lax.fori_loop(0, LINE, body, 0)

        @pl.when(jnp.logical_or(zc == 0, zc == TRIO))
        def _():
            for hop in range(TRIO):
                step_down_line(u, jnp.where(zc == 0, TRIO - hop, hop), zc == 0)

    def second_hop(u, hop):
        @pl.when(jnp.logical_or(zc == 1, zc == PAIR))
        def _():
            d = jnp.where(zc == 1, TRIO - hop, hop)
            add_piece(u, jnp.where(zc == 1, 0, 1), d)
            step_down_line(u, d, zc == 1)

    def third_hop(u):
        @pl.when(jnp.logical_or(zc == 1, zc == PAIR))
        def _():
            d = jnp.where(zc == 1, 0, TRIO)
            add_piece(u, jnp.where(zc == 1, 1, 0), d)
            step_down_line(u, d, zc == PAIR)

    def finish(u):
        layer, name = PIECES[u]

        @pl.when(zc > 0)
        def _():
            add_piece(u, 0, zc)

        @pl.when(zc < TRIO)
        def _():
            add_piece(u, 1, zc)

        if name == "D":
            local(piece(acc[u], u, zc), g_down.at[layer], own_sem.at[u]).start()
            return
        for r in range(PLANE):
            at = pl.ds(pl.multiple_of(BAND * zc + SHARD * (peer(r) % PLANE), SHARD), SHARD)
            if name == "U" and layer:
                pairs = [(acc[u].at[at, pl.ds(TILE * i, TILE)],
                          g_up.at[layer, :, pl.ds(pl.multiple_of(DIM * i + TILE * place, TILE), TILE)]) for i in range(LINE)]
            elif name == "U":
                pairs = [(acc[u].at[at, :], g_up.at[layer, :, pl.ds(pl.multiple_of(WIDE * place, WIDE), WIDE)])]
            else:
                mats = (TRIO,) if name == "O" else (0, 1, PAIR)
                pairs = [(acc[u].at[at, pl.ds(TILE * i, TILE)],
                          g_attn.at[layer, m, :, pl.ds(pl.multiple_of(TILE * place, TILE), TILE)]) for i, m in enumerate(mats)]
            for src, dst in pairs:
                if r == 0:
                    local(src, dst, own_sem.at[u]).start()
                else:
                    remote(src, dst, out_send.at[u], out_recv.at[u], peer(r)).start()

    def sums_plane():
        for r in range(1, PLANE):
            remote(sum_v.at[pl.ds(pl.multiple_of(SHARD * (peer(r) % PLANE), SHARD), SHARD), :], sum_got.at[pl.ds(SHARD * (r - 1), SHARD), :],
                   sum_send.at[0], sum_recv.at[0], peer(r)).start()

    def sums_line():
        drain(sum_got, sum_recv.at[0])
        total = sum_v[pl.ds(pl.multiple_of(SHARD * place, SHARD), SHARD), :]
        for r in range(1, PLANE):
            total = total + sum_got[pl.ds(SHARD * (r - 1), SHARD), :]
        sum_line[pl.ds(0, SHARD), :] = total
        for i in range(LINE):
            at = pl.ds(PLANE * i + SIX, 1)
            sum_line[at, :] = sum_line[at, :] + bias_in[pl.ds(1, 1), pl.ds(TILE * i, TILE)]
        for k in range(1, LINE):
            remote(sum_line.at[pl.ds(pl.multiple_of(PLANE * lax.rem(zc + k, LINE), PLANE), PLANE), :],
                   sum_line.at[pl.ds(SHARD + PLANE * (k - 1), PLANE), :], sum_send.at[1], sum_recv.at[1], line(k)).start()

    def sums_end():
        drain(head(sum_line, DOWN_ROW), sum_recv.at[1])
        total = sum_line[pl.ds(pl.multiple_of(PLANE * zc, PLANE), PLANE), :]
        for k in range(1, LINE):
            total = total + sum_line[pl.ds(SHARD + PLANE * (k - 1), PLANE), :]
        g_small[...] = total

    squares = [(1, k) for k in range(LINE, PLANE)] + [(0, k) for k in range(PLANE)]
    taken = [0, 0]

    def fetch_square(i):
        if i < len(squares):
            l, k = squares[i]
            src = fd.at[pl.ds(DIM * k, DIM), :] if k < LINE else fa.at[l, (TRIO, 0, 1, PAIR)[k - LINE]]
            local(src, square.at[i % PAIR], square_sem.at[i % PAIR]).start()
            if k < LINE:
                local(saved[0, "slope"].at[:, pl.ds(DIM * k, DIM)], slope_v.at[i % PAIR], slope_sem.at[i % PAIR]).start()

    def fetch_wide(i):
        if i < PLANE:
            local(fu.at[pl.ds(TILE * i, TILE), :], wide.at[i % PAIR], wide_sem.at[i % PAIR]).start()

    def with_square(body):
        i = taken[0]
        drain(square.at[i % PAIR], square_sem.at[i % PAIR])
        if squares[i][1] < LINE:
            drain(slope_v.at[i % PAIR], slope_sem.at[i % PAIR])
        body(square.at[i % PAIR], slope_v.at[i % PAIR])
        fetch_square(i + PAIR)
        taken[0] += 1

    def with_wide(body):
        i = taken[1]
        drain(wide.at[i % PAIR], wide_sem.at[i % PAIR])
        body(wide.at[i % PAIR])
        fetch_wide(i + PAIR)
        taken[1] += 1

    def loads(l):
        pairs = [(saved[l, "qkv"], qkv_v), (saved[l, "probs"], probs_v), (saved[l, "mid"], mid_v), ((x_in, y_in)[l], x_v)]
        return [local(src, dst, act_sem.at[i]) for i, (src, dst) in enumerate(pairs)]

    def spill(src, dst):
        local(src, dst, spill_sem.at[0]).start()
        drain(src, spill_sem.at[0])

    def load_all(mine, others, columns):
        parts = [local(mine, head(bc_v, SEQ), load_sem.at[0]), local(others, bc_v.at[pl.ds(SEQ, FAR), :], load_sem.at[FIVE]),
                 local(columns, sl_v, load_sem.at[SIX])]
        for c in parts:
            c.start()
        for c in parts:
            c.wait()

    def cross_start():
        for r in (SIX, PAIR, LINE):
            i = r // PAIR - 1
            remote(part_in.at[pl.ds(HALF_SEQ * r, SEQ), :], cross_far.at[pl.ds(SEQ * i, SEQ), :], cross_send.at[i], cross_recv.at[i],
                   peer(r)).start()
        for i in (0, 1):
            fetch_square(i)
            fetch_wide(i)
        for c in loads(1):
            c.start()
        local(head(part_in, SEQ), d_h, early_sem.at[0]).start()
        local(d_y, d_out, early_sem.at[1]).start()

    def cross_end():
        drain(d_h, early_sem.at[0])
        drain(d_out, early_sem.at[1])
        for i in (PAIR, 0, 1):
            block = cross_far.at[pl.ds(SEQ * i, SEQ), :]
            drain(block, cross_recv.at[i])
            local(block, odd_v, load_sem.at[0]).start()
            drain(odd_v, load_sem.at[0])

            def body(k):
                at = span(k, SHARD)
                d_h[at, :] = d_h[at, :] + odd_v[at, :]

            repeat(SIX, body)
        for c in loads(1):
            c.wait()
        norm_mid(1)

    def norm_mid(l):
        norm_grad_stage(mid_v, d_h, d_out, vec[pl.ds(PLANE * l + SIX, 1), :], g_vec, PLANE * l + SIX, PLANE * l + TRIO, DOWN_ROW + l, d_mid)
        spill(d_mid, d_mid_far.at[l])

    def chain_act():
        for c in loads(0):
            c.start()
        for part in range(LINE):
            with_square(lambda w, sl: act_grad_stage(part, d_out, w, sl, d_pre, g_vec, HEADS))
        spill(d_pre, d_pre_far)

    def chain_mid():
        for part in range(PLANE):
            def body(w, part=part):
                d_h[:, pl.ds(TILE * part, TILE)] = dot(d_pre[...], w[...], 1, 1)

            with_wide(body)
        for c in loads(0):
            c.wait()
        norm_mid(0)

    def chain_attend(l):
        def to_ctx(w, _):
            def body(i):
                d_ctx[:, span(i, BAND)] = dot(d_mid[...], w[span(i, BAND), :], 1, 1).astype(BF16)

            repeat(LINE, body)

        with_square(to_ctx)
        attend_grad_stage(l, qkv_v, probs_v, d_ctx, cos, sin, d_proj, g_vec)
        spill(d_proj, d_proj_far.at[l])

    def chain_norm(l):
        for kind in range(TRIO):
            def to_h(w, _, kind=kind):
                def body(i):
                    part = dot(d_proj[:, pl.ds(DIM * kind, DIM)], w[span(i, BAND), :], 1, 1)
                    d_h[:, span(i, BAND)] = d_h[:, span(i, BAND)] + part if kind else part

                repeat(LINE, body)

            with_square(to_h)
        norm_grad_stage(x_v, d_h, d_mid, vec[pl.ds(PLANE * l + LINE, 1), :], g_vec, PLANE * l + LINE, None, None, d_out)
        spill(d_out, (d_x, d_top)[l])
        if l == 0:
            pack_vectors(g_vec, sum_v)
            sums_plane()

    def end():
        sums_line()
        sums_end()

    g_vec[...] = jnp.zeros_like(g_vec)
    tasks = {"X": cross_start, "Y": cross_end,
             "C2": lambda: chain_attend(1), "C3": lambda: chain_norm(1), "C4": chain_act, "C5": chain_mid,
             "C6": lambda: chain_attend(0), "C7": lambda: chain_norm(0), "END": end}
    for u in range(n):
        if u > 1:
            tasks[f"B{u}"] = functools.partial(casts[u][0], bc_in[u])
            tasks[f"R{u}"], tasks[f"L{u}"] = casts[u][1], casts[u][PAIR]
            tasks[f"S{u}"] = functools.partial(send_sl, u)
        tasks[f"P{u}"] = functools.partial(product, u)
        for hop, name in enumerate("ab"):
            tasks[f"H{u}{name}"] = functools.partial(second_hop, u, hop)
        tasks[f"I{u}"] = functools.partial(third_hop, u)
        tasks[f"F{u}"] = functools.partial(finish, u)
    in_order(BACKWARD_ORDER, tasks)

    for i in range(TRIO):
        drain(head(part_in, SEQ), cross_send.at[i])
    drain(sum_got, sum_send.at[0])
    drain(head(sum_line, DOWN_ROW), sum_send.at[1])
    for u in range(n):
        name = PIECES[u][1]
        if u > 1:
            casts[u][LINE]()
            drain(sl_far[u], sl_send.at[u])
        drain(head(acc[u], TRIO * piece_rows(u)), rs_send.at[u])
        if name == "D":
            drain(head(acc[u], TILE), own_sem.at[u])
        else:
            drain(head(acc[u], SHARD), own_sem.at[u])
            drain(head(acc[u], SPREAD), out_send.at[u])
            drain(head(acc[u], SPREAD), out_recv.at[u])


def backward(weights, mine, vec, cos, sin, x_in, y_in, d_y, saved):
    n = len(PIECES)
    shape, hbm, vmem = jax.ShapeDtypeStruct, pl.BlockSpec(memory_space=pltpu.HBM), pl.BlockSpec(memory_space=pltpu.VMEM)

    def tokens(cols, dtype=BF16):
        return shape((SEQ, cols), dtype)

    far = PIECES[PAIR:]
    sums = [shape((rows, TILE), F32) for rows in (BAND, SPREAD, 56)]
    scratch = [shape((PLANE_SEQ, DIM), BF16), shape((PLANE_SEQ, WIDE), BF16)] + [shape(acc_shape(name), F32) for _, name in PIECES]
    scratch += [shape((PAIR, TRIO * acc_shape(name)[0] // LINE, acc_shape(name)[1]), F32) for _, name in PIECES] + sums
    scratch += [shape((PAIR, DIM, DIM), BF16), shape((PAIR, TILE, FFN), BF16), shape((PAIR, SEQ, DIM), F32), tokens(QKV_COLS),
                shape((HEADS, SEQ, SEQ), BF16), tokens(DIM), tokens(DIM), tokens(DIM), tokens(FFN), tokens(DIM), tokens(QKV_COLS),
                tokens(DIM), tokens(DIM, F32), shape((SHARD, DIM), F32), tokens(DIM, F32)]
    sems = [(n,), (n, SIX), (n,), (n, LINE), (n,), (n,), (PEERS,), (n,), (n, PAIR, LINE), (n,), (n,), (n,), (PAIR,), (PAIR,), (PAIR,), (PAIR,), (PAIR,), (LINE,),
            (1,), (TRIO,), (TRIO,), (PAIR,)]
    outs = pl.pallas_call(
        backward_kernel,
        out_shape=[shape((PAIR, LINE, SHARD, DIM), F32), shape((PAIR, SHARD, FFN), F32), shape((PAIR, TILE, DIM), F32), shape((PLANE, TILE), F32),
                   tokens(DIM)]
        + [shape((FAR, DIM), BF16) for _ in far] + [shape((FAR, WIDTH[name]), BF16) for _, name in far]
        + [tokens(FFN), shape((LAYERS, SEQ, DIM), BF16), shape((LAYERS, SEQ, QKV_COLS), BF16), tokens(DIM),
           shape((576, DIM), F32)],
        in_specs=[hbm] * TRIO + [vmem] * TRIO + [hbm] * PLANE + [vmem] + [hbm] * len(KEPT),
        out_specs=[hbm] * TRIO + [vmem] + [hbm] * (PAIR * len(far) + SIX),
        scratch_shapes=[pltpu.VMEM(s.shape, s.dtype) for s in scratch] + [DMA(s) for s in sems],
        compiler_params=pltpu.CompilerParams(collective_id=1, has_side_effects=True, vmem_limit_bytes=67043328),
        name="backward",
    )(*weights, vec, cos, sin, x_in, y_in, d_y, *mine, *[saved[key] for key in KEPT])
    return outs[:FIVE]


def hand_over_kernel(*refs):
    big, small, refs = refs[:LINE], refs[LINE], refs[FIVE:]
    outs, (gb_attn, g_ln, gb_up, gb_down), refs = refs[:LINE], refs[LINE:PLANE], refs[PLANE:]
    held, (in_sem, out_sem) = refs[:LINE], refs[LINE:]
    for i in range(LINE):
        local(big[i], held[i], in_sem.at[i]).start()
    for l in range(PAIR):
        for t, dst in enumerate((gb_attn, g_ln)):
            row = small[pl.ds(LINE * l + t, 1), :]
            for k in range(LINE):
                dst[l, pl.ds(k, 1), :] = (pltpu.roll(row, TILE - SHARD * k, 1) if k else row)[:, :SHARD]
        gb_up[pl.ds(l, 1), :] = small[pl.ds(LINE * l + PAIR, 1), :]
        gb_down[pl.ds(l, 1), :] = small[pl.ds(LINE * l + TRIO, 1), :][:, :SHARD]
    for i in range(LINE):
        drain(held[i], in_sem.at[i])
        local(held[i], outs[i], out_sem.at[i]).start()
    for i in range(LINE):
        drain(held[i], out_sem.at[i])


def hand_over(big, small):
    shape, hbm, vmem = jax.ShapeDtypeStruct, pl.BlockSpec(memory_space=pltpu.HBM), pl.BlockSpec(memory_space=pltpu.VMEM)
    tails = [shape(s, F32) for s in ((PAIR, LINE, SHARD), (PAIR, LINE, SHARD), (PAIR, TILE), (PAIR, SHARD))]
    return pl.pallas_call(
        hand_over_kernel,
        out_shape=[shape(b.shape, b.dtype) for b in big] + tails,
        in_specs=[hbm] * LINE + [vmem],
        out_specs=[hbm] * LINE + [vmem] * LINE,
        scratch_shapes=[pltpu.VMEM(b.shape, b.dtype) for b in big] + [DMA((LINE,)), DMA((LINE,))],
        name="hand_over",
    )(*big, small)


def solution(mesh):
    axis_name = mesh.axis_names[0]
    batch_spec = P(axis_name)
    by_row, by_input = P(None, axis_name), P(None, None, axis_name)
    weight_specs = (by_input, by_input, by_input, by_row, by_row, by_row, by_row)

    def device_step(x, lengths, d_y, w_attn, b_attn, ln_par, w_up, b_up, w_down, b_down):
        cos, sin = rotary_tables()
        weights, mine, vec, y, saved = forward(w_attn, w_up, w_down, b_attn, ln_par, b_up, b_down, x[0], lengths, cos, sin,
                                               d_y[0])
        g_attn, g_up, g_down, g_small, d_x = backward(weights, mine, vec, cos, sin, x[0], y, d_y[0], saved)
        outs = hand_over((d_x, g_attn, g_up, g_down), g_small)
        return (outs[0][None], outs[1], outs[LINE], outs[FIVE], outs[PAIR], outs[SIX], outs[TRIO], outs[PEERS])

    return jax.shard_map(device_step, mesh=mesh,
                         in_specs=(batch_spec, batch_spec, batch_spec) + weight_specs,
                         out_specs=(batch_spec,) + weight_specs,
                         check_vma=False)
```
